32 devices in a mesh: leaf: 8 (over z, y), blk: 4 (over x, core).
Axes of the slice: x: 2, y: 2, z: 4, core: 2. Of those that a mesh axis runs over, the one named last changes fastest.
Arguments:
- src_pos: int32 [4, 2097152], P('blk', 'leaf'), may hold values from 0 to 8388607, as said below
- strengths: float32 [2, 4, 2097152], P(None, 'blk', 'leaf'), may hold values from -0.001953125 to 0.001953125
- tgt_pos: int32 [8388608], P(('leaf', 'blk')), may hold values from 0 to 201326591, as said below
Outputs:
- field: float32 [2, 8388608], P(None, ('leaf', 'blk'))
The draws below stay inside these ranges and needn't reach their ends.
Inputs may be any that keep to these rules, and one draw needn't show every extreme that they name: `src_pos`: row q holds 16384 runs of 128 cells; run b lies in the 128 cells from (q * 16384 + b) * 128 on. `tgt_pos`: the ticks held by index k of leaf, at every index of blk, come in 2048 runs of 128; run j lies in the 12288 ticks from (j * 8 + r) * 12288 on, where r is k with its 3 binary digits in reverse order.
All inputs are finite; a program needn't handle non-finite values.
Results may differ from the reference program's by a relative error of at most 0.0003.
Values sent between devices are 32-bit elements; how exact they have to be, the bound alone decides.
A program may use at most 128 MiB of HBM per device.

```python
import math
import jax
import jax.numpy as jnp
import numpy as np
from jax import lax

R = 16
PER_BOX = 128
TGT_BOX = 128
BOX_CELLS = 128
TOP_TICKS = 201326592
LB = 2048
GROUP_SRC = 2097152
N_LEAF = 8
N_BLK = 4


def draw_src_pos(key, part):
    column_count = N_LEAF * LB * PER_BOX
    row_ids = jnp.arange(N_BLK, dtype=jnp.int32)[:, None]
    columns = jnp.arange(column_count, dtype=jnp.int32)[None, :]
    box_ids = row_ids * (N_LEAF * LB) + columns // PER_BOX
    inside = jax.random.randint(jax.random.fold_in(key, 11), (N_BLK, column_count), 0, BOX_CELLS, dtype=jnp.int32)
    return box_ids * BOX_CELLS + inside


def draw_tgt_pos(key, part):
    per_device = LB * TGT_BOX
    flat_ids = jnp.arange(N_LEAF * N_BLK * per_device, dtype=jnp.int32)
    device = flat_ids // per_device
    leaf_no = device // N_BLK
    run_no = flat_ids % per_device // TGT_BOX
    bit_count = N_LEAF.bit_length() - 1
    reversed_leaf = jnp.zeros_like(leaf_no)
    for bit_no in range(bit_count):
        reversed_leaf = reversed_leaf * 2 + leaf_no // 2 ** bit_no % 2
    box_ticks = TOP_TICKS // (LB * N_LEAF)
    box_ids = run_no * N_LEAF + reversed_leaf
    inside = jax.random.randint(jax.random.fold_in(key, 23), flat_ids.shape, 0, box_ticks, dtype=jnp.int32)
    return box_ids * box_ticks + inside


def level_of(rng, extent, cuts, low, largest):
    def one(position, shards_of):
        heights = jax.random.uniform(jax.random.fold_in(jax.random.fold_in(rng, 6), position), (shards_of,), jnp.float32, low / len(cuts), largest / len(cuts))
        return jnp.repeat(jnp.exp(heights), extent[position] // shards_of).reshape((-1,) + (1,) * (len(extent) - position - 1))

    factor_of = one(*cuts[0])
    for cut in cuts[1:]:
        factor_of = factor_of * one(*cut)
    return factor_of


def gaussian(rng, dims, scale, most, shards=(), kind=jnp.bfloat16):
    drawn = scale * jax.random.normal(rng, dims, jnp.float32)
    if shards:
        drawn = drawn * level_of(rng, dims, shards, -0.22, 0.18)
    return jnp.clip(drawn, -most, most).astype(kind)


def setup_inputs(seed: int = 0) -> dict:
    splits = jax.random.split(jax.random.key(seed), 4)
    src_pos = draw_src_pos(jax.random.fold_in(splits[3], 71), 0)
    strengths = gaussian(splits[1], (2, N_BLK, GROUP_SRC), (N_BLK * GROUP_SRC) ** -0.5, 0.001953125, ((1, 4), (2, 8)), jnp.float32)
    tgt_pos = draw_tgt_pos(jax.random.fold_in(splits[3], 71), 0)
    return {"src_pos": src_pos, "strengths": strengths, "tgt_pos": tgt_pos}


highest_accuracy = lax.Precision.HIGHEST


def node_offsets(box_cells):
    node_index = np.arange(R)
    unit_nodes = (1.0 - np.cos(np.pi * (node_index + 0.5) / R)) / 2.0
    return np.floor(box_cells * unit_nodes).astype(np.int64)


def lagrange_values(node_pos, points):
    basis_rows = []
    for row_node in range(node_pos.shape[0]):
        column = np.ones(points.shape[0])
        for other_node in range(node_pos.shape[0]):
            if other_node != row_node:
                column = column * (points - node_pos[other_node]) / (node_pos[row_node] - node_pos[other_node])
        basis_rows.append(column)
    return np.stack(basis_rows)


def turn_angle(tick_ids, cell_index_list):
    product = tick_ids * cell_index_list
    return product.astype(jnp.float32) * (2.0 * math.pi / 2.0 ** 32)


def leaf_weights(in_box, amounts):
    box_count = in_box.shape[0]
    block_size = min(box_count, 512)
    center = TOP_TICKS // 2
    leaf_nodes = node_offsets(BOX_CELLS)
    node_angles = np.pi * (np.arange(R) + 0.5) / R
    exact_nodes = np.cos(node_angles)
    at_exact = lagrange_values(2.0 * leaf_nodes / BOX_CELLS - 1.0, exact_nodes)
    cheb_at = np.stack([np.cos(degree * node_angles) for degree in range(R)])
    norm_weights = np.where(np.arange(R) == 0, 1.0, 2.0) / R
    coefficients = jnp.asarray(norm_weights[:, None] * (cheb_at @ at_exact.T), jnp.float32)

    def one_block(block_no):
        box_part = lax.dynamic_slice_in_dim(in_box, block_no * block_size, block_size, 0)
        strength_blk = lax.dynamic_slice_in_dim(amounts, block_no * block_size, block_size, 1)
        angles = turn_angle(jnp.int32(center), box_part)
        rotate_re = jnp.cos(angles)
        rotation_imaginary = jnp.sin(angles)
        source_re = rotate_re * strength_blk[0] - rotation_imaginary * strength_blk[1]
        source_im = rotation_imaginary * strength_blk[0] + rotate_re * strength_blk[1]
        scaled = box_part.astype(jnp.float32) * (2.0 / BOX_CELLS) - 1.0
        chebyshev = [jnp.ones_like(scaled), scaled]
        for degree in range(2, R):
            chebyshev.append(2.0 * scaled * chebyshev[-1] - chebyshev[-2])
        moments = jnp.einsum('nbk,xbk->xnb', jnp.stack(chebyshev), jnp.stack([source_re, source_im]), precision=highest_accuracy)
        return jnp.einsum('nt,xnb->xtb', coefficients, moments, precision=highest_accuracy)

    blocks = lax.map(one_block, jnp.arange(box_count // block_size, dtype=jnp.int32))
    mixed_nodes = jnp.transpose(blocks, (1, 2, 0, 3)).reshape(2, R, box_count)
    post_turn = turn_angle(jnp.int32(center), jnp.asarray(leaf_nodes, jnp.int32))
    post_re = jnp.cos(post_turn)[:, None]
    post_im = jnp.sin(post_turn)[:, None]
    out_re = post_re * mixed_nodes[0] + post_im * mixed_nodes[1]
    out_im = post_re * mixed_nodes[1] - post_im * mixed_nodes[0]
    return jnp.stack([out_re, out_im]).reshape(2, R, 1, box_count)


def parent_level(paired, child_ids, tree_level):
    box_a = child_ids.shape[0]
    box_e = child_ids.shape[1]
    box_s = paired.shape[3]
    child_cells = BOX_CELLS * 2 ** tree_level
    child_nodes = node_offsets(child_cells)
    parent_nodes = node_offsets(2 * child_cells)
    inner_cells = np.concatenate([child_nodes, child_nodes + child_cells])
    blend_matrix = jnp.asarray(lagrange_values(parent_nodes / (2.0 * child_cells), inner_cells / (2.0 * child_cells)).reshape(R, 2, R), jnp.float32)
    box_ticks = TOP_TICKS // 2 ** (tree_level + 1)
    centers = child_ids * box_ticks + box_ticks // 2
    pre_turn = turn_angle(centers[:, :, None], jnp.asarray(inner_cells, jnp.int32)[None, None, :]).reshape(box_a, box_e, 2, R)
    pre_re = jnp.cos(pre_turn)[..., None]
    pre_im = jnp.sin(pre_turn)[..., None]
    source = jnp.transpose(paired, (0, 2, 4, 1, 3))[:, :, None]
    rotated_real = pre_re * source[0] - pre_im * source[1]
    rotated_imaginary = pre_im * source[0] + pre_re * source[1]
    accumulated_sum = jnp.einsum('jiw,fpziwd->fjpzd', blend_matrix, jnp.stack([rotated_real, rotated_imaginary]), precision=highest_accuracy)
    post_turn = turn_angle(centers[:, :, None], jnp.asarray(parent_nodes, jnp.int32)[None, None, :])
    post_re = jnp.transpose(jnp.cos(post_turn), (2, 0, 1))[:, :, :, None]
    post_im = jnp.transpose(jnp.sin(post_turn), (2, 0, 1))[:, :, :, None]
    out_re = post_re * accumulated_sum[0] + post_im * accumulated_sum[1]
    out_im = post_re * accumulated_sum[1] - post_im * accumulated_sum[0]
    return jnp.stack([out_re, out_im]).reshape(2, R, box_a * box_e, box_s)


def tree_up(weights, tree_level, first_box):
    box_a = weights.shape[2]
    box_s = weights.shape[3]
    paired = weights.reshape(2, R, box_a, box_s // 2, 2)
    parents = first_box + jnp.arange(box_a, dtype=jnp.int32)
    child_ids = 2 * parents[:, None] + jnp.arange(2, dtype=jnp.int32)[None, :]
    return parent_level(paired, child_ids, tree_level)


def reference(src_pos, strengths, tgt_pos):
    block_count = src_pos.shape[0]
    group_boxes = src_pos.shape[1] // PER_BOX
    tree_depth = group_boxes.bit_length() - 1
    group_cells = group_boxes * BOX_CELLS
    root_list = []
    for source_blk in range(block_count):
        in_box = (src_pos[source_blk] % BOX_CELLS).reshape(group_boxes, PER_BOX)
        amounts = strengths[:, source_blk].reshape(2, group_boxes, PER_BOX)
        weights = leaf_weights(in_box, amounts)
        for tree_level in range(tree_depth):
            weights = tree_up(weights, tree_level, 0)
        root_list.append(weights.reshape(2, R, group_boxes))
    root_sets = jnp.stack(root_list)
    top_nodes = jnp.asarray(node_offsets(group_cells), jnp.int32)
    final_ticks = TOP_TICKS // group_boxes
    target_count = tgt_pos.shape[0]
    block_size = min(target_count, 65536)

    def one_block(block_no):
        ticks_blk = lax.dynamic_slice_in_dim(tgt_pos, block_no * block_size, block_size, 0)
        box_ids = ticks_blk // final_ticks
        picked = jnp.take(root_sets, box_ids, axis=3)
        angles = turn_angle(ticks_blk[None, :], top_nodes[:, None])
        phase_re = jnp.cos(angles)
        phase_im = jnp.sin(angles)
        field_re = jnp.zeros(ticks_blk.shape, jnp.float32)
        field_imaginary = jnp.zeros(ticks_blk.shape, jnp.float32)
        for source_blk in range(block_count):
            part_re = picked[source_blk, 0]
            part_im = picked[source_blk, 1]
            inner_re = jnp.sum(phase_re * part_re - phase_im * part_im, axis=0)
            inner_im = jnp.sum(phase_re * part_im + phase_im * part_re, axis=0)
            outer_turn = turn_angle(ticks_blk, jnp.int32(source_blk * group_cells))
            outer_re = jnp.cos(outer_turn)
            outer_im = jnp.sin(outer_turn)
            field_re = field_re + outer_re * inner_re - outer_im * inner_im
            field_imaginary = field_imaginary + outer_re * inner_im + outer_im * inner_re
        return jnp.stack([field_re, field_imaginary])

    blocks = lax.map(one_block, jnp.arange(target_count // block_size, dtype=jnp.int32))
    return jnp.transpose(blocks, (1, 0, 2)).reshape(2, target_count)
```

```python
import functools
import math

import jax
import jax.numpy as jnp
import numpy as np
from jax import lax
from jax.experimental import pallas as pl
from jax.experimental.pallas import tpu as pltpu
from jax.sharding import PartitionSpec as P

R = 16
PER_BOX = 128
TGT_BOX = 128
BOX_CELLS = 128
TOP_TICKS = 201326592
LANES = 128
HIGHEST = lax.Precision.HIGHEST


def fit_even(values, span, count):
    u = 0.5 * span * span * (1.0 + np.cos(np.pi * (np.arange(400) + 0.5) / 400))
    cheb = np.polynomial.chebyshev.Chebyshev.fit(u, values(np.sqrt(u)), count - 1, domain=[0, span * span])
    return [float(c) for c in cheb.convert(kind=np.polynomial.Polynomial).coef]


COS_POLY = fit_even(lambda y: np.cos(np.pi * y), 0.5, 5)
SIN_POLY = fit_even(lambda y: np.sin(np.pi * y) / y, 0.5, 4)


def horner(coefs, u):
    out = u * coefs[-1] + coefs[-2]
    for c in coefs[-3::-1]:
        out = out * u + c
    return out


def cos_sin_turns(y):
    u = y * y
    c, s = horner(COS_POLY, u), y * horner(SIN_POLY, u)
    twice = s + s
    return 1.0 - twice * s, twice * c


def node_offsets(box_cells):
    node_index = np.arange(R)
    unit_nodes = (1.0 - np.cos(np.pi * (node_index + 0.5) / R)) / 2.0
    return np.floor(box_cells * unit_nodes).astype(np.int64)


def lagrange_values(node_pos, points):
    rows = []
    for row_node in range(node_pos.shape[0]):
        column = np.ones(points.shape[0])
        for other in range(node_pos.shape[0]):
            if other != row_node:
                column = column * (points - node_pos[other]) / (node_pos[row_node] - node_pos[other])
        rows.append(column)
    return np.stack(rows)


def as_real(m):
    return np.block([[m.real, -m.imag], [m.imag, m.real]])


def turn64(a, b):
    product = (a * b + 2**31) % 2**32 - 2**31
    return product * (2.0 * np.pi / 2.0**32)


@functools.cache
def step_matrix(level):
    cells = BOX_CELLS * 2**level
    child, parent = node_offsets(cells), node_offsets(2 * cells)
    inner = np.concatenate([child, child + cells])
    blend = lagrange_values(parent / (2.0 * cells), inner / (2.0 * cells)).reshape(R, 2, R)
    half = TOP_TICKS // 2 ** (level + 2)
    assert half * cells % 2**32 == 2**31
    out = np.zeros((2, 2, 2 * R, 2 * R))
    for e in range(2):
        phase = np.exp(1j * turn64(half if e else -half, child))
        for j in range(2):
            out[e, j] = as_real((-1.0) ** j * blend[:, j, :] * phase[None, :])
    return out


def radix_matrix(first, count):
    total = np.eye(2 * R)[None, None]
    for k in range(count):
        m = step_matrix(first + k)
        n = total.shape[0]
        new = np.zeros((2 * n, 2 * n, 2 * R, 2 * R))
        for a in range(n):
            for b in range(n):
                for e in range(2):
                    for j in range(2):
                        new[2 * a + e, b + j * n] = m[e, j] @ total[a, b]
        total = new
    n = total.shape[0]
    return total.transpose(0, 2, 1, 3).reshape(n * 2 * R, n * 2 * R)


DEGREE = 4


def fit_turn(theta):
    s = np.cos(np.pi * (np.arange(64) + 0.5) / 64)
    fit = np.polynomial.chebyshev.chebfit(s, np.exp(1j * s[:, None] * theta[None, :]), DEGREE)
    power = np.zeros((DEGREE + 1, DEGREE + 1))
    for n in range(DEGREE + 1):
        c = np.polynomial.chebyshev.cheb2poly(np.eye(DEGREE + 1)[n])
        power[: len(c), n] = c
    return power @ fit


@functools.cache
def grid_matrix(depth, blocks):
    cells = BOX_CELLS * 2**depth
    ticks = TOP_TICKS // 2**depth
    step = ticks // LANES
    assert step * LANES == ticks and step % 2 == 0
    nodes = (np.arange(blocks)[:, None] * cells + node_offsets(cells)[None, :]).reshape(-1)
    centers = np.arange(LANES) * step + step // 2 - ticks // 2
    phase = np.exp(1j * turn64(centers[None, :], nodes[:, None]))
    off = (nodes - (blocks * cells - 1) / 2.0) * (step // 2) * (2.0 * np.pi / 2.0**32)
    poly = fit_turn(off)
    out = np.zeros((blocks, 2, R, DEGREE + 1, 2, LANES))
    for p in range(DEGREE + 1):
        b = (poly[p][:, None] * phase).reshape(blocks, R, LANES)
        out[:, 0, :, p, 0], out[:, 0, :, p, 1] = b.real, b.imag
        out[:, 1, :, p, 0], out[:, 1, :, p, 1] = -b.imag, b.real
    return out.reshape(blocks * 2 * R, (DEGREE + 1) * 2 * LANES)


def split_rows(m):
    hi = m.astype(jnp.bfloat16)
    lo = (m - hi.astype(np.float64)).astype(jnp.bfloat16)
    return jnp.asarray(np.concatenate([hi, hi, lo], axis=0))


def leaf_matrix():
    nodes = node_offsets(BOX_CELLS)
    angles = np.pi * (np.arange(R) + 0.5) / R
    at_exact = lagrange_values(2.0 * nodes / BOX_CELLS - 1.0, np.cos(angles))
    cheb_at = np.stack([np.cos(n * angles) for n in range(R)])
    norm = np.where(np.arange(R) == 0, 1.0, 2.0) / R
    g = (norm[:, None] * (cheb_at @ at_exact.T)).astype(np.float32)
    wide = np.repeat(g.T, 8, axis=1)
    zero = np.zeros_like(wide)
    return np.block([[wide, zero], [zero, wide]]).astype(np.float32)


def leaf_kernel(pos_ref, str_ref, mix_ref, out_ref, p_t, re_t, im_t, *, digits):
    def turn_over(beta, slot):
        rows = pl.ds(beta, LANES, stride=digits)
        p_t[slot] = pos_ref[rows, :].T
        re_t[slot] = str_ref[0, rows, :].T
        im_t[slot] = str_ref[1, rows, :].T

    def tile(beta, carry):
        slot = lax.rem(beta, 2)
        turn_over(jnp.minimum(beta + 1, digits - 1), 1 - slot)
        zero = jnp.zeros((8, LANES), jnp.float32)
        acc = tuple((zero, zero) for _ in range(R))
        for i in range(PER_BOX // 8):
            acc = chunk(slot, i, acc)
        low, high = list(acc[: R // 2]), list(acc[R // 2 :])
        top = [high[0]]
        for k in range(1, R // 2):
            top.append(tuple(2.0 * h - m for h, m in zip(high[k], low[R // 2 - k])))
        both = low + top
        stack = jnp.concatenate([x for x, _ in both] + [y for _, y in both], axis=0)
        out_ref[beta] = jnp.dot(mix_ref[...], stack, precision=HIGHEST, preferred_element_type=jnp.float32)
        return carry

    def chunk(slot, i, acc):
        here = pl.ds(i * 8, 8)
        r = p_t[slot, here, :] & (BOX_CELLS - 1)
        turn = (r * (TOP_TICKS // 2)).astype(jnp.float32) * (2.0**-32)
        c, s = cos_sin_turns(turn)
        a, b = re_t[slot, here, :], im_t[slot, here, :]
        v = r.astype(jnp.float32) * (2.0 / BOX_CELLS) - 1.0
        v2 = v + v
        cheb = [None, v]
        for k in range(2, R // 2 + 1):
            cheb.append(v2 * v - 1.0 if k == 2 else v2 * cheb[-1] - cheb[-2])
        x, y = c * a - s * b, s * a + c * b
        out = []
        for part, (x, y) in enumerate([(x, y), (cheb[-1] * x, cheb[-1] * y)]):
            for k in range(R // 2):
                u, w = acc[part * (R // 2) + k]
                out.append((u + x, w + y) if k == 0 else (u + cheb[k] * x, w + cheb[k] * y))
        return tuple(out)

    turn_over(0, 0)
    lax.fori_loop(0, digits, tile, 0)


def leaf_call(pos, strengths):
    boxes = pos.shape[0]
    digits = boxes // LANES
    whole = pl.BlockSpec(memory_space=pltpu.VMEM)
    return pl.pallas_call(
        functools.partial(leaf_kernel, digits=digits),
        out_shape=jax.ShapeDtypeStruct((digits, 2 * R, LANES), jnp.float32),
        in_specs=[whole, whole, whole],
        out_specs=whole,
        scratch_shapes=[
            pltpu.VMEM((2, LANES, LANES), jnp.int32),
            pltpu.VMEM((2, LANES, LANES), jnp.float32),
            pltpu.VMEM((2, LANES, LANES), jnp.float32),
        ],
        name="leaf",
    )(pos, strengths, jnp.asarray(leaf_matrix()))


def finish_kernel(w_ref, tgt_hbm, m_ref, a_hbm, out_hbm, tgt, out, a_buf, tab, bufs, got, coefs,
                  send, recv, gsend, grecv, tsem, asem, osem, *, leaves, blocks, chunks, depth, rows):
    leaf_no, blk_no = lax.axis_index("leaf"), lax.axis_index("blk")
    bits = leaves.bit_length() - 1
    boxes = w_ref.shape[1]
    width = boxes // chunks
    tiles = width // LANES
    cells = BOX_CELLS * 2**depth
    ticks = TOP_TICKS // 2**depth
    sides = [leaf_no // 2**k % 2 for k in range(bits)]
    partners = [leaf_no + (1 - 2 * sides[k]) * 2**k for k in range(bits)]
    suffix = jnp.int32(0)
    for k in range(bits):
        suffix = 2 * suffix + sides[k]
    peers = [lax.rem(blk_no + d, blocks) for d in range(1, blocks)]
    fetch = pltpu.make_async_copy(tgt_hbm, tgt, tsem)
    fetch.start()
    load = pltpu.make_async_copy(a_hbm, a_buf, asem)
    load.start()

    barrier = pltpu.get_barrier_semaphore()
    for k in range(bits):
        pl.semaphore_signal(barrier, inc=1, device_id=(partners[k], blk_no), device_id_type=pl.DeviceIdType.MESH)
    for peer in peers:
        pl.semaphore_signal(barrier, inc=1, device_id=(leaf_no, peer), device_id_type=pl.DeviceIdType.MESH)
    pl.semaphore_wait(barrier, bits + blocks - 1)

    def own(stage, c):
        return w_ref.at[:, pl.ds(c * width, width)] if stage == 0 else bufs.at[stage - 1, c]

    def exchange(stage, c):
        return pltpu.make_async_remote_copy(
            src_ref=own(stage, c), dst_ref=got.at[stage, c],
            send_sem=send.at[stage, c], recv_sem=recv.at[stage, c],
            device_id=(partners[stage], blk_no), device_id_type=pl.DeviceIdType.MESH,
        )

    def spread(d, c):
        here = coefs.at[blk_no, pl.ds(c * tiles, tiles)]
        return pltpu.make_async_remote_copy(
            src_ref=here, dst_ref=here,
            send_sem=gsend.at[d - 1, c], recv_sem=grecv.at[d - 1, c],
            device_id=(leaf_no, peers[d - 1]), device_id_type=pl.DeviceIdType.MESH,
        )

    def combine(todo):
        for stage, c in todo:
            exchange(stage, c).wait_recv()
        results = []
        for stage, c in todo:
            pair = jnp.concatenate([own(stage, c)[...], got[stage, c]], axis=0)
            results.append(mm(m_ref[stage, sides[stage]], pair))
        for (stage, c), w in zip(todo, results):
            if stage < bits - 1:
                bufs[stage, c] = w
            else:
                for i in range(tiles):
                    coefs[blk_no, c * tiles + i] = w[:, i * LANES : (i + 1) * LANES]
        for stage, c in todo:
            if stage < bits - 1:
                exchange(stage + 1, c).start()
            else:
                for d in range(1, blocks):
                    spread(d, c).start()

    pitch = ticks // LANES
    tilt = (blocks * cells - 1) / 2.0 * (pitch // 2) / 2.0**32
    cos_poly = fit_even(lambda y: np.cos(2 * np.pi * y), tilt, 3)
    sin_poly = fit_even(lambda y: np.sin(2 * np.pi * y) / y, tilt, 3)
    cos_poly = [c * tilt ** (2 * k) for k, c in enumerate(cos_poly)]
    sin_poly = [c * tilt ** (2 * k + 1) for k, c in enumerate(sin_poly)]
    below = lax.broadcasted_iota(jnp.int32, (rows, LANES), 0) * (leaves * ticks)

    def evaluate(tile, carry):
        whole = jnp.concatenate([coefs[q, tile] for q in range(blocks)], axis=0).T
        hi = whole.astype(jnp.bfloat16)
        lo = (whole - hi.astype(jnp.float32)).astype(jnp.bfloat16)
        lhs = jnp.concatenate([hi, lo, hi], axis=1)
        for n in range(2 * (DEGREE + 1)):
            tab[n] = jnp.dot(lhs, a_buf[:, n * LANES : (n + 1) * LANES], preferred_element_type=jnp.float32)
        first = pl.multiple_of(tile * LANES, LANES)
        for i in range(LANES // rows):
            base = ((first + i * rows) * leaves + suffix) * ticks
            u = (tgt[pl.ds(first + i * rows, rows), :] - (below + base)).astype(jnp.float32)
            cell = (u * (1.0 / pitch) + (0.5 / pitch)).astype(jnp.int32)
            s = (u - cell.astype(jnp.float32) * pitch) * (2.0 / pitch) - 1.0
            got_at = [jnp.take_along_axis(tab[n, i * rows : (i + 1) * rows, :], cell, axis=1)
                      for n in range(2 * (DEGREE + 1))]
            re, im = got_at[-2], got_at[-1]
            for p in range(DEGREE - 1, -1, -1):
                re, im = re * s + got_at[2 * p], im * s + got_at[2 * p + 1]
            z = s * s
            pc, ps = horner(cos_poly, z), s * horner(sin_poly, z)
            out[pl.ds(2 * (first + i * rows), rows, stride=2), :] = pc * re - ps * im
            out[pl.ds(2 * (first + i * rows) + 1, rows, stride=2), :] = pc * im + ps * re
        return carry

    def put(c):
        span = pl.ds(2 * c * width, 2 * width)
        return pltpu.make_async_copy(out.at[span], out_hbm.at[span], osem.at[c])

    def field(c):
        if c == 0:
            fetch.wait()
            load.wait()
        for d in range(1, blocks):
            spread(d, c).wait_recv()
        lax.fori_loop(c * tiles, (c + 1) * tiles, evaluate, 0)
        put(c).start()

    ahead = min(3, chunks)
    for c in range(ahead):
        exchange(0, c).start()
    for step in range(chunks + bits):
        combine([(k, step - k) for k in range(bits - 1, -1, -1) if 0 <= step - k < chunks])
        if step + ahead < chunks:
            exchange(0, step + ahead).start()
        if step >= bits:
            field(step - bits)
    for c in range(chunks):
        for stage in range(bits):
            exchange(stage, c).wait_send()
        for d in range(1, blocks):
            spread(d, c).wait_send()
        put(c).wait()


def finish_call(weights, ticks, matrices, grid, leaves, blocks, depth, chunks):
    boxes = ticks.shape[0]
    bits = leaves.bit_length() - 1
    width = boxes // chunks
    whole = pl.BlockSpec(memory_space=pltpu.VMEM)
    anywhere = pl.BlockSpec(memory_space=pl.ANY)
    dma = pltpu.SemaphoreType.DMA
    return pl.pallas_call(
        functools.partial(finish_kernel, leaves=leaves, blocks=blocks, chunks=chunks, depth=depth, rows=8),
        out_shape=jax.ShapeDtypeStruct((2 * boxes, TGT_BOX), jnp.float32),
        in_specs=[whole, anywhere, whole, anywhere],
        out_specs=anywhere,
        scratch_shapes=[
            pltpu.VMEM((boxes, TGT_BOX), jnp.int32),
            pltpu.VMEM((2 * boxes, TGT_BOX), jnp.float32),
            pltpu.VMEM(grid.shape, jnp.bfloat16),
            pltpu.VMEM((2 * (DEGREE + 1), LANES, LANES), jnp.float32),
            pltpu.VMEM((bits - 1, chunks, 2 * R, width), jnp.float32),
            pltpu.VMEM((bits, chunks, 2 * R, width), jnp.float32),
            pltpu.VMEM((blocks, boxes // LANES, 2 * R, LANES), jnp.float32),
        ] + [
            dma((bits, chunks)), dma((bits, chunks)),
            dma((blocks - 1, chunks)), dma((blocks - 1, chunks)),
            dma, dma, dma((chunks,)),
        ],
        compiler_params=pltpu.CompilerParams(collective_id=0, has_side_effects=True),
        name="finish",
    )(weights, ticks, matrices, grid)


def table(m):
    return jnp.asarray(m.astype(np.float32))


def mm(a, b):
    return jnp.dot(a, b, precision=HIGHEST, preferred_element_type=jnp.float32)


def local_tree(leaf, boxes):
    low = leaf.shape[0]
    n1 = low.bit_length() - 1
    rest = boxes.bit_length() - 1 - n1
    n2 = rest - rest // 2
    n3 = rest - n2
    c = 2 * R
    y = mm(table(radix_matrix(0, n1)), leaf.reshape(low * c, -1))
    y = y.reshape(low, c, 2**n3, 2**n2).transpose(3, 1, 0, 2).reshape(2**n2 * c, -1)
    y = mm(table(radix_matrix(n1, n2)), y)
    y = y.reshape(2**n2, c, low, 2**n3).transpose(3, 1, 2, 0).reshape(2**n3 * c, -1)
    y = mm(table(radix_matrix(n1 + n2, n3)), y)
    return y.reshape(2**n3, c, low * 2**n2).transpose(1, 2, 0).reshape(c, boxes)


def local(src_pos, strengths, tgt_pos):
    leaf_count = lax.axis_size("leaf")
    leaf_bits = leaf_count.bit_length() - 1
    boxes = src_pos.shape[1] // PER_BOX
    local_depth = boxes.bit_length() - 1
    leaf = leaf_call(src_pos.reshape(boxes, PER_BOX), strengths.reshape(2, boxes, PER_BOX))
    weights = local_tree(leaf, boxes)
    steps = np.stack([step_matrix(local_depth + k) for k in range(leaf_bits)])
    steps[:, 1] = steps[:, 1, ::-1]
    steps = np.concatenate([steps[:, :, 0], steps[:, :, 1]], axis=-1)
    out = finish_call(
        weights, tgt_pos.reshape(boxes, TGT_BOX), table(steps),
        split_rows(grid_matrix(local_depth + leaf_bits, lax.axis_size("blk"))), leaf_count, lax.axis_size("blk"),
        local_depth + leaf_bits, 8,
    )
    return out.reshape(boxes, 2, TGT_BOX).transpose(1, 0, 2).reshape(2, boxes * TGT_BOX)


def solution(mesh):
    return jax.shard_map(
        local,
        mesh=mesh,
        in_specs=(P("blk", "leaf"), P(None, "blk", "leaf"), P(("leaf", "blk"))),
        out_specs=P(None, ("leaf", "blk")),
        check_vma=False,
    )
```

```python
import functools
import math

import jax
import jax.numpy as jnp
import numpy as np
from jax import lax
from jax.experimental import pallas as pl
from jax.experimental.pallas import tpu as pltpu
from jax.sharding import PartitionSpec as P

R = 16
PER_BOX = 128
TGT_BOX = 128
BOX_CELLS = 128
TOP_TICKS = 201326592
LANES = 128
HIGHEST = lax.Precision.HIGHEST


def fit_even(values, span, count):
    u = 0.5 * span * span * (1.0 + np.cos(np.pi * (np.arange(400) + 0.5) / 400))
    cheb = np.polynomial.chebyshev.Chebyshev.fit(u, values(np.sqrt(u)), count - 1, domain=[0, span * span])
    return [float(c) for c in cheb.convert(kind=np.polynomial.Polynomial).coef]


COS_POLY = fit_even(lambda y: np.cos(np.pi * y), 0.5, 5)
SIN_POLY = fit_even(lambda y: np.sin(np.pi * y) / y, 0.5, 4)


def horner(coefs, u):
    out = u * coefs[-1] + coefs[-2]
    for c in coefs[-3::-1]:
        out = out * u + c
    return out


def cos_sin_turns(y):
    u = y * y
    c, s = horner(COS_POLY, u), y * horner(SIN_POLY, u)
    twice = s + s
    return 1.0 - twice * s, twice * c


def node_offsets(box_cells):
    node_index = np.arange(R)
    unit_nodes = (1.0 - np.cos(np.pi * (node_index + 0.5) / R)) / 2.0
    return np.floor(box_cells * unit_nodes).astype(np.int64)


def lagrange_values(node_pos, points):
    rows = []
    for row_node in range(node_pos.shape[0]):
        column = np.ones(points.shape[0])
        for other in range(node_pos.shape[0]):
            if other != row_node:
                column = column * (points - node_pos[other]) / (node_pos[row_node] - node_pos[other])
        rows.append(column)
    return np.stack(rows)


def as_real(m):
    return np.block([[m.real, -m.imag], [m.imag, m.real]])


def turn64(a, b):
    product = (a * b + 2**31) % 2**32 - 2**31
    return product * (2.0 * np.pi / 2.0**32)


@functools.cache
def step_matrix(level):
    cells = BOX_CELLS * 2**level
    child, parent = node_offsets(cells), node_offsets(2 * cells)
    inner = np.concatenate([child, child + cells])
    blend = lagrange_values(parent / (2.0 * cells), inner / (2.0 * cells)).reshape(R, 2, R)
    half = TOP_TICKS // 2 ** (level + 2)
    assert half * cells % 2**32 == 2**31
    out = np.zeros((2, 2, 2 * R, 2 * R))
    for e in range(2):
        phase = np.exp(1j * turn64(half if e else -half, child))
        for j in range(2):
            out[e, j] = as_real((-1.0) ** j * blend[:, j, :] * phase[None, :])
    return out


def radix_matrix(first, count):
    total = np.eye(2 * R)[None, None]
    for k in range(count):
        m = step_matrix(first + k)
        n = total.shape[0]
        new = np.zeros((2 * n, 2 * n, 2 * R, 2 * R))
        for a in range(n):
            for b in range(n):
                for e in range(2):
                    for j in range(2):
                        new[2 * a + e, b + j * n] = m[e, j] @ total[a, b]
        total = new
    n = total.shape[0]
    return total.transpose(0, 2, 1, 3).reshape(n * 2 * R, n * 2 * R)


DEGREE = 4


def fit_turn(theta):
    s = np.cos(np.pi * (np.arange(64) + 0.5) / 64)
    fit = np.polynomial.chebyshev.chebfit(s, np.exp(1j * s[:, None] * theta[None, :]), DEGREE)
    power = np.zeros((DEGREE + 1, DEGREE + 1))
    for n in range(DEGREE + 1):
        c = np.polynomial.chebyshev.cheb2poly(np.eye(DEGREE + 1)[n])
        power[: len(c), n] = c
    return power @ fit


@functools.cache
def grid_matrix(depth, blocks):
    cells = BOX_CELLS * 2**depth
    ticks = TOP_TICKS // 2**depth
    step = ticks // LANES
    assert step * LANES == ticks and step % 2 == 0
    nodes = (np.arange(blocks)[:, None] * cells + node_offsets(cells)[None, :]).reshape(-1)
    centers = np.arange(LANES) * step + step // 2 - ticks // 2
    phase = np.exp(1j * turn64(centers[None, :], nodes[:, None]))
    off = (nodes - (blocks * cells - 1) / 2.0) * (step // 2) * (2.0 * np.pi / 2.0**32)
    poly = fit_turn(off)
    out = np.zeros((blocks, 2, R, DEGREE + 1, 2, LANES))
    for p in range(DEGREE + 1):
        b = (poly[p][:, None] * phase).reshape(blocks, R, LANES)
        out[:, 0, :, p, 0], out[:, 0, :, p, 1] = b.real, b.imag
        out[:, 1, :, p, 0], out[:, 1, :, p, 1] = -b.imag, b.real
    return out.reshape(blocks * 2 * R, (DEGREE + 1) * 2 * LANES)


def split_rows(m):
    hi = m.astype(jnp.bfloat16)
    lo = (m - hi.astype(np.float64)).astype(jnp.bfloat16)
    return jnp.asarray(np.concatenate([hi, hi, lo], axis=0))


def leaf_matrix():
    nodes = node_offsets(BOX_CELLS)
    angles = np.pi * (np.arange(R) + 0.5) / R
    at_exact = lagrange_values(2.0 * nodes / BOX_CELLS - 1.0, np.cos(angles))
    cheb_at = np.stack([np.cos(n * angles) for n in range(R)])
    norm = np.where(np.arange(R) == 0, 1.0, 2.0) / R
    g = (norm[:, None] * (cheb_at @ at_exact.T)).astype(np.float32)
    wide = np.repeat(g.T, 8, axis=1)
    zero = np.zeros_like(wide)
    return np.block([[wide, zero], [zero, wide]]).astype(np.float32)


def leaf_kernel(pos_ref, str_ref, mix_ref, out_ref, p_t, re_t, im_t, *, digits):
    def turn_over(beta, slot):
        rows = pl.ds(beta, LANES, stride=digits)
        p_t[slot] = pos_ref[rows, :].T
        re_t[slot] = str_ref[0, rows, :].T
        im_t[slot] = str_ref[1, rows, :].T

    def tile(beta, carry):
        slot = lax.rem(beta, 2)
        turn_over(jnp.minimum(beta + 1, digits - 1), 1 - slot)
        zero = jnp.zeros((8, LANES), jnp.float32)
        acc = tuple((zero, zero) for _ in range(R))
        for i in range(PER_BOX // 8):
            acc = chunk(slot, i, acc)
        low, high = list(acc[: R // 2]), list(acc[R // 2 :])
        top = [high[0]]
        for k in range(1, R // 2):
            top.append(tuple(2.0 * h - m for h, m in zip(high[k], low[R // 2 - k])))
        both = low + top
        stack = jnp.concatenate([x for x, _ in both] + [y for _, y in both], axis=0)
        out_ref[beta] = jnp.dot(mix_ref[...], stack, precision=HIGHEST, preferred_element_type=jnp.float32)
        return carry

    def chunk(slot, i, acc):
        here = pl.ds(i * 8, 8)
        r = p_t[slot, here, :] & (BOX_CELLS - 1)
        turn = (r * (TOP_TICKS // 2)).astype(jnp.float32) * (2.0**-32)
        c, s = cos_sin_turns(turn)
        a, b = re_t[slot, here, :], im_t[slot, here, :]
        v = r.astype(jnp.float32) * (2.0 / BOX_CELLS) - 1.0
        v2 = v + v
        cheb = [None, v]
        for k in range(2, R // 2 + 1):
            cheb.append(v2 * v - 1.0 if k == 2 else v2 * cheb[-1] - cheb[-2])
        x, y = c * a - s * b, s * a + c * b
        out = []
        for part, (x, y) in enumerate([(x, y), (cheb[-1] * x, cheb[-1] * y)]):
            for k in range(R // 2):
                u, w = acc[part * (R // 2) + k]
                out.append((u + x, w + y) if k == 0 else (u + cheb[k] * x, w + cheb[k] * y))
        return tuple(out)

    turn_over(0, 0)
    lax.fori_loop(0, digits, tile, 0)


def leaf_call(pos, strengths):
    boxes = pos.shape[0]
    digits = boxes // LANES
    whole = pl.BlockSpec(memory_space=pltpu.VMEM)
    return pl.pallas_call(
        functools.partial(leaf_kernel, digits=digits),
        out_shape=jax.ShapeDtypeStruct((digits, 2 * R, LANES), jnp.float32),
        in_specs=[whole, whole, whole],
        out_specs=whole,
        scratch_shapes=[
            pltpu.VMEM((2, LANES, LANES), jnp.int32),
            pltpu.VMEM((2, LANES, LANES), jnp.float32),
            pltpu.VMEM((2, LANES, LANES), jnp.float32),
        ],
        name="leaf",
    )(pos, strengths, jnp.asarray(leaf_matrix()))


def finish_kernel(w_ref, tgt_hbm, m_ref, a_hbm, out_hbm, tgt, out, a_buf, tab, bufs, got, coefs,
                  send, recv, gsend, grecv, tsem, asem, osem, *, leaves, blocks, chunks, depth, rows):
    leaf_no, blk_no = lax.axis_index("leaf"), lax.axis_index("blk")
    bits = leaves.bit_length() - 1
    boxes = w_ref.shape[1]
    width = boxes // chunks
    tiles = width // LANES
    cells = BOX_CELLS * 2**depth
    ticks = TOP_TICKS // 2**depth
    sides = [leaf_no // 2**k % 2 for k in range(bits)]
    partners = [leaf_no + (1 - 2 * sides[k]) * 2**k for k in range(bits)]
    suffix = jnp.int32(0)
    for k in range(bits):
        suffix = 2 * suffix + sides[k]
    peers = [lax.rem(blk_no + d, blocks) for d in range(1, blocks)]
    fetch = pltpu.make_async_copy(tgt_hbm, tgt, tsem)
    fetch.start()
    load = pltpu.make_async_copy(a_hbm, a_buf, asem)
    load.start()

    barrier = pltpu.get_barrier_semaphore()
    for k in range(bits):
        pl.semaphore_signal(barrier, inc=1, device_id=(partners[k], blk_no), device_id_type=pl.DeviceIdType.MESH)
    for peer in peers:
        pl.semaphore_signal(barrier, inc=1, device_id=(leaf_no, peer), device_id_type=pl.DeviceIdType.MESH)
    pl.semaphore_wait(barrier, bits + blocks - 1)

    def own(stage, c):
        return w_ref.at[:, pl.ds(c * width, width)] if stage == 0 else bufs.at[stage - 1, c]

    def exchange(stage, c):
        return pltpu.make_async_remote_copy(
            src_ref=own(stage, c), dst_ref=got.at[stage, c],
            send_sem=send.at[stage, c], recv_sem=recv.at[stage, c],
            device_id=(partners[stage], blk_no), device_id_type=pl.DeviceIdType.MESH,
        )

    def spread(d, c):
        here = coefs.at[blk_no, pl.ds(c * tiles, tiles)]
        return pltpu.make_async_remote_copy(
            src_ref=here, dst_ref=here,
            send_sem=gsend.at[d - 1, c], recv_sem=grecv.at[d - 1, c],
            device_id=(leaf_no, peers[d - 1]), device_id_type=pl.DeviceIdType.MESH,
        )

    def combine(todo):
        for stage, c in todo:
            exchange(stage, c).wait_recv()
        results = []
        for stage, c in todo:
            pair = jnp.concatenate([own(stage, c)[...], got[stage, c]], axis=0)
            results.append(mm(m_ref[stage, sides[stage]], pair))
        for (stage, c), w in zip(todo, results):
            if stage < bits - 1:
                bufs[stage, c] = w
            else:
                for i in range(tiles):
                    coefs[blk_no, c * tiles + i] = w[:, i * LANES : (i + 1) * LANES]
        for stage, c in todo:
            if stage < bits - 1:
                exchange(stage + 1, c).start()
            else:
                for d in range(1, blocks):
                    spread(d, c).start()

    pitch = ticks // LANES
    tilt = (blocks * cells - 1) / 2.0 * (pitch // 2) / 2.0**32
    cos_poly = fit_even(lambda y: np.cos(2 * np.pi * y), tilt, 3)
    sin_poly = fit_even(lambda y: np.sin(2 * np.pi * y) / y, tilt, 3)
    cos_poly = [c * tilt ** (2 * k) for k, c in enumerate(cos_poly)]
    sin_poly = [c * tilt ** (2 * k + 1) for k, c in enumerate(sin_poly)]
    below = lax.broadcasted_iota(jnp.int32, (rows, LANES), 0) * (leaves * ticks)

    def evaluate(tile, carry):
        whole = jnp.concatenate([coefs[q, tile] for q in range(blocks)], axis=0).T
        hi = whole.astype(jnp.bfloat16)
        lo = (whole - hi.astype(jnp.float32)).astype(jnp.bfloat16)
        lhs = jnp.concatenate([hi, lo, hi], axis=1)
        for n in range(2 * (DEGREE + 1)):
            tab[n] = jnp.dot(lhs, a_buf[:, n * LANES : (n + 1) * LANES], preferred_element_type=jnp.float32)
        first = pl.multiple_of(tile * LANES, LANES)
        for i in range(LANES // rows):
            base = ((first + i * rows) * leaves + suffix) * ticks
            u = (tgt[pl.ds(first + i * rows, rows), :] - (below + base)).astype(jnp.float32)
            cell = (u * (1.0 / pitch) + (0.5 / pitch)).astype(jnp.int32)
            s = (u - cell.astype(jnp.float32) * pitch) * (2.0 / pitch) - 1.0
            got_at = [jnp.take_along_axis(tab[n, i * rows : (i + 1) * rows, :], cell, axis=1)
                      for n in range(2 * (DEGREE + 1))]
            re, im = got_at[-2], got_at[-1]
            for p in range(DEGREE - 1, -1, -1):
                re, im = re * s + got_at[2 * p], im * s + got_at[2 * p + 1]
            z = s * s
            pc, ps = horner(cos_poly, z), s * horner(sin_poly, z)
            out[pl.ds(2 * (first + i * rows), rows, stride=2), :] = pc * re - ps * im
            out[pl.ds(2 * (first + i * rows) + 1, rows, stride=2), :] = pc * im + ps * re
        return carry

    def put(c):
        span = pl.ds(2 * c * width, 2 * width)
        return pltpu.make_async_copy(out.at[span], out_hbm.at[span], osem.at[c])

    def field(c):
        if c == 0:
            fetch.wait()
            load.wait()
        for d in range(1, blocks):
            spread(d, c).wait_recv()
        lax.fori_loop(c * tiles, (c + 1) * tiles, evaluate, 0)
        put(c).start()

    ahead = min(3, chunks)
    for c in range(ahead):
        exchange(0, c).start()
    for step in range(chunks + bits):
        combine([(k, step - k) for k in range(bits - 1, -1, -1) if 0 <= step - k < chunks])
        if step + ahead < chunks:
            exchange(0, step + ahead).start()
        if step >= bits:
            field(step - bits)
    for c in range(chunks):
        for stage in range(bits):
            exchange(stage, c).wait_send()
        for d in range(1, blocks):
            spread(d, c).wait_send()
        put(c).wait()


def finish_call(weights, ticks, matrices, grid, leaves, blocks, depth, chunks):
    boxes = ticks.shape[0]
    bits = leaves.bit_length() - 1
    width = boxes // chunks
    whole = pl.BlockSpec(memory_space=pltpu.VMEM)
    anywhere = pl.BlockSpec(memory_space=pl.ANY)
    dma = pltpu.SemaphoreType.DMA
    return pl.pallas_call(
        functools.partial(finish_kernel, leaves=leaves, blocks=blocks, chunks=chunks, depth=depth, rows=8),
        out_shape=jax.ShapeDtypeStruct((2 * boxes, TGT_BOX), jnp.float32),
        in_specs=[whole, anywhere, whole, anywhere],
        out_specs=anywhere,
        scratch_shapes=[
            pltpu.VMEM((boxes, TGT_BOX), jnp.int32),
            pltpu.VMEM((2 * boxes, TGT_BOX), jnp.float32),
            pltpu.VMEM(grid.shape, jnp.bfloat16),
            pltpu.VMEM((2 * (DEGREE + 1), LANES, LANES), jnp.float32),
            pltpu.VMEM((bits - 1, chunks, 2 * R, width), jnp.float32),
            pltpu.VMEM((bits, chunks, 2 * R, width), jnp.float32),
            pltpu.VMEM((blocks, boxes // LANES, 2 * R, LANES), jnp.float32),
        ] + [
            dma((bits, chunks)), dma((bits, chunks)),
            dma((blocks - 1, chunks)), dma((blocks - 1, chunks)),
            dma, dma, dma((chunks,)),
        ],
        compiler_params=pltpu.CompilerParams(collective_id=0, has_side_effects=True),
        name="finish",
    )(weights, ticks, matrices, grid)


def table(m):
    return jnp.asarray(m.astype(np.float32))


def mm(a, b):
    return jnp.dot(a, b, precision=HIGHEST, preferred_element_type=jnp.float32)


def local_tree(leaf, boxes):
    low = leaf.shape[0]
    n1 = low.bit_length() - 1
    rest = boxes.bit_length() - 1 - n1
    n2 = rest - rest // 2
    n3 = rest - n2
    c = 2 * R
    y = mm(table(radix_matrix(0, n1)), leaf.reshape(low * c, -1))
    y = y.reshape(low, c, 2**n3, 2**n2).transpose(3, 1, 0, 2).reshape(2**n2 * c, -1)
    y = mm(table(radix_matrix(n1, n2)), y)
    y = y.reshape(2**n2, c, low, 2**n3).transpose(3, 1, 2, 0).reshape(2**n3 * c, -1)
    y = mm(table(radix_matrix(n1 + n2, n3)), y)
    return y.reshape(2**n3, c, low * 2**n2).transpose(1, 2, 0).reshape(c, boxes)


def local_butterfly(src_pos, strengths, tgt_pos):
    leaf_count = lax.axis_size("leaf")
    leaf_bits = leaf_count.bit_length() - 1
    boxes = src_pos.shape[1] // PER_BOX
    local_depth = boxes.bit_length() - 1
    leaf = leaf_call(src_pos.reshape(boxes, PER_BOX), strengths.reshape(2, boxes, PER_BOX))
    weights = local_tree(leaf, boxes)
    steps = np.stack([step_matrix(local_depth + k) for k in range(leaf_bits)])
    steps[:, 1] = steps[:, 1, ::-1]
    steps = np.concatenate([steps[:, :, 0], steps[:, :, 1]], axis=-1)
    out = finish_call(
        weights, tgt_pos.reshape(boxes, TGT_BOX), table(steps),
        split_rows(grid_matrix(local_depth + leaf_bits, lax.axis_size("blk"))), leaf_count, lax.axis_size("blk"),
        local_depth + leaf_bits, 8,
    )
    return out.reshape(boxes, 2, TGT_BOX).transpose(1, 0, 2).reshape(2, boxes * TGT_BOX)


def xor(a, d, bits):
    return sum(((a // 2**k % 2 + (d >> k) % 2) % 2) * 2**k for k in range(bits))


def reverse_bits(a, bits):
    return sum((a // 2**k % 2) * 2 ** (bits - 1 - k) for k in range(bits))


def split_pair(x):
    hi = x.astype(jnp.bfloat16)
    return hi, (x - hi.astype(jnp.float32)).astype(jnp.bfloat16)


def dot16(a, b):
    return jnp.dot(a, b, preferred_element_type=jnp.float32)


def far_first(leaves):
    half = leaves // 2
    return [1] + list(range(half, leaves)) + list(range(2, half)) if leaves > 2 else [1]


def up_kernel(pos_ref, str_ref, mix_ref, w_hbm, out_ref, p_t, re_t, im_t, stack, w_buf, y, got,
              send, recv, wsem, *, digits, leaves):
    me, blk_no = lax.axis_index("leaf"), lax.axis_index("blk")
    bits = leaves.bit_length() - 1
    load = pltpu.make_async_copy(w_hbm, w_buf, wsem)
    load.start()
    barrier = pltpu.get_barrier_semaphore()
    for d in range(1, leaves):
        pl.semaphore_signal(barrier, inc=1, device_id=(xor(me, d, bits), blk_no), device_id_type=pl.DeviceIdType.MESH)
    leaf_kernel(pos_ref, str_ref, mix_ref, stack, p_t, re_t, im_t, digits=digits)
    hi, lo = split_pair(stack[...].reshape(digits * 2 * R, LANES))
    load.wait()
    y[...] = (dot16(w_buf[0], hi) + dot16(w_buf[0], lo) + dot16(w_buf[1], hi)).reshape(y.shape)
    pl.semaphore_wait(barrier, leaves - 1)

    def ship(d):
        peer = xor(me, d, bits)
        return pltpu.make_async_remote_copy(
            src_ref=y.at[peer], dst_ref=got.at[me],
            send_sem=send.at[d - 1], recv_sem=recv.at[d - 1],
            device_id=(peer, blk_no), device_id_type=pl.DeviceIdType.MESH,
        )

    for d in far_first(leaves):
        ship(d).start()
    out_ref[me] = y[me]
    for d in far_first(leaves):
        ship(d).wait_recv()
        peer = xor(me, d, bits)
        out_ref[peer] = got[peer]
    for d in far_first(leaves):
        ship(d).wait_send()


def up_call(pos, strengths, leaves):
    boxes = pos.shape[0]
    digits = boxes // LANES
    whole = pl.BlockSpec(memory_space=pltpu.VMEM)
    anywhere = pl.BlockSpec(memory_space=pl.ANY)
    dma = pltpu.SemaphoreType.DMA
    n = digits * 2 * R
    part = (leaves, n // leaves, LANES)
    return pl.pallas_call(
        functools.partial(up_kernel, digits=digits, leaves=leaves),
        out_shape=jax.ShapeDtypeStruct(part, jnp.float32),
        in_specs=[whole, whole, whole, anywhere],
        out_specs=whole,
        scratch_shapes=[
            pltpu.VMEM((2, LANES, LANES), jnp.int32),
            pltpu.VMEM((2, LANES, LANES), jnp.float32),
            pltpu.VMEM((2, LANES, LANES), jnp.float32),
            pltpu.VMEM((digits, 2 * R, LANES), jnp.float32),
            pltpu.VMEM((2, n, n), jnp.bfloat16),
            pltpu.VMEM(part, jnp.float32),
            pltpu.VMEM(part, jnp.float32),
            dma((leaves - 1,)), dma((leaves - 1,)), dma,
        ],
        compiler_params=pltpu.CompilerParams(collective_id=0, has_side_effects=True),
        name="up",
    )(pos, strengths, jnp.asarray(leaf_matrix()), two_parts(radix_matrix(0, digits.bit_length() - 1)))


def two_parts(m):
    hi = m.astype(jnp.bfloat16)
    return jnp.asarray(np.stack([hi, (m - hi.astype(np.float64)).astype(jnp.bfloat16)]))


def middle_tree(part, leaves, digits, boxes):
    c = 2 * R
    bits = leaves.bit_length() - 1
    first = digits.bit_length() - 1
    total = boxes.bit_length() - 1 + bits
    high = LANES.bit_length() - 1
    n2 = high - high // 2
    n3 = high - n2
    own = digits // leaves
    x = part.reshape(leaves, own, c, 2**n3, 2**n2)
    x = x.transpose(4, 2, 0, 1, 3).reshape(2**n2 * c, -1)
    x = mm(table(radix_matrix(first, n2)), x)
    x = x.reshape(2**n2, c, leaves, own, 2**n3).transpose(4, 1, 2, 3, 0).reshape(2**n3 * c, -1)
    x = mm(table(radix_matrix(first + n2, n3)), x)
    x = x.reshape(2**n3, c, leaves, own * 2**n2).transpose(2, 1, 3, 0).reshape(leaves * c, -1)
    x = mm(table(radix_matrix(total - bits, bits)), x)
    return x.reshape(leaves, c, -1)


def down_kernel(w_ref, tgt_hbm, a_hbm, out_hbm, tgt, out, a_buf, tab, coefs,
                send, recv, gsend, grecv, tsem, asem, osem, *, leaves, blocks, depth, rows):
    me, blk_no = lax.axis_index("leaf"), lax.axis_index("blk")
    bits = leaves.bit_length() - 1
    width = w_ref.shape[2]
    tiles = width // LANES
    cells = BOX_CELLS * 2**depth
    ticks = TOP_TICKS // 2**depth
    suffix = reverse_bits(me, bits)
    across = lax.rem(blk_no + blocks // 2, blocks)
    beside = blk_no + 1 - 2 * (blk_no % 2)
    fetch = pltpu.make_async_copy(tgt_hbm, tgt, tsem)
    load = pltpu.make_async_copy(a_hbm, a_buf, asem)
    load.start()
    fetch.start()

    barrier = pltpu.get_barrier_semaphore()
    for d in range(1, leaves):
        pl.semaphore_signal(barrier, inc=1, device_id=(xor(me, d, bits), blk_no), device_id_type=pl.DeviceIdType.MESH)
    for peer in (across, beside):
        pl.semaphore_signal(barrier, inc=1, device_id=(me, peer), device_id_type=pl.DeviceIdType.MESH)
    pl.semaphore_wait(barrier, leaves + 1)

    def ship(d):
        peer = xor(me, d, bits)
        return pltpu.make_async_remote_copy(
            src_ref=w_ref.at[reverse_bits(peer, bits)], dst_ref=coefs.at[blk_no, me],
            send_sem=send.at[d - 1], recv_sem=recv.at[d - 1],
            device_id=(peer, blk_no), device_id_type=pl.DeviceIdType.MESH,
        )

    def spread(way, d):
        here = coefs.at[across if way == 2 else blk_no, xor(me, d, bits)]
        return pltpu.make_async_remote_copy(
            src_ref=here, dst_ref=here,
            send_sem=gsend.at[way, d], recv_sem=grecv.at[way, d],
            device_id=(me, across if way == 0 else beside), device_id_type=pl.DeviceIdType.MESH,
        )

    pitch = ticks // LANES
    tilt = (blocks * cells - 1) / 2.0 * (pitch // 2) / 2.0**32
    cos_poly = fit_even(lambda y: np.cos(2 * np.pi * y), tilt, 3)
    sin_poly = fit_even(lambda y: np.sin(2 * np.pi * y) / y, tilt, 3)
    cos_poly = [c * tilt ** (2 * k) for k, c in enumerate(cos_poly)]
    sin_poly = [c * tilt ** (2 * k + 1) for k, c in enumerate(sin_poly)]
    below = lax.broadcasted_iota(jnp.int32, (rows, LANES), 0) * (leaves * ticks)

    def evaluate(chunk, t):
        pack = jnp.concatenate([coefs[q, chunk, :, t * LANES : (t + 1) * LANES] for q in range(blocks)], axis=0)
        hi, lo = split_pair(pack.T)
        lhs = jnp.concatenate([hi, lo, hi], axis=1)
        for n in range(2 * (DEGREE + 1)):
            tab[t, n] = dot16(lhs, a_buf[:, n * LANES : (n + 1) * LANES])
        first = pl.multiple_of(chunk * width + t * LANES, LANES)
        for i in range(LANES // rows):
            base = ((first + i * rows) * leaves + suffix) * ticks
            u = (tgt[pl.ds(first + i * rows, rows), :] - (below + base)).astype(jnp.float32)
            cell = (u * (1.0 / pitch) + (0.5 / pitch)).astype(jnp.int32)
            s = (u - cell.astype(jnp.float32) * pitch) * (2.0 / pitch) - 1.0
            got_at = [jnp.take_along_axis(tab[t, n, i * rows : (i + 1) * rows, :], cell, axis=1)
                      for n in range(2 * (DEGREE + 1))]
            z = s * s
            powers = [None, s, z, z * s, z * z]
            re, im = [[got_at[2 * p + part] * powers[p] if p else got_at[part] for p in range(DEGREE + 1)]
                      for part in range(2)]
            re = (re[0] + re[1]) + (re[2] + re[3]) + re[4]
            im = (im[0] + im[1]) + (im[2] + im[3]) + im[4]
            pc, ps = horner(cos_poly, z), s * horner(sin_poly, z)
            out[pl.ds(2 * (first + i * rows), rows, stride=2), :] = pc * re - ps * im
            out[pl.ds(2 * (first + i * rows) + 1, rows, stride=2), :] = pc * im + ps * re

    def put(d):
        span = pl.ds(pl.multiple_of(xor(me, d, bits) * (2 * width), 2 * width), 2 * width)
        return pltpu.make_async_copy(out.at[span], out_hbm.at[span], osem.at[d])

    order = [0] + far_first(leaves)
    for d in order[1:]:
        ship(d).start()
    coefs[blk_no, me] = w_ref[suffix]
    for step in range(leaves + 4):
        if step < leaves:
            d = order[step]
            if d:
                ship(d).wait_recv()
            spread(0, d).start()
            spread(1, d).start()
        if 0 <= step - 4:
            d = order[step - 4]
            if step == 4:
                load.wait()
                fetch.wait()
            spread(1, d).wait_recv()
            spread(2, d).wait_recv()
            for t in range(tiles):
                evaluate(xor(me, d, bits), t)
            put(d).start()
        if 0 <= step - 2 < leaves:
            d = order[step - 2]
            spread(0, d).wait_recv()
            spread(2, d).start()
    for d in order:
        if d:
            ship(d).wait_send()
        for way in range(3):
            spread(way, d).wait_send()
        put(d).wait()


def down_call(weights, ticks, grid, leaves, blocks, depth):
    boxes = ticks.shape[0]
    width = boxes // leaves
    whole = pl.BlockSpec(memory_space=pltpu.VMEM)
    anywhere = pl.BlockSpec(memory_space=pl.ANY)
    dma = pltpu.SemaphoreType.DMA
    return pl.pallas_call(
        functools.partial(down_kernel, leaves=leaves, blocks=blocks, depth=depth, rows=8),
        out_shape=jax.ShapeDtypeStruct((2 * boxes, TGT_BOX), jnp.float32),
        in_specs=[whole, anywhere, anywhere],
        out_specs=anywhere,
        scratch_shapes=[
            pltpu.VMEM((boxes, TGT_BOX), jnp.int32),
            pltpu.VMEM((2 * boxes, TGT_BOX), jnp.float32),
            pltpu.VMEM(grid.shape, jnp.bfloat16),
            pltpu.VMEM((width // LANES, 2 * (DEGREE + 1), LANES, LANES), jnp.float32),
            pltpu.VMEM((blocks, leaves, 2 * R, width), jnp.float32),
            dma((leaves - 1,)), dma((leaves - 1,)), dma((3, leaves)), dma((3, leaves)),
            dma, dma, dma((leaves,)),
        ],
        compiler_params=pltpu.CompilerParams(collective_id=1, has_side_effects=True),
        name="down",
    )(weights, ticks, grid)


def local_two_shuffles(src_pos, strengths, tgt_pos):
    leaves, blocks = lax.axis_size("leaf"), lax.axis_size("blk")
    boxes = src_pos.shape[1] // PER_BOX
    depth = boxes.bit_length() - 1 + leaves.bit_length() - 1
    part = up_call(src_pos.reshape(boxes, PER_BOX), strengths.reshape(2, boxes, PER_BOX), leaves)
    weights = middle_tree(part, leaves, boxes // LANES, boxes)
    grid = split_rows(grid_matrix(depth, blocks))
    out = down_call(weights, tgt_pos.reshape(boxes, TGT_BOX), grid, leaves, blocks, depth)
    return out.reshape(boxes, 2, TGT_BOX).transpose(1, 0, 2).reshape(2, boxes * TGT_BOX)


def solution(mesh):
    def local(src_pos, strengths, tgt_pos):
        boxes = src_pos.shape[1] // PER_BOX
        near = mesh.shape["leaf"] * LANES <= boxes and mesh.shape["blk"] == 4
        run = local_two_shuffles if near else local_butterfly
        return run(src_pos, strengths, tgt_pos)

    return jax.shard_map(
        local,
        mesh=mesh,
        in_specs=(P("blk", "leaf"), P(None, "blk", "leaf"), P(("leaf", "blk"))),
        out_specs=P(None, ("leaf", "blk")),
        check_vma=False,
    )
```

```python
import functools
import math

import jax
import jax.numpy as jnp
import numpy as np
from jax import lax
from jax.experimental import pallas as pl
from jax.experimental.pallas import tpu as pltpu
from jax.sharding import PartitionSpec as P

R = 16
PER_BOX = 128
TGT_BOX = 128
BOX_CELLS = 128
TOP_TICKS = 201326592
LANES = 128
HIGHEST = lax.Precision.HIGHEST


def fit_even(values, span, count):
    u = 0.5 * span * span * (1.0 + np.cos(np.pi * (np.arange(400) + 0.5) / 400))
    cheb = np.polynomial.chebyshev.Chebyshev.fit(u, values(np.sqrt(u)), count - 1, domain=[0, span * span])
    return [float(c) for c in cheb.convert(kind=np.polynomial.Polynomial).coef]


COS_POLY = fit_even(lambda y: np.cos(np.pi * y), 0.5, 5)
SIN_POLY = fit_even(lambda y: np.sin(np.pi * y) / y, 0.5, 4)


def horner(coefs, u):
    out = u * coefs[-1] + coefs[-2]
    for c in coefs[-3::-1]:
        out = out * u + c
    return out


def cos_sin_turns(y):
    u = y * y
    c, s = horner(COS_POLY, u), y * horner(SIN_POLY, u)
    twice = s + s
    return 1.0 - twice * s, twice * c


def node_offsets(box_cells):
    node_index = np.arange(R)
    unit_nodes = (1.0 - np.cos(np.pi * (node_index + 0.5) / R)) / 2.0
    return np.floor(box_cells * unit_nodes).astype(np.int64)


def lagrange_values(node_pos, points):
    rows = []
    for row_node in range(node_pos.shape[0]):
        column = np.ones(points.shape[0])
        for other in range(node_pos.shape[0]):
            if other != row_node:
                column = column * (points - node_pos[other]) / (node_pos[row_node] - node_pos[other])
        rows.append(column)
    return np.stack(rows)


def as_real(m):
    return np.block([[m.real, -m.imag], [m.imag, m.real]])


def turn64(a, b):
    product = (a * b + 2**31) % 2**32 - 2**31
    return product * (2.0 * np.pi / 2.0**32)


@functools.cache
def step_matrix(level):
    cells = BOX_CELLS * 2**level
    child, parent = node_offsets(cells), node_offsets(2 * cells)
    inner = np.concatenate([child, child + cells])
    blend = lagrange_values(parent / (2.0 * cells), inner / (2.0 * cells)).reshape(R, 2, R)
    half = TOP_TICKS // 2 ** (level + 2)
    assert half * cells % 2**32 == 2**31
    out = np.zeros((2, 2, 2 * R, 2 * R))
    for e in range(2):
        phase = np.exp(1j * turn64(half if e else -half, child))
        for j in range(2):
            out[e, j] = as_real((-1.0) ** j * blend[:, j, :] * phase[None, :])
    return out


def radix_matrix(first, count):
    total = np.eye(2 * R)[None, None]
    for k in range(count):
        m = step_matrix(first + k)
        n = total.shape[0]
        new = np.zeros((2 * n, 2 * n, 2 * R, 2 * R))
        for a in range(n):
            for b in range(n):
                for e in range(2):
                    for j in range(2):
                        new[2 * a + e, b + j * n] = m[e, j] @ total[a, b]
        total = new
    n = total.shape[0]
    return total.transpose(0, 2, 1, 3).reshape(n * 2 * R, n * 2 * R)


DEGREE = 4


def fit_turn(theta):
    s = np.cos(np.pi * (np.arange(64) + 0.5) / 64)
    fit = np.polynomial.chebyshev.chebfit(s, np.exp(1j * s[:, None] * theta[None, :]), DEGREE)
    power = np.zeros((DEGREE + 1, DEGREE + 1))
    for n in range(DEGREE + 1):
        c = np.polynomial.chebyshev.cheb2poly(np.eye(DEGREE + 1)[n])
        power[: len(c), n] = c
    return power @ fit


@functools.cache
def grid_matrix(depth, blocks):
    cells = BOX_CELLS * 2**depth
    ticks = TOP_TICKS // 2**depth
    step = ticks // LANES
    assert step * LANES == ticks and step % 2 == 0
    nodes = (np.arange(blocks)[:, None] * cells + node_offsets(cells)[None, :]).reshape(-1)
    centers = np.arange(LANES) * step + step // 2 - ticks // 2
    phase = np.exp(1j * turn64(centers[None, :], nodes[:, None]))
    off = (nodes - (blocks * cells - 1) / 2.0) * (step // 2) * (2.0 * np.pi / 2.0**32)
    poly = fit_turn(off)
    out = np.zeros((blocks, 2, R, DEGREE + 1, 2, LANES))
    for p in range(DEGREE + 1):
        b = (poly[p][:, None] * phase).reshape(blocks, R, LANES)
        out[:, 0, :, p, 0], out[:, 0, :, p, 1] = b.real, b.imag
        out[:, 1, :, p, 0], out[:, 1, :, p, 1] = -b.imag, b.real
    return out.reshape(blocks * 2 * R, (DEGREE + 1) * 2 * LANES)


def split_rows(m):
    hi = m.astype(jnp.bfloat16)
    lo = (m - hi.astype(np.float64)).astype(jnp.bfloat16)
    return jnp.asarray(np.concatenate([hi, hi, lo], axis=0))


def leaf_matrix():
    nodes = node_offsets(BOX_CELLS)
    angles = np.pi * (np.arange(R) + 0.5) / R
    at_exact = lagrange_values(2.0 * nodes / BOX_CELLS - 1.0, np.cos(angles))
    cheb_at = np.stack([np.cos(n * angles) for n in range(R)])
    norm = np.where(np.arange(R) == 0, 1.0, 2.0) / R
    g = (norm[:, None] * (cheb_at @ at_exact.T)).astype(np.float32)
    wide = np.repeat(g.T, 8, axis=1)
    zero = np.zeros_like(wide)
    return np.block([[wide, zero], [zero, wide]]).astype(np.float32)


def leaf_kernel(pos_ref, str_ref, mix_ref, out_ref, p_t, re_t, im_t, *, digits):
    def turn_over(beta, slot):
        rows = pl.ds(beta, LANES, stride=digits)
        p_t[slot] = pos_ref[rows, :].T
        re_t[slot] = str_ref[0, rows, :].T
        im_t[slot] = str_ref[1, rows, :].T

    def tile(beta, carry):
        slot = lax.rem(beta, 2)
        turn_over(jnp.minimum(beta + 1, digits - 1), 1 - slot)
        zero = jnp.zeros((8, LANES), jnp.float32)
        acc = tuple((zero, zero) for _ in range(R))
        for i in range(PER_BOX // 8):
            acc = chunk(slot, i, acc)
        low, high = list(acc[: R // 2]), list(acc[R // 2 :])
        top = [high[0]]
        for k in range(1, R // 2):
            top.append(tuple(2.0 * h - m for h, m in zip(high[k], low[R // 2 - k])))
        both = low + top
        stack = jnp.concatenate([x for x, _ in both] + [y for _, y in both], axis=0)
        out_ref[beta] = jnp.dot(mix_ref[...], stack, precision=HIGHEST, preferred_element_type=jnp.float32)
        return carry

    def chunk(slot, i, acc):
        here = pl.ds(i * 8, 8)
        r = p_t[slot, here, :] & (BOX_CELLS - 1)
        turn = (r * (TOP_TICKS // 2)).astype(jnp.float32) * (2.0**-32)
        c, s = cos_sin_turns(turn)
        a, b = re_t[slot, here, :], im_t[slot, here, :]
        v = r.astype(jnp.float32) * (2.0 / BOX_CELLS) - 1.0
        v2 = v + v
        cheb = [None, v]
        for k in range(2, R // 2 + 1):
            cheb.append(v2 * v - 1.0 if k == 2 else v2 * cheb[-1] - cheb[-2])
        x, y = c * a - s * b, s * a + c * b
        out = []
        for part, (x, y) in enumerate([(x, y), (cheb[-1] * x, cheb[-1] * y)]):
            for k in range(R // 2):
                u, w = acc[part * (R // 2) + k]
                out.append((u + x, w + y) if k == 0 else (u + cheb[k] * x, w + cheb[k] * y))
        return tuple(out)

    turn_over(0, 0)
    lax.fori_loop(0, digits, tile, 0)


def leaf_call(pos, strengths):
    boxes = pos.shape[0]
    digits = boxes // LANES
    whole = pl.BlockSpec(memory_space=pltpu.VMEM)
    return pl.pallas_call(
        functools.partial(leaf_kernel, digits=digits),
        out_shape=jax.ShapeDtypeStruct((digits, 2 * R, LANES), jnp.float32),
        in_specs=[whole, whole, whole],
        out_specs=whole,
        scratch_shapes=[
            pltpu.VMEM((2, LANES, LANES), jnp.int32),
            pltpu.VMEM((2, LANES, LANES), jnp.float32),
            pltpu.VMEM((2, LANES, LANES), jnp.float32),
        ],
        name="leaf",
    )(pos, strengths, jnp.asarray(leaf_matrix()))


def finish_kernel(w_ref, tgt_hbm, m_ref, a_hbm, out_hbm, tgt, out, a_buf, tab, bufs, got, coefs,
                  send, recv, gsend, grecv, tsem, asem, osem, *, leaves, blocks, chunks, depth, rows):
    leaf_no, blk_no = lax.axis_index("leaf"), lax.axis_index("blk")
    bits = leaves.bit_length() - 1
    boxes = w_ref.shape[1]
    width = boxes // chunks
    tiles = width // LANES
    cells = BOX_CELLS * 2**depth
    ticks = TOP_TICKS // 2**depth
    sides = [leaf_no // 2**k % 2 for k in range(bits)]
    partners = [leaf_no + (1 - 2 * sides[k]) * 2**k for k in range(bits)]
    suffix = jnp.int32(0)
    for k in range(bits):
        suffix = 2 * suffix + sides[k]
    peers = [lax.rem(blk_no + d, blocks) for d in range(1, blocks)]
    fetch = pltpu.make_async_copy(tgt_hbm, tgt, tsem)
    fetch.start()
    load = pltpu.make_async_copy(a_hbm, a_buf, asem)
    load.start()

    barrier = pltpu.get_barrier_semaphore()
    for k in range(bits):
        pl.semaphore_signal(barrier, inc=1, device_id=(partners[k], blk_no), device_id_type=pl.DeviceIdType.MESH)
    for peer in peers:
        pl.semaphore_signal(barrier, inc=1, device_id=(leaf_no, peer), device_id_type=pl.DeviceIdType.MESH)
    pl.semaphore_wait(barrier, bits + blocks - 1)

    def own(stage, c):
        return w_ref.at[:, pl.ds(c * width, width)] if stage == 0 else bufs.at[stage - 1, c]

    def exchange(stage, c):
        return pltpu.make_async_remote_copy(
            src_ref=own(stage, c), dst_ref=got.at[stage, c],
            send_sem=send.at[stage, c], recv_sem=recv.at[stage, c],
            device_id=(partners[stage], blk_no), device_id_type=pl.DeviceIdType.MESH,
        )

    def spread(d, c):
        here = coefs.at[blk_no, pl.ds(c * tiles, tiles)]
        return pltpu.make_async_remote_copy(
            src_ref=here, dst_ref=here,
            send_sem=gsend.at[d - 1, c], recv_sem=grecv.at[d - 1, c],
            device_id=(leaf_no, peers[d - 1]), device_id_type=pl.DeviceIdType.MESH,
        )

    def combine(todo):
        for stage, c in todo:
            exchange(stage, c).wait_recv()
        results = []
        for stage, c in todo:
            pair = jnp.concatenate([own(stage, c)[...], got[stage, c]], axis=0)
            results.append(mm(m_ref[stage, sides[stage]], pair))
        for (stage, c), w in zip(todo, results):
            if stage < bits - 1:
                bufs[stage, c] = w
            else:
                for i in range(tiles):
                    coefs[blk_no, c * tiles + i] = w[:, i * LANES : (i + 1) * LANES]
        for stage, c in todo:
            if stage < bits - 1:
                exchange(stage + 1, c).start()
            else:
                for d in range(1, blocks):
                    spread(d, c).start()

    pitch = ticks // LANES
    tilt = (blocks * cells - 1) / 2.0 * (pitch // 2) / 2.0**32
    cos_poly = fit_even(lambda y: np.cos(2 * np.pi * y), tilt, 3)
    sin_poly = fit_even(lambda y: np.sin(2 * np.pi * y) / y, tilt, 3)
    cos_poly = [c * tilt ** (2 * k) for k, c in enumerate(cos_poly)]
    sin_poly = [c * tilt ** (2 * k + 1) for k, c in enumerate(sin_poly)]
    below = lax.broadcasted_iota(jnp.int32, (rows, LANES), 0) * (leaves * ticks)

    def evaluate(tile, carry):
        whole = jnp.concatenate([coefs[q, tile] for q in range(blocks)], axis=0).T
        hi = whole.astype(jnp.bfloat16)
        lo = (whole - hi.astype(jnp.float32)).astype(jnp.bfloat16)
        lhs = jnp.concatenate([hi, lo, hi], axis=1)
        for n in range(2 * (DEGREE + 1)):
            tab[n] = jnp.dot(lhs, a_buf[:, n * LANES : (n + 1) * LANES], preferred_element_type=jnp.float32)
        first = pl.multiple_of(tile * LANES, LANES)
        for i in range(LANES // rows):
            base = ((first + i * rows) * leaves + suffix) * ticks
            u = (tgt[pl.ds(first + i * rows, rows), :] - (below + base)).astype(jnp.float32)
            cell = (u * (1.0 / pitch) + (0.5 / pitch)).astype(jnp.int32)
            s = (u - cell.astype(jnp.float32) * pitch) * (2.0 / pitch) - 1.0
            got_at = [jnp.take_along_axis(tab[n, i * rows : (i + 1) * rows, :], cell, axis=1)
                      for n in range(2 * (DEGREE + 1))]
            re, im = got_at[-2], got_at[-1]
            for p in range(DEGREE - 1, -1, -1):
                re, im = re * s + got_at[2 * p], im * s + got_at[2 * p + 1]
            z = s * s
            pc, ps = horner(cos_poly, z), s * horner(sin_poly, z)
            out[pl.ds(2 * (first + i * rows), rows, stride=2), :] = pc * re - ps * im
            out[pl.ds(2 * (first + i * rows) + 1, rows, stride=2), :] = pc * im + ps * re
        return carry

    def put(c):
        span = pl.ds(2 * c * width, 2 * width)
        return pltpu.make_async_copy(out.at[span], out_hbm.at[span], osem.at[c])

    def field(c):
        if c == 0:
            fetch.wait()
            load.wait()
        for d in range(1, blocks):
            spread(d, c).wait_recv()
        lax.fori_loop(c * tiles, (c + 1) * tiles, evaluate, 0)
        put(c).start()

    ahead = min(3, chunks)
    for c in range(ahead):
        exchange(0, c).start()
    for step in range(chunks + bits):
        combine([(k, step - k) for k in range(bits - 1, -1, -1) if 0 <= step - k < chunks])
        if step + ahead < chunks:
            exchange(0, step + ahead).start()
        if step >= bits:
            field(step - bits)
    for c in range(chunks):
        for stage in range(bits):
            exchange(stage, c).wait_send()
        for d in range(1, blocks):
            spread(d, c).wait_send()
        put(c).wait()


def finish_call(weights, ticks, matrices, grid, leaves, blocks, depth, chunks):
    boxes = ticks.shape[0]
    bits = leaves.bit_length() - 1
    width = boxes // chunks
    whole = pl.BlockSpec(memory_space=pltpu.VMEM)
    anywhere = pl.BlockSpec(memory_space=pl.ANY)
    dma = pltpu.SemaphoreType.DMA
    return pl.pallas_call(
        functools.partial(finish_kernel, leaves=leaves, blocks=blocks, chunks=chunks, depth=depth, rows=8),
        out_shape=jax.ShapeDtypeStruct((2 * boxes, TGT_BOX), jnp.float32),
        in_specs=[whole, anywhere, whole, anywhere],
        out_specs=anywhere,
        scratch_shapes=[
            pltpu.VMEM((boxes, TGT_BOX), jnp.int32),
            pltpu.VMEM((2 * boxes, TGT_BOX), jnp.float32),
            pltpu.VMEM(grid.shape, jnp.bfloat16),
            pltpu.VMEM((2 * (DEGREE + 1), LANES, LANES), jnp.float32),
            pltpu.VMEM((bits - 1, chunks, 2 * R, width), jnp.float32),
            pltpu.VMEM((bits, chunks, 2 * R, width), jnp.float32),
            pltpu.VMEM((blocks, boxes // LANES, 2 * R, LANES), jnp.float32),
        ] + [
            dma((bits, chunks)), dma((bits, chunks)),
            dma((blocks - 1, chunks)), dma((blocks - 1, chunks)),
            dma, dma, dma((chunks,)),
        ],
        compiler_params=pltpu.CompilerParams(collective_id=0, has_side_effects=True),
        name="finish",
    )(weights, ticks, matrices, grid)


def table(m):
    return jnp.asarray(m.astype(np.float32))


def mm(a, b):
    return jnp.dot(a, b, precision=HIGHEST, preferred_element_type=jnp.float32)


def local_tree(leaf, boxes):
    low = leaf.shape[0]
    n1 = low.bit_length() - 1
    rest = boxes.bit_length() - 1 - n1
    n2 = rest - rest // 2
    n3 = rest - n2
    c = 2 * R
    y = mm(table(radix_matrix(0, n1)), leaf.reshape(low * c, -1))
    y = y.reshape(low, c, 2**n3, 2**n2).transpose(3, 1, 0, 2).reshape(2**n2 * c, -1)
    y = mm(table(radix_matrix(n1, n2)), y)
    y = y.reshape(2**n2, c, low, 2**n3).transpose(3, 1, 2, 0).reshape(2**n3 * c, -1)
    y = mm(table(radix_matrix(n1 + n2, n3)), y)
    return y.reshape(2**n3, c, low * 2**n2).transpose(1, 2, 0).reshape(c, boxes)


def local_butterfly(src_pos, strengths, tgt_pos):
    leaf_count = lax.axis_size("leaf")
    leaf_bits = leaf_count.bit_length() - 1
    boxes = src_pos.shape[1] // PER_BOX
    local_depth = boxes.bit_length() - 1
    leaf = leaf_call(src_pos.reshape(boxes, PER_BOX), strengths.reshape(2, boxes, PER_BOX))
    weights = local_tree(leaf, boxes)
    steps = np.stack([step_matrix(local_depth + k) for k in range(leaf_bits)])
    steps[:, 1] = steps[:, 1, ::-1]
    steps = np.concatenate([steps[:, :, 0], steps[:, :, 1]], axis=-1)
    out = finish_call(
        weights, tgt_pos.reshape(boxes, TGT_BOX), table(steps),
        split_rows(grid_matrix(local_depth + leaf_bits, lax.axis_size("blk"))), leaf_count, lax.axis_size("blk"),
        local_depth + leaf_bits, 8,
    )
    return out.reshape(boxes, 2, TGT_BOX).transpose(1, 0, 2).reshape(2, boxes * TGT_BOX)


def xor(a, d, bits):
    return sum(((a // 2**k % 2 + (d >> k) % 2) % 2) * 2**k for k in range(bits))


def reverse_bits(a, bits):
    return sum((a // 2**k % 2) * 2 ** (bits - 1 - k) for k in range(bits))


def split_pair(x):
    hi = x.astype(jnp.bfloat16)
    return hi, (x - hi.astype(jnp.float32)).astype(jnp.bfloat16)


def dot16(a, b):
    return jnp.dot(a, b, preferred_element_type=jnp.float32)


def far_first(leaves):
    half = leaves // 2
    return [1] + list(range(half, leaves)) + list(range(2, half)) if leaves > 2 else [1]


def two_parts(m):
    hi = m.astype(jnp.bfloat16)
    return jnp.asarray(np.stack([hi, (m - hi.astype(np.float64)).astype(jnp.bfloat16)]))


def moment_matrix():
    wide = leaf_matrix()
    g = wide[:R, : 8 * R : 8].astype(np.float64)
    half = R // 2
    q = np.zeros((R, R))
    for n in range(half):
        q[n, n] = 1.0
        q[half + n, half + n] = 2.0 if n else 1.0
        if n:
            q[half + n, half - n] = -1.0
    return np.kron(np.eye(2), g @ q)


def first_matrix(count):
    m = radix_matrix(0, count)
    return np.einsum("xbc,cd->xbd", m.reshape(m.shape[0], -1, 2 * R), moment_matrix()).reshape(m.shape)


def merge_rows(parts):
    row = lax.broadcasted_iota(jnp.int32, (8, LANES), 0)
    step = 1
    while len(parts) > 1:
        low = row // step % 2 == 0
        half = len(parts) // 2
        pairs = [(parts[2 * k], parts[2 * k + 1]) for k in range(half)]
        parts = [jnp.where(low, a, b) + pltpu.roll(jnp.where(low, b, a), step, 0) for a, b in pairs]
        step *= 2
    return parts[0]


def swap_bits(slots, pairs):
    lane = lax.broadcasted_iota(jnp.int32, (8, LANES), 1)
    slots = list(slots)
    for slot_bit, lane_bit in pairs:
        low = lane // 2**lane_bit % 2 == 0
        for k in range(len(slots)):
            if k >> slot_bit & 1 == 0:
                a, b = slots[k], slots[k + 2**slot_bit]
                slots[k] = jnp.where(low, a, pltpu.roll(b, 2**lane_bit, 1))
                slots[k + 2**slot_bit] = jnp.where(low, pltpu.roll(a, LANES - 2**lane_bit, 1), b)
    return slots


def mm3(w, x):
    hi, lo = split_pair(x)
    return dot16(w[0], hi) + dot16(w[0], lo) + dot16(w[1], hi)


def whole_kernel(pos_hbm, str_hbm, w1_hbm, w2_hbm, w3_hbm, w4_hbm, a_hbm, tgt_hbm, out_hbm,
                 pos, amp, p_t, re_t, im_t, stack, w1, w2, w3, w4, y, got, x2, x3, x4, mine,
                 tgt, out, a_buf, tab, coefs,
                 isem, wsem, send1, recv1, send, recv, gsend, grecv, osem,
                 *, digits, leaves, blocks, depth, rows):
    me, blk_no = lax.axis_index("leaf"), lax.axis_index("blk")
    bits = leaves.bit_length() - 1
    own = digits // leaves
    mesh_id = pl.DeviceIdType.MESH
    across = lax.rem(blk_no + blocks // 2, blocks)
    beside = blk_no + 1 - 2 * (blk_no % 2)
    groups = digits // 8

    def take(g):
        return [
            pltpu.make_async_copy(pos_hbm.at[:, g], pos.at[g], isem.at[0, g]),
            pltpu.make_async_copy(str_hbm.at[0, :, g], amp.at[0, g], isem.at[1, g]),
            pltpu.make_async_copy(str_hbm.at[1, :, g], amp.at[1, g], isem.at[2, g]),
        ]

    later = [
        pltpu.make_async_copy(src, dst, wsem.at[k])
        for k, (src, dst) in enumerate([(w1_hbm, w1), (w2_hbm, w2), (w3_hbm, w3), (w4_hbm, w4), (a_hbm, a_buf), (tgt_hbm, tgt)])
    ]
    for g in range(groups):
        for copy in take(g):
            copy.start()
    for copy in later:
        copy.start()
    barrier = pltpu.get_barrier_semaphore()
    for d in range(1, leaves):
        pl.semaphore_signal(barrier, inc=1, device_id=(xor(me, d, bits), blk_no), device_id_type=mesh_id)
    for peer in (across, beside):
        pl.semaphore_signal(barrier, inc=1, device_id=(me, peer), device_id_type=mesh_id)

    cells_at = lax.broadcasted_iota(jnp.int32, (8, LANES), 1)
    cos_at, sin_at = cos_sin_turns((cells_at * (TOP_TICKS // 2)).astype(jnp.float32) * (2.0**-32))

    def turn_over(g, beta, slot):
        here = pl.ds(beta, LANES, stride=8)
        p_t[slot] = pos.reshape(groups, LANES * 8, LANES)[g, here, :].T
        re_t[slot] = amp.reshape(2, groups, LANES * 8, LANES)[0, g, here, :].T
        im_t[slot] = amp.reshape(2, groups, LANES * 8, LANES)[1, g, here, :].T

    def chunk(slot, i, acc):
        here = pl.ds(i * 8, 8)
        r = p_t[slot, here, :] & (BOX_CELLS - 1)
        c = jnp.take_along_axis(cos_at, r, axis=1)
        s = jnp.take_along_axis(sin_at, r, axis=1)
        a, b = re_t[slot, here, :], im_t[slot, here, :]
        v = r.astype(jnp.float32) * (2.0 / BOX_CELLS) - 1.0
        v2 = v + v
        cheb = [None, v]
        for k in range(2, R // 2 + 1):
            cheb.append(v2 * v - 1.0 if k == 2 else v2 * cheb[-1] - cheb[-2])
        x, z = c * a - s * b, s * a + c * b
        result = []
        for part, (x, z) in enumerate([(x, z), (cheb[-1] * x, cheb[-1] * z)]):
            for k in range(R // 2):
                u, w = acc[part * (R // 2) + k]
                result.append((u + x, w + z) if k == 0 else (u + cheb[k] * x, w + cheb[k] * z))
        return tuple(result)

    for g in range(groups):
        for copy in take(g):
            copy.wait()
        turn_over(g, 0, 0)

        def tile(beta, carry, g=g):
            slot = lax.rem(beta, 2)
            turn_over(g, jnp.minimum(beta + 1, 7), 1 - slot)
            zero = jnp.zeros((8, LANES), jnp.float32)
            acc = tuple((zero, zero) for _ in range(R))
            for i in range(PER_BOX // 8):
                acc = chunk(slot, i, acc)
            half = R // 2
            for part in range(2):
                for k in range(2):
                    stack[g * 8 + beta, (2 * part + k) * 8 : (2 * part + k + 1) * 8, :] = merge_rows(
                        [acc[k * half + n][part] for n in range(half)])
            return carry

        lax.fori_loop(0, 8, tile, 0)

    later[0].wait()
    y[...] = mm3(w1, stack[...].reshape(digits * 2 * R, LANES)).reshape(y.shape)
    pl.semaphore_wait(barrier, leaves + 1)

    def shuffle(d):
        peer = xor(me, d, bits)
        return pltpu.make_async_remote_copy(
            src_ref=y.at[peer], dst_ref=got.at[me],
            send_sem=send1.at[d - 1], recv_sem=recv1.at[d - 1],
            device_id=(peer, blk_no), device_id_type=mesh_id,
        )

    for d in far_first(leaves):
        shuffle(d).start()
    got[me] = y[me]
    for d in far_first(leaves):
        shuffle(d).wait_recv()

    n2, n3 = digits.bit_length() - 1, LANES.bit_length() - digits.bit_length()
    for cg in range(2 * R // 8):
        slots = [got[k, a * 2 * R + cg * 8 : a * 2 * R + cg * 8 + 8, :] for a in range(own) for k in range(leaves)]
        slots = swap_bits(slots, [(k, k) for k in range(n2)])
        for k, v in enumerate(slots):
            x2[k * 2 * R + cg * 8 : k * 2 * R + cg * 8 + 8, :] = v
    later[1].wait()
    z2 = mm3(w2, x2[...])
    x2[...] = z2
    for cg in range(2 * R // 8):
        slots = [x2[k * 2 * R + cg * 8 : k * 2 * R + cg * 8 + 8, :] for k in range(digits)]
        slots = swap_bits(slots, [(k, n3 + k) for k in range(n2)])
        for k, v in enumerate(slots):
            x3[k // own * 2 * R + cg * 8 : k // own * 2 * R + cg * 8 + 8, k % own * LANES : (k % own + 1) * LANES] = v
    later[2].wait()
    x4[...] = mm3(w3, x3[...])
    for cg in range(2 * R // 8):
        for a in range(own):
            cols = slice(a * LANES, (a + 1) * LANES)
            slots = [x4[k * 2 * R + cg * 8 : k * 2 * R + cg * 8 + 8, cols] for k in range(leaves)]
            slots = swap_bits(slots, [(k, k) for k in range(n3)])
            for k, v in enumerate(slots):
                x3[k * 2 * R + cg * 8 : k * 2 * R + cg * 8 + 8, cols] = v
    later[3].wait()
    z4 = mm3(w4, x3[...])
    for a in range(own):
        mine[:, a] = z4[:, a * LANES : (a + 1) * LANES].reshape(leaves, 2 * R, LANES)

    width = own * LANES
    cells = BOX_CELLS * 2**depth
    ticks = TOP_TICKS // 2**depth
    suffix = reverse_bits(me, bits)

    def ship(d):
        peer = xor(me, d, bits)
        return pltpu.make_async_remote_copy(
            src_ref=mine.at[reverse_bits(peer, bits)], dst_ref=coefs.at[blk_no, me],
            send_sem=send.at[d - 1], recv_sem=recv.at[d - 1],
            device_id=(peer, blk_no), device_id_type=mesh_id,
        )

    def spread(way, d):
        here = coefs.at[across if way == 2 else blk_no, xor(me, d, bits)]
        return pltpu.make_async_remote_copy(
            src_ref=here, dst_ref=here,
            send_sem=gsend.at[way, d], recv_sem=grecv.at[way, d],
            device_id=(me, across if way == 0 else beside), device_id_type=mesh_id,
        )

    pitch = ticks // LANES
    tilt = (blocks * cells - 1) / 2.0 * (pitch // 2) / 2.0**32
    cos_poly = fit_even(lambda y: np.cos(2 * np.pi * y), tilt, 3)
    sin_poly = fit_even(lambda y: np.sin(2 * np.pi * y) / y, tilt, 3)
    cos_poly = [c * tilt ** (2 * k) for k, c in enumerate(cos_poly)]
    sin_poly = [c * tilt ** (2 * k + 1) for k, c in enumerate(sin_poly)]
    below = lax.broadcasted_iota(jnp.int32, (rows, LANES), 0) * (leaves * ticks)

    def evaluate(chunk, t):
        pack = jnp.concatenate([coefs[q, chunk, t] for q in range(blocks)], axis=0)
        hi, lo = split_pair(pack.T)
        lhs = jnp.concatenate([hi, lo, hi], axis=1)
        for n in range(2 * (DEGREE + 1)):
            tab[t, n] = dot16(lhs, a_buf[:, n * LANES : (n + 1) * LANES])
        first = pl.multiple_of(chunk * width + t * LANES, LANES)
        for i in range(LANES // rows):
            base = ((first + i * rows) * leaves + suffix) * ticks
            u = (tgt[pl.ds(first + i * rows, rows), :] - (below + base)).astype(jnp.float32)
            cell = (u * (1.0 / pitch) + (0.5 / pitch)).astype(jnp.int32)
            s = (u - cell.astype(jnp.float32) * pitch) * (2.0 / pitch) - 1.0
            got_at = [jnp.take_along_axis(tab[t, n, i * rows : (i + 1) * rows, :], cell, axis=1)
                      for n in range(2 * (DEGREE + 1))]
            z = s * s
            powers = [None, s, z, z * s, z * z]
            re, im = [[got_at[2 * p + part] * powers[p] if p else got_at[part] for p in range(DEGREE + 1)]
                      for part in range(2)]
            re = (re[0] + re[1]) + (re[2] + re[3]) + re[4]
            im = (im[0] + im[1]) + (im[2] + im[3]) + im[4]
            pc, ps = horner(cos_poly, z), s * horner(sin_poly, z)
            out[pl.ds(2 * (first + i * rows), rows, stride=2), :] = pc * re - ps * im
            out[pl.ds(2 * (first + i * rows) + 1, rows, stride=2), :] = pc * im + ps * re

    def put(d):
        span = pl.ds(pl.multiple_of(xor(me, d, bits) * (2 * width), 2 * width), 2 * width)
        return pltpu.make_async_copy(out.at[span], out_hbm.at[span], osem.at[d])

    order = [0] + far_first(leaves)
    for d in order[1:]:
        ship(d).start()
    coefs[blk_no, me] = mine[suffix]
    for step in range(leaves + 4):
        if step < leaves:
            d = order[step]
            if d:
                ship(d).wait_recv()
            spread(0, d).start()
            spread(1, d).start()
        if 0 <= step - 4:
            d = order[step - 4]
            if step == 4:
                later[4].wait()
                later[5].wait()
            spread(1, d).wait_recv()
            spread(2, d).wait_recv()
            for t in range(own):
                evaluate(xor(me, d, bits), t)
            put(d).start()
        if 0 <= step - 2 < leaves:
            d = order[step - 2]
            spread(0, d).wait_recv()
            spread(2, d).start()
    for d in order:
        if d:
            shuffle(d).wait_send()
            ship(d).wait_send()
        for way in range(3):
            spread(way, d).wait_send()
        put(d).wait()


def whole_call(pos, strengths, ticks, leaves, blocks, depth):
    boxes = ticks.shape[0]
    digits = boxes // LANES
    groups = digits // 8
    own = digits // leaves
    n1 = digits.bit_length() - 1
    n3 = LANES.bit_length() - digits.bit_length()
    n, m = digits * 2 * R, 2**n3 * 2 * R
    grid = split_rows(grid_matrix(depth, blocks))
    anywhere = pl.BlockSpec(memory_space=pl.ANY)
    dma = pltpu.SemaphoreType.DMA
    f32, bf16 = jnp.float32, jnp.bfloat16
    return pl.pallas_call(
        functools.partial(whole_kernel, digits=digits, leaves=leaves, blocks=blocks, depth=depth, rows=8),
        out_shape=jax.ShapeDtypeStruct((2 * boxes, TGT_BOX), f32),
        in_specs=[anywhere] * 8,
        out_specs=anywhere,
        scratch_shapes=[
            pltpu.VMEM((groups, LANES, 8, LANES), jnp.int32),
            pltpu.VMEM((2, groups, LANES, 8, LANES), f32),
            pltpu.VMEM((2, LANES, LANES), jnp.int32),
            pltpu.VMEM((2, LANES, LANES), f32),
            pltpu.VMEM((2, LANES, LANES), f32),
            pltpu.VMEM((digits, 2 * R, LANES), f32),
            pltpu.VMEM((2, n, n), bf16),
            pltpu.VMEM((2, n, n), bf16),
            pltpu.VMEM((2, m, m), bf16),
            pltpu.VMEM((2, m, m), bf16),
            pltpu.VMEM((leaves, n // leaves, LANES), f32),
            pltpu.VMEM((leaves, n // leaves, LANES), f32),
            pltpu.VMEM((n, LANES), f32),
            pltpu.VMEM((m, own * LANES), f32),
            pltpu.VMEM((m, own * LANES), f32),
            pltpu.VMEM((leaves, own, 2 * R, LANES), f32),
            pltpu.VMEM((boxes, TGT_BOX), jnp.int32),
            pltpu.VMEM((2 * boxes, TGT_BOX), f32),
            pltpu.VMEM(grid.shape, bf16),
            pltpu.VMEM((own, 2 * (DEGREE + 1), LANES, LANES), f32),
            pltpu.VMEM((blocks, leaves, own, 2 * R, LANES), f32),
            dma((3, groups)), dma((6,)), dma((leaves - 1,)), dma((leaves - 1,)),
            dma((leaves - 1,)), dma((leaves - 1,)), dma((3, leaves)), dma((3, leaves)), dma((leaves,)),
        ],
        compiler_params=pltpu.CompilerParams(collective_id=0, has_side_effects=True),
        name="whole",
    )(
        pos.reshape(LANES, groups, 8, LANES), strengths.reshape(2, LANES, groups, 8, LANES),
        two_parts(first_matrix(n1)), two_parts(radix_matrix(n1, n1)),
        two_parts(radix_matrix(2 * n1, n3)), two_parts(radix_matrix(2 * n1 + n3, n3)),
        grid, ticks,
    )


def local_two_shuffles(src_pos, strengths, tgt_pos):
    leaves, blocks = lax.axis_size("leaf"), lax.axis_size("blk")
    boxes = src_pos.shape[1] // PER_BOX
    depth = boxes.bit_length() - 1 + leaves.bit_length() - 1
    out = whole_call(src_pos, strengths, tgt_pos.reshape(boxes, TGT_BOX), leaves, blocks, depth)
    return out.reshape(boxes, 2, TGT_BOX).transpose(1, 0, 2).reshape(2, boxes * TGT_BOX)


def solution(mesh):
    def local(src_pos, strengths, tgt_pos):
        boxes = src_pos.shape[1] // PER_BOX
        digits = boxes // LANES
        fits = digits % 8 == 0 and digits == 2 * mesh.shape["leaf"] and mesh.shape["leaf"] * digits == LANES
        near = fits and mesh.shape["blk"] == 4
        run = local_two_shuffles if near else local_butterfly
        return run(src_pos, strengths, tgt_pos)

    return jax.shard_map(
        local,
        mesh=mesh,
        in_specs=(P("blk", "leaf"), P(None, "blk", "leaf"), P(("leaf", "blk"))),
        out_specs=P(None, ("leaf", "blk")),
        check_vma=False,
    )
```

```python
import functools
import math

import jax
import jax.numpy as jnp
import numpy as np
from jax import lax
from jax.experimental import pallas as pl
from jax.experimental.pallas import tpu as pltpu
from jax.sharding import PartitionSpec as P

R = 16
PER_BOX = 128
TGT_BOX = 128
BOX_CELLS = 128
TOP_TICKS = 201326592
LANES = 128
HIGHEST = lax.Precision.HIGHEST


def fit_even(values, span, count):
    u = 0.5 * span * span * (1.0 + np.cos(np.pi * (np.arange(400) + 0.5) / 400))
    cheb = np.polynomial.chebyshev.Chebyshev.fit(u, values(np.sqrt(u)), count - 1, domain=[0, span * span])
    return [float(c) for c in cheb.convert(kind=np.polynomial.Polynomial).coef]


COS_POLY = fit_even(lambda y: np.cos(np.pi * y), 0.5, 5)
SIN_POLY = fit_even(lambda y: np.sin(np.pi * y) / y, 0.5, 4)


def horner(coefs, u):
    out = u * coefs[-1] + coefs[-2]
    for c in coefs[-3::-1]:
        out = out * u + c
    return out


def cos_sin_turns(y):
    u = y * y
    c, s = horner(COS_POLY, u), y * horner(SIN_POLY, u)
    twice = s + s
    return 1.0 - twice * s, twice * c


def node_offsets(box_cells):
    node_index = np.arange(R)
    unit_nodes = (1.0 - np.cos(np.pi * (node_index + 0.5) / R)) / 2.0
    return np.floor(box_cells * unit_nodes).astype(np.int64)


def lagrange_values(node_pos, points):
    rows = []
    for row_node in range(node_pos.shape[0]):
        column = np.ones(points.shape[0])
        for other in range(node_pos.shape[0]):
            if other != row_node:
                column = column * (points - node_pos[other]) / (node_pos[row_node] - node_pos[other])
        rows.append(column)
    return np.stack(rows)


def as_real(m):
    return np.block([[m.real, -m.imag], [m.imag, m.real]])


def turn64(a, b):
    product = (a * b + 2**31) % 2**32 - 2**31
    return product * (2.0 * np.pi / 2.0**32)


@functools.cache
def step_matrix(level):
    cells = BOX_CELLS * 2**level
    child, parent = node_offsets(cells), node_offsets(2 * cells)
    inner = np.concatenate([child, child + cells])
    blend = lagrange_values(parent / (2.0 * cells), inner / (2.0 * cells)).reshape(R, 2, R)
    half = TOP_TICKS // 2 ** (level + 2)
    assert half * cells % 2**32 == 2**31
    out = np.zeros((2, 2, 2 * R, 2 * R))
    for e in range(2):
        phase = np.exp(1j * turn64(half if e else -half, child))
        for j in range(2):
            out[e, j] = as_real((-1.0) ** j * blend[:, j, :] * phase[None, :])
    return out


def radix_matrix(first, count):
    total = np.eye(2 * R)[None, None]
    for k in range(count):
        m = step_matrix(first + k)
        n = total.shape[0]
        new = np.zeros((2 * n, 2 * n, 2 * R, 2 * R))
        for a in range(n):
            for b in range(n):
                for e in range(2):
                    for j in range(2):
                        new[2 * a + e, b + j * n] = m[e, j] @ total[a, b]
        total = new
    n = total.shape[0]
    return total.transpose(0, 2, 1, 3).reshape(n * 2 * R, n * 2 * R)


DEGREE = 4


def fit_turn(theta):
    s = np.cos(np.pi * (np.arange(64) + 0.5) / 64)
    fit = np.polynomial.chebyshev.chebfit(s, np.exp(1j * s[:, None] * theta[None, :]), DEGREE)
    power = np.zeros((DEGREE + 1, DEGREE + 1))
    for n in range(DEGREE + 1):
        c = np.polynomial.chebyshev.cheb2poly(np.eye(DEGREE + 1)[n])
        power[: len(c), n] = c
    return power @ fit


@functools.cache
def grid_matrix(depth, blocks):
    cells = BOX_CELLS * 2**depth
    ticks = TOP_TICKS // 2**depth
    step = ticks // LANES
    assert step * LANES == ticks and step % 2 == 0
    nodes = (np.arange(blocks)[:, None] * cells + node_offsets(cells)[None, :]).reshape(-1)
    centers = np.arange(LANES) * step + step // 2 - ticks // 2
    phase = np.exp(1j * turn64(centers[None, :], nodes[:, None]))
    off = (nodes - (blocks * cells - 1) / 2.0) * (step // 2) * (2.0 * np.pi / 2.0**32)
    poly = fit_turn(off)
    out = np.zeros((blocks, 2, R, DEGREE + 1, 2, LANES))
    for p in range(DEGREE + 1):
        b = (poly[p][:, None] * phase).reshape(blocks, R, LANES)
        out[:, 0, :, p, 0], out[:, 0, :, p, 1] = b.real, b.imag
        out[:, 1, :, p, 0], out[:, 1, :, p, 1] = -b.imag, b.real
    return out.reshape(blocks * 2 * R, (DEGREE + 1) * 2 * LANES)


def split_rows(m):
    hi = m.astype(jnp.bfloat16)
    lo = (m - hi.astype(np.float64)).astype(jnp.bfloat16)
    return jnp.asarray(np.concatenate([hi, hi, lo], axis=0))


def leaf_matrix():
    nodes = node_offsets(BOX_CELLS)
    angles = np.pi * (np.arange(R) + 0.5) / R
    at_exact = lagrange_values(2.0 * nodes / BOX_CELLS - 1.0, np.cos(angles))
    cheb_at = np.stack([np.cos(n * angles) for n in range(R)])
    norm = np.where(np.arange(R) == 0, 1.0, 2.0) / R
    g = (norm[:, None] * (cheb_at @ at_exact.T)).astype(np.float32)
    wide = np.repeat(g.T, 8, axis=1)
    zero = np.zeros_like(wide)
    return np.block([[wide, zero], [zero, wide]]).astype(np.float32)


def leaf_kernel(pos_ref, str_ref, mix_ref, out_ref, p_t, re_t, im_t, *, digits):
    def turn_over(beta, slot):
        rows = pl.ds(beta, LANES, stride=digits)
        p_t[slot] = pos_ref[rows, :].T
        re_t[slot] = str_ref[0, rows, :].T
        im_t[slot] = str_ref[1, rows, :].T

    def tile(beta, carry):
        slot = lax.rem(beta, 2)
        turn_over(jnp.minimum(beta + 1, digits - 1), 1 - slot)
        zero = jnp.zeros((8, LANES), jnp.float32)
        acc = tuple((zero, zero) for _ in range(R))
        for i in range(PER_BOX // 8):
            acc = chunk(slot, i, acc)
        low, high = list(acc[: R // 2]), list(acc[R // 2 :])
        top = [high[0]]
        for k in range(1, R // 2):
            top.append(tuple(2.0 * h - m for h, m in zip(high[k], low[R // 2 - k])))
        both = low + top
        stack = jnp.concatenate([x for x, _ in both] + [y for _, y in both], axis=0)
        out_ref[beta] = jnp.dot(mix_ref[...], stack, precision=HIGHEST, preferred_element_type=jnp.float32)
        return carry

    def chunk(slot, i, acc):
        here = pl.ds(i * 8, 8)
        r = p_t[slot, here, :] & (BOX_CELLS - 1)
        turn = (r * (TOP_TICKS // 2)).astype(jnp.float32) * (2.0**-32)
        c, s = cos_sin_turns(turn)
        a, b = re_t[slot, here, :], im_t[slot, here, :]
        v = r.astype(jnp.float32) * (2.0 / BOX_CELLS) - 1.0
        v2 = v + v
        cheb = [None, v]
        for k in range(2, R // 2 + 1):
            cheb.append(v2 * v - 1.0 if k == 2 else v2 * cheb[-1] - cheb[-2])
        x, y = c * a - s * b, s * a + c * b
        out = []
        for part, (x, y) in enumerate([(x, y), (cheb[-1] * x, cheb[-1] * y)]):
            for k in range(R // 2):
                u, w = acc[part * (R // 2) + k]
                out.append((u + x, w + y) if k == 0 else (u + cheb[k] * x, w + cheb[k] * y))
        return tuple(out)

    turn_over(0, 0)
    lax.fori_loop(0, digits, tile, 0)


def leaf_call(pos, strengths):
    boxes = pos.shape[0]
    digits = boxes // LANES
    whole = pl.BlockSpec(memory_space=pltpu.VMEM)
    return pl.pallas_call(
        functools.partial(leaf_kernel, digits=digits),
        out_shape=jax.ShapeDtypeStruct((digits, 2 * R, LANES), jnp.float32),
        in_specs=[whole, whole, whole],
        out_specs=whole,
        scratch_shapes=[
            pltpu.VMEM((2, LANES, LANES), jnp.int32),
            pltpu.VMEM((2, LANES, LANES), jnp.float32),
            pltpu.VMEM((2, LANES, LANES), jnp.float32),
        ],
        name="leaf",
    )(pos, strengths, jnp.asarray(leaf_matrix()))


def finish_kernel(w_ref, tgt_hbm, m_ref, a_hbm, out_hbm, tgt, out, a_buf, tab, bufs, got, coefs,
                  send, recv, gsend, grecv, tsem, asem, osem, *, leaves, blocks, chunks, depth, rows):
    leaf_no, blk_no = lax.axis_index("leaf"), lax.axis_index("blk")
    bits = leaves.bit_length() - 1
    boxes = w_ref.shape[1]
    width = boxes // chunks
    tiles = width // LANES
    cells = BOX_CELLS * 2**depth
    ticks = TOP_TICKS // 2**depth
    sides = [leaf_no // 2**k % 2 for k in range(bits)]
    partners = [leaf_no + (1 - 2 * sides[k]) * 2**k for k in range(bits)]
    suffix = jnp.int32(0)
    for k in range(bits):
        suffix = 2 * suffix + sides[k]
    peers = [lax.rem(blk_no + d, blocks) for d in range(1, blocks)]
    fetch = pltpu.make_async_copy(tgt_hbm, tgt, tsem)
    fetch.start()
    load = pltpu.make_async_copy(a_hbm, a_buf, asem)
    load.start()

    barrier = pltpu.get_barrier_semaphore()
    for k in range(bits):
        pl.semaphore_signal(barrier, inc=1, device_id=(partners[k], blk_no), device_id_type=pl.DeviceIdType.MESH)
    for peer in peers:
        pl.semaphore_signal(barrier, inc=1, device_id=(leaf_no, peer), device_id_type=pl.DeviceIdType.MESH)
    pl.semaphore_wait(barrier, bits + blocks - 1)

    def own(stage, c):
        return w_ref.at[:, pl.ds(c * width, width)] if stage == 0 else bufs.at[stage - 1, c]

    def exchange(stage, c):
        return pltpu.make_async_remote_copy(
            src_ref=own(stage, c), dst_ref=got.at[stage, c],
            send_sem=send.at[stage, c], recv_sem=recv.at[stage, c],
            device_id=(partners[stage], blk_no), device_id_type=pl.DeviceIdType.MESH,
        )

    def spread(d, c):
        here = coefs.at[blk_no, pl.ds(c * tiles, tiles)]
        return pltpu.make_async_remote_copy(
            src_ref=here, dst_ref=here,
            send_sem=gsend.at[d - 1, c], recv_sem=grecv.at[d - 1, c],
            device_id=(leaf_no, peers[d - 1]), device_id_type=pl.DeviceIdType.MESH,
        )

    def combine(todo):
        for stage, c in todo:
            exchange(stage, c).wait_recv()
        results = []
        for stage, c in todo:
            pair = jnp.concatenate([own(stage, c)[...], got[stage, c]], axis=0)
            results.append(mm(m_ref[stage, sides[stage]], pair))
        for (stage, c), w in zip(todo, results):
            if stage < bits - 1:
                bufs[stage, c] = w
            else:
                for i in range(tiles):
                    coefs[blk_no, c * tiles + i] = w[:, i * LANES : (i + 1) * LANES]
        for stage, c in todo:
            if stage < bits - 1:
                exchange(stage + 1, c).start()
            else:
                for d in range(1, blocks):
                    spread(d, c).start()

    pitch = ticks // LANES
    tilt = (blocks * cells - 1) / 2.0 * (pitch // 2) / 2.0**32
    cos_poly = fit_even(lambda y: np.cos(2 * np.pi * y), tilt, 3)
    sin_poly = fit_even(lambda y: np.sin(2 * np.pi * y) / y, tilt, 3)
    cos_poly = [c * tilt ** (2 * k) for k, c in enumerate(cos_poly)]
    sin_poly = [c * tilt ** (2 * k + 1) for k, c in enumerate(sin_poly)]
    below = lax.broadcasted_iota(jnp.int32, (rows, LANES), 0) * (leaves * ticks)

    def evaluate(tile, carry):
        whole = jnp.concatenate([coefs[q, tile] for q in range(blocks)], axis=0).T
        hi = whole.astype(jnp.bfloat16)
        lo = (whole - hi.astype(jnp.float32)).astype(jnp.bfloat16)
        lhs = jnp.concatenate([hi, lo, hi], axis=1)
        for n in range(2 * (DEGREE + 1)):
            tab[n] = jnp.dot(lhs, a_buf[:, n * LANES : (n + 1) * LANES], preferred_element_type=jnp.float32)
        first = pl.multiple_of(tile * LANES, LANES)
        for i in range(LANES // rows):
            base = ((first + i * rows) * leaves + suffix) * ticks
            u = (tgt[pl.ds(first + i * rows, rows), :] - (below + base)).astype(jnp.float32)
            cell = (u * (1.0 / pitch) + (0.5 / pitch)).astype(jnp.int32)
            s = (u - cell.astype(jnp.float32) * pitch) * (2.0 / pitch) - 1.0
            got_at = [jnp.take_along_axis(tab[n, i * rows : (i + 1) * rows, :], cell, axis=1)
                      for n in range(2 * (DEGREE + 1))]
            re, im = got_at[-2], got_at[-1]
            for p in range(DEGREE - 1, -1, -1):
                re, im = re * s + got_at[2 * p], im * s + got_at[2 * p + 1]
            z = s * s
            pc, ps = horner(cos_poly, z), s * horner(sin_poly, z)
            out[pl.ds(2 * (first + i * rows), rows, stride=2), :] = pc * re - ps * im
            out[pl.ds(2 * (first + i * rows) + 1, rows, stride=2), :] = pc * im + ps * re
        return carry

    def put(c):
        span = pl.ds(2 * c * width, 2 * width)
        return pltpu.make_async_copy(out.at[span], out_hbm.at[span], osem.at[c])

    def field(c):
        if c == 0:
            fetch.wait()
            load.wait()
        for d in range(1, blocks):
            spread(d, c).wait_recv()
        lax.fori_loop(c * tiles, (c + 1) * tiles, evaluate, 0)
        put(c).start()

    ahead = min(3, chunks)
    for c in range(ahead):
        exchange(0, c).start()
    for step in range(chunks + bits):
        combine([(k, step - k) for k in range(bits - 1, -1, -1) if 0 <= step - k < chunks])
        if step + ahead < chunks:
            exchange(0, step + ahead).start()
        if step >= bits:
            field(step - bits)
    for c in range(chunks):
        for stage in range(bits):
            exchange(stage, c).wait_send()
        for d in range(1, blocks):
            spread(d, c).wait_send()
        put(c).wait()


def finish_call(weights, ticks, matrices, grid, leaves, blocks, depth, chunks):
    boxes = ticks.shape[0]
    bits = leaves.bit_length() - 1
    width = boxes // chunks
    whole = pl.BlockSpec(memory_space=pltpu.VMEM)
    anywhere = pl.BlockSpec(memory_space=pl.ANY)
    dma = pltpu.SemaphoreType.DMA
    return pl.pallas_call(
        functools.partial(finish_kernel, leaves=leaves, blocks=blocks, chunks=chunks, depth=depth, rows=8),
        out_shape=jax.ShapeDtypeStruct((2 * boxes, TGT_BOX), jnp.float32),
        in_specs=[whole, anywhere, whole, anywhere],
        out_specs=anywhere,
        scratch_shapes=[
            pltpu.VMEM((boxes, TGT_BOX), jnp.int32),
            pltpu.VMEM((2 * boxes, TGT_BOX), jnp.float32),
            pltpu.VMEM(grid.shape, jnp.bfloat16),
            pltpu.VMEM((2 * (DEGREE + 1), LANES, LANES), jnp.float32),
            pltpu.VMEM((bits - 1, chunks, 2 * R, width), jnp.float32),
            pltpu.VMEM((bits, chunks, 2 * R, width), jnp.float32),
            pltpu.VMEM((blocks, boxes // LANES, 2 * R, LANES), jnp.float32),
        ] + [
            dma((bits, chunks)), dma((bits, chunks)),
            dma((blocks - 1, chunks)), dma((blocks - 1, chunks)),
            dma, dma, dma((chunks,)),
        ],
        compiler_params=pltpu.CompilerParams(collective_id=0, has_side_effects=True),
        name="finish",
    )(weights, ticks, matrices, grid)


def table(m):
    return jnp.asarray(m.astype(np.float32))


def mm(a, b):
    return jnp.dot(a, b, precision=HIGHEST, preferred_element_type=jnp.float32)


def local_tree(leaf, boxes):
    low = leaf.shape[0]
    n1 = low.bit_length() - 1
    rest = boxes.bit_length() - 1 - n1
    n2 = rest - rest // 2
    n3 = rest - n2
    c = 2 * R
    y = mm(table(radix_matrix(0, n1)), leaf.reshape(low * c, -1))
    y = y.reshape(low, c, 2**n3, 2**n2).transpose(3, 1, 0, 2).reshape(2**n2 * c, -1)
    y = mm(table(radix_matrix(n1, n2)), y)
    y = y.reshape(2**n2, c, low, 2**n3).transpose(3, 1, 2, 0).reshape(2**n3 * c, -1)
    y = mm(table(radix_matrix(n1 + n2, n3)), y)
    return y.reshape(2**n3, c, low * 2**n2).transpose(1, 2, 0).reshape(c, boxes)


def local_butterfly(src_pos, strengths, tgt_pos):
    leaf_count = lax.axis_size("leaf")
    leaf_bits = leaf_count.bit_length() - 1
    boxes = src_pos.shape[1] // PER_BOX
    local_depth = boxes.bit_length() - 1
    leaf = leaf_call(src_pos.reshape(boxes, PER_BOX), strengths.reshape(2, boxes, PER_BOX))
    weights = local_tree(leaf, boxes)
    steps = np.stack([step_matrix(local_depth + k) for k in range(leaf_bits)])
    steps[:, 1] = steps[:, 1, ::-1]
    steps = np.concatenate([steps[:, :, 0], steps[:, :, 1]], axis=-1)
    out = finish_call(
        weights, tgt_pos.reshape(boxes, TGT_BOX), table(steps),
        split_rows(grid_matrix(local_depth + leaf_bits, lax.axis_size("blk"))), leaf_count, lax.axis_size("blk"),
        local_depth + leaf_bits, 8,
    )
    return out.reshape(boxes, 2, TGT_BOX).transpose(1, 0, 2).reshape(2, boxes * TGT_BOX)


def xor(a, d, bits):
    return sum(((a // 2**k % 2 + (d >> k) % 2) % 2) * 2**k for k in range(bits))


def reverse_bits(a, bits):
    return sum((a // 2**k % 2) * 2 ** (bits - 1 - k) for k in range(bits))


def split_pair(x):
    hi = x.astype(jnp.bfloat16)
    return hi, (x - hi.astype(jnp.float32)).astype(jnp.bfloat16)


def dot16(a, b):
    return jnp.dot(a, b, preferred_element_type=jnp.float32)


def far_first(leaves):
    half = leaves // 2
    return [1] + list(range(half, leaves)) + list(range(2, half)) if leaves > 2 else [1]


def two_parts(m):
    hi = m.astype(jnp.bfloat16)
    return jnp.asarray(np.stack([hi, (m - hi.astype(np.float64)).astype(jnp.bfloat16)]))


def moment_matrix():
    wide = leaf_matrix()
    g = wide[:R, : 8 * R : 8].astype(np.float64)
    half = R // 2
    q = np.zeros((R, R))
    for n in range(half):
        q[n, n] = 1.0
        q[half + n, half + n] = 2.0 if n else 1.0
        if n:
            q[half + n, half - n] = -1.0
    return np.kron(np.eye(2), g @ q)


def first_matrix(count):
    m = radix_matrix(0, count)
    return np.einsum("xbc,cd->xbd", m.reshape(m.shape[0], -1, 2 * R), moment_matrix()).reshape(m.shape)


def merge_rows(parts):
    row = lax.broadcasted_iota(jnp.int32, (8, LANES), 0)
    step = 1
    while len(parts) > 1:
        low = row // step % 2 == 0
        half = len(parts) // 2
        pairs = [(parts[2 * k], parts[2 * k + 1]) for k in range(half)]
        parts = [jnp.where(low, a, b) + pltpu.roll(jnp.where(low, b, a), step, 0) for a, b in pairs]
        step *= 2
    return parts[0]


def swap_bits(slots, pairs):
    lane = lax.broadcasted_iota(jnp.int32, (8, LANES), 1)
    slots = list(slots)
    for slot_bit, lane_bit in pairs:
        low = lane // 2**lane_bit % 2 == 0
        for k in range(len(slots)):
            if k >> slot_bit & 1 == 0:
                a, b = slots[k], slots[k + 2**slot_bit]
                slots[k] = jnp.where(low, a, pltpu.roll(b, 2**lane_bit, 1))
                slots[k + 2**slot_bit] = jnp.where(low, pltpu.roll(a, LANES - 2**lane_bit, 1), b)
    return slots


def mm3(w, x):
    hi, lo = split_pair(x)
    return dot16(w[0], hi) + dot16(w[0], lo) + dot16(w[1], hi)


def whole_kernel(pos_hbm, str_hbm, w1_hbm, w2_hbm, w3_hbm, w4_hbm, a_hbm, tgt_hbm, out_hbm,
                 pos, amp, p_t, re_t, im_t, stack, w1, w2, w3, w4, y, got, x2, x3, x4, mine,
                 tgt, out, a_buf, tab, coefs,
                 isem, wsem, send1, recv1, send, recv, gsend, grecv, osem,
                 *, digits, leaves, blocks, depth, rows):
    me, blk_no = lax.axis_index("leaf"), lax.axis_index("blk")
    bits = leaves.bit_length() - 1
    own = digits // leaves
    mesh_id = pl.DeviceIdType.MESH
    across = lax.rem(blk_no + blocks // 2, blocks)
    beside = blk_no + 1 - 2 * (blk_no % 2)
    groups = digits // 8

    def take(g):
        return [
            pltpu.make_async_copy(pos_hbm.at[:, g], pos.at[g], isem.at[0, g]),
            pltpu.make_async_copy(str_hbm.at[0, :, g], amp.at[0, g], isem.at[1, g]),
            pltpu.make_async_copy(str_hbm.at[1, :, g], amp.at[1, g], isem.at[2, g]),
        ]

    later = [
        pltpu.make_async_copy(src, dst, wsem.at[k])
        for k, (src, dst) in enumerate([(w1_hbm, w1), (w2_hbm, w2), (w3_hbm, w3), (w4_hbm, w4), (a_hbm, a_buf), (tgt_hbm, tgt)])
    ]
    for g in range(groups):
        for copy in take(g):
            copy.start()
    barrier = pltpu.get_barrier_semaphore()
    for d in range(leaves):
        for peer in (blk_no, across) if d else (beside, across):
            pl.semaphore_signal(barrier, inc=1, device_id=(xor(me, d, bits), peer), device_id_type=mesh_id)

    cells_at = lax.broadcasted_iota(jnp.int32, (8, LANES), 1)
    cos_at, sin_at = cos_sin_turns((cells_at * (TOP_TICKS // 2)).astype(jnp.float32) * (2.0**-32))

    def turn_over(g, beta, slot):
        here = pl.ds(beta, LANES, stride=8)
        p_t[slot] = pos.reshape(groups, LANES * 8, LANES)[g, here, :].T
        re_t[slot] = amp.reshape(2, groups, LANES * 8, LANES)[0, g, here, :].T
        im_t[slot] = amp.reshape(2, groups, LANES * 8, LANES)[1, g, here, :].T

    def chunk(slot, i, acc):
        here = pl.ds(i * 8, 8)
        r = p_t[slot, here, :] & (BOX_CELLS - 1)
        c = jnp.take_along_axis(cos_at, r, axis=1)
        s = jnp.take_along_axis(sin_at, r, axis=1)
        a, b = re_t[slot, here, :], im_t[slot, here, :]
        v = r.astype(jnp.float32) * (2.0 / BOX_CELLS) - 1.0
        v2 = v + v
        cheb = [None, v]
        for k in range(2, R // 2 + 1):
            cheb.append(v2 * v - 1.0 if k == 2 else v2 * cheb[-1] - cheb[-2])
        x, z = c * a - s * b, s * a + c * b
        result = []
        for part, (x, z) in enumerate([(x, z), (cheb[-1] * x, cheb[-1] * z)]):
            for k in range(R // 2):
                u, w = acc[part * (R // 2) + k]
                result.append((u + x, w + z) if k == 0 else (u + cheb[k] * x, w + cheb[k] * z))
        return tuple(result)

    for g in range(groups):
        for copy in take(g):
            copy.wait()
        if g == 0:
            for copy in later:
                copy.start()
        turn_over(g, 0, 0)

        def tile(beta, carry, g=g):
            slot = lax.rem(beta, 2)
            turn_over(g, jnp.minimum(beta + 1, 7), 1 - slot)
            zero = jnp.zeros((8, LANES), jnp.float32)
            acc = tuple((zero, zero) for _ in range(R))
            for i in range(PER_BOX // 8):
                acc = chunk(slot, i, acc)
            half = R // 2
            for part in range(2):
                for k in range(2):
                    stack[g * 8 + beta, (2 * part + k) * 8 : (2 * part + k + 1) * 8, :] = merge_rows(
                        [acc[k * half + n][part] for n in range(half)])
            return carry

        lax.fori_loop(0, 8, tile, 0)

    later[0].wait()
    y[...] = mm3(w1, stack[...].reshape(digits * 2 * R, LANES)).reshape(y.shape)
    pl.semaphore_wait(barrier, 2 * leaves)

    def shuffle(d):
        peer = xor(me, d, bits)
        return pltpu.make_async_remote_copy(
            src_ref=y.at[peer], dst_ref=got.at[me],
            send_sem=send1.at[d - 1], recv_sem=recv1.at[d - 1],
            device_id=(peer, blk_no), device_id_type=mesh_id,
        )

    for d in far_first(leaves):
        shuffle(d).start()
    got[me] = y[me]
    for d in far_first(leaves):
        shuffle(d).wait_recv()

    n2, n3 = digits.bit_length() - 1, LANES.bit_length() - digits.bit_length()
    for cg in range(2 * R // 8):
        slots = [got[k, a * 2 * R + cg * 8 : a * 2 * R + cg * 8 + 8, :] for a in range(own) for k in range(leaves)]
        slots = swap_bits(slots, [(k, k) for k in range(n2)])
        for k, v in enumerate(slots):
            x2[k * 2 * R + cg * 8 : k * 2 * R + cg * 8 + 8, :] = v
    later[1].wait()
    z2 = mm3(w2, x2[...])
    x2[...] = z2
    for cg in range(2 * R // 8):
        slots = [x2[k * 2 * R + cg * 8 : k * 2 * R + cg * 8 + 8, :] for k in range(digits)]
        slots = swap_bits(slots, [(k, n3 + k) for k in range(n2)])
        for k, v in enumerate(slots):
            x3[k // own * 2 * R + cg * 8 : k // own * 2 * R + cg * 8 + 8, k % own * LANES : (k % own + 1) * LANES] = v
    later[2].wait()
    x4[...] = mm3(w3, x3[...])
    for cg in range(2 * R // 8):
        for a in range(own):
            cols = slice(a * LANES, (a + 1) * LANES)
            slots = [x4[k * 2 * R + cg * 8 : k * 2 * R + cg * 8 + 8, cols] for k in range(leaves)]
            slots = swap_bits(slots, [(k, k) for k in range(n3)])
            for k, v in enumerate(slots):
                x3[k * 2 * R + cg * 8 : k * 2 * R + cg * 8 + 8, cols] = v
    later[3].wait()
    z4 = mm3(w4, x3[...])
    for a in range(own):
        mine[:, a] = z4[:, a * LANES : (a + 1) * LANES].reshape(leaves, 2 * R, LANES)

    width = own * LANES
    cells = BOX_CELLS * 2**depth
    ticks = TOP_TICKS // 2**depth
    suffix = reverse_bits(me, bits)

    def ship(way, d):
        peer = xor(me, d, bits)
        return pltpu.make_async_remote_copy(
            src_ref=mine.at[reverse_bits(peer, bits)], dst_ref=coefs.at[blk_no, me],
            send_sem=send.at[way, d], recv_sem=recv.at[way, d],
            device_id=(peer, across if way else blk_no), device_id_type=mesh_id,
        )

    def forward(way, d):
        here = coefs.at[across if way else blk_no, xor(me, d, bits)]
        return pltpu.make_async_remote_copy(
            src_ref=here, dst_ref=here,
            send_sem=gsend.at[way, d], recv_sem=grecv.at[way, d],
            device_id=(me, beside), device_id_type=mesh_id,
        )

    pitch = ticks // LANES
    tilt = (blocks * cells - 1) / 2.0 * (pitch // 2) / 2.0**32
    cos_poly = fit_even(lambda y: np.cos(2 * np.pi * y), tilt, 3)
    sin_poly = fit_even(lambda y: np.sin(2 * np.pi * y) / y, tilt, 3)
    cos_poly = [c * tilt ** (2 * k) for k, c in enumerate(cos_poly)]
    sin_poly = [c * tilt ** (2 * k + 1) for k, c in enumerate(sin_poly)]
    below = lax.broadcasted_iota(jnp.int32, (rows, LANES), 0) * (leaves * ticks)

    def tables(chunk, slot):
        parts = [split_pair(jnp.concatenate([coefs[q, chunk, t] for q in range(blocks)], axis=0).T) for t in range(own)]
        hi, lo = [jnp.concatenate(part, axis=0) for part in zip(*parts)]
        lhs = jnp.concatenate([hi, lo, hi], axis=1)
        for p in range(DEGREE + 1):
            both = dot16(lhs, a_buf[:, 2 * p * LANES : 2 * (p + 1) * LANES])
            tab[slot, 2 * p] = both[:, :LANES]
            tab[slot, 2 * p + 1] = both[:, LANES:]

    def points(chunk, slot):
        first = pl.multiple_of(chunk * width, width)
        for i in range(width // rows):
            base = ((first + i * rows) * leaves + suffix) * ticks
            u = (tgt[pl.ds(first + i * rows, rows), :] - (below + base)).astype(jnp.float32)
            cell = (u * (1.0 / pitch) + (0.5 / pitch)).astype(jnp.int32)
            s = (u - cell.astype(jnp.float32) * pitch) * (2.0 / pitch) - 1.0
            got_at = [jnp.take_along_axis(tab[slot, n, i * rows : (i + 1) * rows, :], cell, axis=1)
                      for n in range(2 * (DEGREE + 1))]
            z = s * s
            powers = [None, s, z, z * s, z * z]
            re, im = [[got_at[2 * p + part] * powers[p] if p else got_at[part] for p in range(DEGREE + 1)]
                      for part in range(2)]
            re = (re[0] + re[1]) + (re[2] + re[3]) + re[4]
            im = (im[0] + im[1]) + (im[2] + im[3]) + im[4]
            pc, ps = horner(cos_poly, z), s * horner(sin_poly, z)
            out[pl.ds(2 * (first + i * rows), rows, stride=2), :] = pc * re - ps * im
            out[pl.ds(2 * (first + i * rows) + 1, rows, stride=2), :] = pc * im + ps * re

    def put(d):
        span = pl.ds(pl.multiple_of(xor(me, d, bits) * (2 * width), 2 * width), 2 * width)
        return pltpu.make_async_copy(out.at[span], out_hbm.at[span], osem.at[d])

    order = [0] + far_first(leaves)
    both = [(way, d) for d in order for way in range(2) if way or d]
    for way, d in both:
        ship(way, d).start()
    coefs[blk_no, me] = mine[suffix]
    lag = 2
    for step in range(leaves + lag + 1):
        if step < leaves:
            d = order[step]
            for way in range(2):
                if way or d:
                    ship(way, d).wait_recv()
                forward(way, d).start()
        if step == lag:
            later[4].wait()
            later[5].wait()
        if 0 <= step - lag < leaves:
            d = order[step - lag]
            for way in range(2):
                forward(way, d).wait_recv()
            tables(xor(me, d, bits), (step - lag) % 2)
        if 0 <= step - lag - 1:
            d = order[step - lag - 1]
            points(xor(me, d, bits), (step - lag - 1) % 2)
            put(d).start()
    for d in order:
        if d:
            shuffle(d).wait_send()
        for way in range(2):
            if way or d:
                ship(way, d).wait_send()
            forward(way, d).wait_send()
        put(d).wait()


def whole_call(pos, strengths, ticks, leaves, blocks, depth):
    boxes = ticks.shape[0]
    digits = boxes // LANES
    groups = digits // 8
    own = digits // leaves
    n1 = digits.bit_length() - 1
    n3 = LANES.bit_length() - digits.bit_length()
    n, m = digits * 2 * R, 2**n3 * 2 * R
    grid = split_rows(grid_matrix(depth, blocks))
    anywhere = pl.BlockSpec(memory_space=pl.ANY)
    dma = pltpu.SemaphoreType.DMA
    f32, bf16 = jnp.float32, jnp.bfloat16
    return pl.pallas_call(
        functools.partial(whole_kernel, digits=digits, leaves=leaves, blocks=blocks, depth=depth, rows=8),
        out_shape=jax.ShapeDtypeStruct((2 * boxes, TGT_BOX), f32),
        in_specs=[anywhere] * 8,
        out_specs=anywhere,
        scratch_shapes=[
            pltpu.VMEM((groups, LANES, 8, LANES), jnp.int32),
            pltpu.VMEM((2, groups, LANES, 8, LANES), f32),
            pltpu.VMEM((2, LANES, LANES), jnp.int32),
            pltpu.VMEM((2, LANES, LANES), f32),
            pltpu.VMEM((2, LANES, LANES), f32),
            pltpu.VMEM((digits, 2 * R, LANES), f32),
            pltpu.VMEM((2, n, n), bf16),
            pltpu.VMEM((2, n, n), bf16),
            pltpu.VMEM((2, m, m), bf16),
            pltpu.VMEM((2, m, m), bf16),
            pltpu.VMEM((leaves, n // leaves, LANES), f32),
            pltpu.VMEM((leaves, n // leaves, LANES), f32),
            pltpu.VMEM((n, LANES), f32),
            pltpu.VMEM((m, own * LANES), f32),
            pltpu.VMEM((m, own * LANES), f32),
            pltpu.VMEM((leaves, own, 2 * R, LANES), f32),
            pltpu.VMEM((boxes, TGT_BOX), jnp.int32),
            pltpu.VMEM((2 * boxes, TGT_BOX), f32),
            pltpu.VMEM(grid.shape, bf16),
            pltpu.VMEM((2, 2 * (DEGREE + 1), own * LANES, LANES), f32),
            pltpu.VMEM((blocks, leaves, own, 2 * R, LANES), f32),
            dma((3, groups)), dma((6,)), dma((leaves - 1,)), dma((leaves - 1,)),
            dma((2, leaves)), dma((2, leaves)), dma((2, leaves)), dma((2, leaves)), dma((leaves,)),
        ],
        compiler_params=pltpu.CompilerParams(collective_id=0, has_side_effects=True),
        name="whole",
    )(
        pos.reshape(LANES, groups, 8, LANES), strengths.reshape(2, LANES, groups, 8, LANES),
        two_parts(first_matrix(n1)), two_parts(radix_matrix(n1, n1)),
        two_parts(radix_matrix(2 * n1, n3)), two_parts(radix_matrix(2 * n1 + n3, n3)),
        grid, ticks,
    )


def local_two_shuffles(src_pos, strengths, tgt_pos):
    leaves, blocks = lax.axis_size("leaf"), lax.axis_size("blk")
    boxes = src_pos.shape[1] // PER_BOX
    depth = boxes.bit_length() - 1 + leaves.bit_length() - 1
    out = whole_call(src_pos, strengths, tgt_pos.reshape(boxes, TGT_BOX), leaves, blocks, depth)
    return out.reshape(boxes, 2, TGT_BOX).transpose(1, 0, 2).reshape(2, boxes * TGT_BOX)


def solution(mesh):
    def local(src_pos, strengths, tgt_pos):
        boxes = src_pos.shape[1] // PER_BOX
        digits = boxes // LANES
        fits = digits % 8 == 0 and digits == 2 * mesh.shape["leaf"] and mesh.shape["leaf"] * digits == LANES
        near = fits and mesh.shape["blk"] == 4
        run = local_two_shuffles if near else local_butterfly
        return run(src_pos, strengths, tgt_pos)

    return jax.shard_map(
        local,
        mesh=mesh,
        in_specs=(P("blk", "leaf"), P(None, "blk", "leaf"), P(("leaf", "blk"))),
        out_specs=P(None, ("leaf", "blk")),
        check_vma=False,
    )
```

```python
import functools
import math

import jax
import jax.numpy as jnp
import numpy as np
from jax import lax
from jax.experimental import pallas as pl
from jax.experimental.pallas import tpu as pltpu
from jax.sharding import PartitionSpec as P

R = 16
PER_BOX = 128
TGT_BOX = 128
BOX_CELLS = 128
TOP_TICKS = 201326592
LANES = 128
HIGHEST = lax.Precision.HIGHEST


def fit_even(values, span, count):
    u = 0.5 * span * span * (1.0 + np.cos(np.pi * (np.arange(400) + 0.5) / 400))
    cheb = np.polynomial.chebyshev.Chebyshev.fit(u, values(np.sqrt(u)), count - 1, domain=[0, span * span])
    return [float(c) for c in cheb.convert(kind=np.polynomial.Polynomial).coef]


COS_POLY = fit_even(lambda y: np.cos(np.pi * y), 0.5, 5)
SIN_POLY = fit_even(lambda y: np.sin(np.pi * y) / y, 0.5, 4)


def horner(coefs, u):
    out = u * coefs[-1] + coefs[-2]
    for c in coefs[-3::-1]:
        out = out * u + c
    return out


def cos_sin_turns(y):
    u = y * y
    c, s = horner(COS_POLY, u), y * horner(SIN_POLY, u)
    twice = s + s
    return 1.0 - twice * s, twice * c


def node_offsets(box_cells):
    node_index = np.arange(R)
    unit_nodes = (1.0 - np.cos(np.pi * (node_index + 0.5) / R)) / 2.0
    return np.floor(box_cells * unit_nodes).astype(np.int64)


def lagrange_values(node_pos, points):
    rows = []
    for row_node in range(node_pos.shape[0]):
        column = np.ones(points.shape[0])
        for other in range(node_pos.shape[0]):
            if other != row_node:
                column = column * (points - node_pos[other]) / (node_pos[row_node] - node_pos[other])
        rows.append(column)
    return np.stack(rows)


def as_real(m):
    return np.block([[m.real, -m.imag], [m.imag, m.real]])


def turn64(a, b):
    product = (a * b + 2**31) % 2**32 - 2**31
    return product * (2.0 * np.pi / 2.0**32)


@functools.cache
def step_matrix(level):
    cells = BOX_CELLS * 2**level
    child, parent = node_offsets(cells), node_offsets(2 * cells)
    inner = np.concatenate([child, child + cells])
    blend = lagrange_values(parent / (2.0 * cells), inner / (2.0 * cells)).reshape(R, 2, R)
    half = TOP_TICKS // 2 ** (level + 2)
    assert half * cells % 2**32 == 2**31
    out = np.zeros((2, 2, 2 * R, 2 * R))
    for e in range(2):
        phase = np.exp(1j * turn64(half if e else -half, child))
        for j in range(2):
            out[e, j] = as_real((-1.0) ** j * blend[:, j, :] * phase[None, :])
    return out


def radix_matrix(first, count):
    total = np.eye(2 * R)[None, None]
    for k in range(count):
        m = step_matrix(first + k)
        n = total.shape[0]
        new = np.zeros((2 * n, 2 * n, 2 * R, 2 * R))
        for a in range(n):
            for b in range(n):
                for e in range(2):
                    for j in range(2):
                        new[2 * a + e, b + j * n] = m[e, j] @ total[a, b]
        total = new
    n = total.shape[0]
    return total.transpose(0, 2, 1, 3).reshape(n * 2 * R, n * 2 * R)


DEGREE = 4


def fit_turn(theta):
    s = np.cos(np.pi * (np.arange(64) + 0.5) / 64)
    fit = np.polynomial.chebyshev.chebfit(s, np.exp(1j * s[:, None] * theta[None, :]), DEGREE)
    power = np.zeros((DEGREE + 1, DEGREE + 1))
    for n in range(DEGREE + 1):
        c = np.polynomial.chebyshev.cheb2poly(np.eye(DEGREE + 1)[n])
        power[: len(c), n] = c
    return power @ fit


@functools.cache
def grid_matrix(depth, blocks):
    cells = BOX_CELLS * 2**depth
    ticks = TOP_TICKS // 2**depth
    step = ticks // LANES
    assert step * LANES == ticks and step % 2 == 0
    nodes = (np.arange(blocks)[:, None] * cells + node_offsets(cells)[None, :]).reshape(-1)
    centers = np.arange(LANES) * step + step // 2 - ticks // 2
    phase = np.exp(1j * turn64(centers[None, :], nodes[:, None]))
    off = (nodes - (blocks * cells - 1) / 2.0) * (step // 2) * (2.0 * np.pi / 2.0**32)
    poly = fit_turn(off)
    out = np.zeros((blocks, 2, R, DEGREE + 1, 2, LANES))
    for p in range(DEGREE + 1):
        b = (poly[p][:, None] * phase).reshape(blocks, R, LANES)
        out[:, 0, :, p, 0], out[:, 0, :, p, 1] = b.real, b.imag
        out[:, 1, :, p, 0], out[:, 1, :, p, 1] = -b.imag, b.real
    return out.reshape(blocks * 2 * R, (DEGREE + 1) * 2 * LANES)


def split_rows(m):
    hi = m.astype(jnp.bfloat16)
    lo = (m - hi.astype(np.float64)).astype(jnp.bfloat16)
    return jnp.asarray(np.concatenate([hi, hi, lo], axis=0))


def leaf_matrix():
    nodes = node_offsets(BOX_CELLS)
    angles = np.pi * (np.arange(R) + 0.5) / R
    at_exact = lagrange_values(2.0 * nodes / BOX_CELLS - 1.0, np.cos(angles))
    cheb_at = np.stack([np.cos(n * angles) for n in range(R)])
    norm = np.where(np.arange(R) == 0, 1.0, 2.0) / R
    g = (norm[:, None] * (cheb_at @ at_exact.T)).astype(np.float32)
    wide = np.repeat(g.T, 8, axis=1)
    zero = np.zeros_like(wide)
    return np.block([[wide, zero], [zero, wide]]).astype(np.float32)


def leaf_kernel(pos_ref, str_ref, mix_ref, out_ref, p_t, re_t, im_t, *, digits):
    def turn_over(beta, slot):
        rows = pl.ds(beta, LANES, stride=digits)
        p_t[slot] = pos_ref[rows, :].T
        re_t[slot] = str_ref[0, rows, :].T
        im_t[slot] = str_ref[1, rows, :].T

    def tile(beta, carry):
        slot = lax.rem(beta, 2)
        turn_over(jnp.minimum(beta + 1, digits - 1), 1 - slot)
        zero = jnp.zeros((8, LANES), jnp.float32)
        acc = tuple((zero, zero) for _ in range(R))
        for i in range(PER_BOX // 8):
            acc = chunk(slot, i, acc)
        low, high = list(acc[: R // 2]), list(acc[R // 2 :])
        top = [high[0]]
        for k in range(1, R // 2):
            top.append(tuple(2.0 * h - m for h, m in zip(high[k], low[R // 2 - k])))
        both = low + top
        stack = jnp.concatenate([x for x, _ in both] + [y for _, y in both], axis=0)
        out_ref[beta] = jnp.dot(mix_ref[...], stack, precision=HIGHEST, preferred_element_type=jnp.float32)
        return carry

    def chunk(slot, i, acc):
        here = pl.ds(i * 8, 8)
        r = p_t[slot, here, :] & (BOX_CELLS - 1)
        turn = (r * (TOP_TICKS // 2)).astype(jnp.float32) * (2.0**-32)
        c, s = cos_sin_turns(turn)
        a, b = re_t[slot, here, :], im_t[slot, here, :]
        v = r.astype(jnp.float32) * (2.0 / BOX_CELLS) - 1.0
        v2 = v + v
        cheb = [None, v]
        for k in range(2, R // 2 + 1):
            cheb.append(v2 * v - 1.0 if k == 2 else v2 * cheb[-1] - cheb[-2])
        x, y = c * a - s * b, s * a + c * b
        out = []
        for part, (x, y) in enumerate([(x, y), (cheb[-1] * x, cheb[-1] * y)]):
            for k in range(R // 2):
                u, w = acc[part * (R // 2) + k]
                out.append((u + x, w + y) if k == 0 else (u + cheb[k] * x, w + cheb[k] * y))
        return tuple(out)

    turn_over(0, 0)
    lax.fori_loop(0, digits, tile, 0)


def leaf_call(pos, strengths):
    boxes = pos.shape[0]
    digits = boxes // LANES
    whole = pl.BlockSpec(memory_space=pltpu.VMEM)
    return pl.pallas_call(
        functools.partial(leaf_kernel, digits=digits),
        out_shape=jax.ShapeDtypeStruct((digits, 2 * R, LANES), jnp.float32),
        in_specs=[whole, whole, whole],
        out_specs=whole,
        scratch_shapes=[
            pltpu.VMEM((2, LANES, LANES), jnp.int32),
            pltpu.VMEM((2, LANES, LANES), jnp.float32),
            pltpu.VMEM((2, LANES, LANES), jnp.float32),
        ],
        name="leaf",
    )(pos, strengths, jnp.asarray(leaf_matrix()))


def finish_kernel(w_ref, tgt_hbm, m_ref, a_hbm, out_hbm, tgt, out, a_buf, tab, bufs, got, coefs,
                  send, recv, gsend, grecv, tsem, asem, osem, *, leaves, blocks, chunks, depth, rows):
    leaf_no, blk_no = lax.axis_index("leaf"), lax.axis_index("blk")
    bits = leaves.bit_length() - 1
    boxes = w_ref.shape[1]
    width = boxes // chunks
    tiles = width // LANES
    cells = BOX_CELLS * 2**depth
    ticks = TOP_TICKS // 2**depth
    sides = [leaf_no // 2**k % 2 for k in range(bits)]
    partners = [leaf_no + (1 - 2 * sides[k]) * 2**k for k in range(bits)]
    suffix = jnp.int32(0)
    for k in range(bits):
        suffix = 2 * suffix + sides[k]
    peers = [lax.rem(blk_no + d, blocks) for d in range(1, blocks)]
    fetch = pltpu.make_async_copy(tgt_hbm, tgt, tsem)
    fetch.start()
    load = pltpu.make_async_copy(a_hbm, a_buf, asem)
    load.start()

    barrier = pltpu.get_barrier_semaphore()
    for k in range(bits):
        pl.semaphore_signal(barrier, inc=1, device_id=(partners[k], blk_no), device_id_type=pl.DeviceIdType.MESH)
    for peer in peers:
        pl.semaphore_signal(barrier, inc=1, device_id=(leaf_no, peer), device_id_type=pl.DeviceIdType.MESH)
    pl.semaphore_wait(barrier, bits + blocks - 1)

    def own(stage, c):
        return w_ref.at[:, pl.ds(c * width, width)] if stage == 0 else bufs.at[stage - 1, c]

    def exchange(stage, c):
        return pltpu.make_async_remote_copy(
            src_ref=own(stage, c), dst_ref=got.at[stage, c],
            send_sem=send.at[stage, c], recv_sem=recv.at[stage, c],
            device_id=(partners[stage], blk_no), device_id_type=pl.DeviceIdType.MESH,
        )

    def spread(d, c):
        here = coefs.at[blk_no, pl.ds(c * tiles, tiles)]
        return pltpu.make_async_remote_copy(
            src_ref=here, dst_ref=here,
            send_sem=gsend.at[d - 1, c], recv_sem=grecv.at[d - 1, c],
            device_id=(leaf_no, peers[d - 1]), device_id_type=pl.DeviceIdType.MESH,
        )

    def combine(todo):
        for stage, c in todo:
            exchange(stage, c).wait_recv()
        results = []
        for stage, c in todo:
            pair = jnp.concatenate([own(stage, c)[...], got[stage, c]], axis=0)
            results.append(mm(m_ref[stage, sides[stage]], pair))
        for (stage, c), w in zip(todo, results):
            if stage < bits - 1:
                bufs[stage, c] = w
            else:
                for i in range(tiles):
                    coefs[blk_no, c * tiles + i] = w[:, i * LANES : (i + 1) * LANES]
        for stage, c in todo:
            if stage < bits - 1:
                exchange(stage + 1, c).start()
            else:
                for d in range(1, blocks):
                    spread(d, c).start()

    pitch = ticks // LANES
    tilt = (blocks * cells - 1) / 2.0 * (pitch // 2) / 2.0**32
    cos_poly = fit_even(lambda y: np.cos(2 * np.pi * y), tilt, 3)
    sin_poly = fit_even(lambda y: np.sin(2 * np.pi * y) / y, tilt, 3)
    cos_poly = [c * tilt ** (2 * k) for k, c in enumerate(cos_poly)]
    sin_poly = [c * tilt ** (2 * k + 1) for k, c in enumerate(sin_poly)]
    below = lax.broadcasted_iota(jnp.int32, (rows, LANES), 0) * (leaves * ticks)

    def evaluate(tile, carry):
        whole = jnp.concatenate([coefs[q, tile] for q in range(blocks)], axis=0).T
        hi = whole.astype(jnp.bfloat16)
        lo = (whole - hi.astype(jnp.float32)).astype(jnp.bfloat16)
        lhs = jnp.concatenate([hi, lo, hi], axis=1)
        for n in range(2 * (DEGREE + 1)):
            tab[n] = jnp.dot(lhs, a_buf[:, n * LANES : (n + 1) * LANES], preferred_element_type=jnp.float32)
        first = pl.multiple_of(tile * LANES, LANES)
        for i in range(LANES // rows):
            base = ((first + i * rows) * leaves + suffix) * ticks
            u = (tgt[pl.ds(first + i * rows, rows), :] - (below + base)).astype(jnp.float32)
            cell = (u * (1.0 / pitch) + (0.5 / pitch)).astype(jnp.int32)
            s = (u - cell.astype(jnp.float32) * pitch) * (2.0 / pitch) - 1.0
            got_at = [jnp.take_along_axis(tab[n, i * rows : (i + 1) * rows, :], cell, axis=1)
                      for n in range(2 * (DEGREE + 1))]
            re, im = got_at[-2], got_at[-1]
            for p in range(DEGREE - 1, -1, -1):
                re, im = re * s + got_at[2 * p], im * s + got_at[2 * p + 1]
            z = s * s
            pc, ps = horner(cos_poly, z), s * horner(sin_poly, z)
            out[pl.ds(2 * (first + i * rows), rows, stride=2), :] = pc * re - ps * im
            out[pl.ds(2 * (first + i * rows) + 1, rows, stride=2), :] = pc * im + ps * re
        return carry

    def put(c):
        span = pl.ds(2 * c * width, 2 * width)
        return pltpu.make_async_copy(out.at[span], out_hbm.at[span], osem.at[c])

    def field(c):
        if c == 0:
            fetch.wait()
            load.wait()
        for d in range(1, blocks):
            spread(d, c).wait_recv()
        lax.fori_loop(c * tiles, (c + 1) * tiles, evaluate, 0)
        put(c).start()

    ahead = min(3, chunks)
    for c in range(ahead):
        exchange(0, c).start()
    for step in range(chunks + bits):
        combine([(k, step - k) for k in range(bits - 1, -1, -1) if 0 <= step - k < chunks])
        if step + ahead < chunks:
            exchange(0, step + ahead).start()
        if step >= bits:
            field(step - bits)
    for c in range(chunks):
        for stage in range(bits):
            exchange(stage, c).wait_send()
        for d in range(1, blocks):
            spread(d, c).wait_send()
        put(c).wait()


def finish_call(weights, ticks, matrices, grid, leaves, blocks, depth, chunks):
    boxes = ticks.shape[0]
    bits = leaves.bit_length() - 1
    width = boxes // chunks
    whole = pl.BlockSpec(memory_space=pltpu.VMEM)
    anywhere = pl.BlockSpec(memory_space=pl.ANY)
    dma = pltpu.SemaphoreType.DMA
    return pl.pallas_call(
        functools.partial(finish_kernel, leaves=leaves, blocks=blocks, chunks=chunks, depth=depth, rows=8),
        out_shape=jax.ShapeDtypeStruct((2 * boxes, TGT_BOX), jnp.float32),
        in_specs=[whole, anywhere, whole, anywhere],
        out_specs=anywhere,
        scratch_shapes=[
            pltpu.VMEM((boxes, TGT_BOX), jnp.int32),
            pltpu.VMEM((2 * boxes, TGT_BOX), jnp.float32),
            pltpu.VMEM(grid.shape, jnp.bfloat16),
            pltpu.VMEM((2 * (DEGREE + 1), LANES, LANES), jnp.float32),
            pltpu.VMEM((bits - 1, chunks, 2 * R, width), jnp.float32),
            pltpu.VMEM((bits, chunks, 2 * R, width), jnp.float32),
            pltpu.VMEM((blocks, boxes // LANES, 2 * R, LANES), jnp.float32),
        ] + [
            dma((bits, chunks)), dma((bits, chunks)),
            dma((blocks - 1, chunks)), dma((blocks - 1, chunks)),
            dma, dma, dma((chunks,)),
        ],
        compiler_params=pltpu.CompilerParams(collective_id=0, has_side_effects=True),
        name="finish",
    )(weights, ticks, matrices, grid)


def table(m):
    return jnp.asarray(m.astype(np.float32))


def mm(a, b):
    return jnp.dot(a, b, precision=HIGHEST, preferred_element_type=jnp.float32)


def local_tree(leaf, boxes):
    low = leaf.shape[0]
    n1 = low.bit_length() - 1
    rest = boxes.bit_length() - 1 - n1
    n2 = rest - rest // 2
    n3 = rest - n2
    c = 2 * R
    y = mm(table(radix_matrix(0, n1)), leaf.reshape(low * c, -1))
    y = y.reshape(low, c, 2**n3, 2**n2).transpose(3, 1, 0, 2).reshape(2**n2 * c, -1)
    y = mm(table(radix_matrix(n1, n2)), y)
    y = y.reshape(2**n2, c, low, 2**n3).transpose(3, 1, 2, 0).reshape(2**n3 * c, -1)
    y = mm(table(radix_matrix(n1 + n2, n3)), y)
    return y.reshape(2**n3, c, low * 2**n2).transpose(1, 2, 0).reshape(c, boxes)


def local_butterfly(src_pos, strengths, tgt_pos):
    leaf_count = lax.axis_size("leaf")
    leaf_bits = leaf_count.bit_length() - 1
    boxes = src_pos.shape[1] // PER_BOX
    local_depth = boxes.bit_length() - 1
    leaf = leaf_call(src_pos.reshape(boxes, PER_BOX), strengths.reshape(2, boxes, PER_BOX))
    weights = local_tree(leaf, boxes)
    steps = np.stack([step_matrix(local_depth + k) for k in range(leaf_bits)])
    steps[:, 1] = steps[:, 1, ::-1]
    steps = np.concatenate([steps[:, :, 0], steps[:, :, 1]], axis=-1)
    out = finish_call(
        weights, tgt_pos.reshape(boxes, TGT_BOX), table(steps),
        split_rows(grid_matrix(local_depth + leaf_bits, lax.axis_size("blk"))), leaf_count, lax.axis_size("blk"),
        local_depth + leaf_bits, 8,
    )
    return out.reshape(boxes, 2, TGT_BOX).transpose(1, 0, 2).reshape(2, boxes * TGT_BOX)


def xor(a, d, bits):
    return sum(((a // 2**k % 2 + (d >> k) % 2) % 2) * 2**k for k in range(bits))


def reverse_bits(a, bits):
    return sum((a // 2**k % 2) * 2 ** (bits - 1 - k) for k in range(bits))


def split_pair(x):
    hi = x.astype(jnp.bfloat16)
    return hi, (x - hi.astype(jnp.float32)).astype(jnp.bfloat16)


def dot16(a, b):
    return jnp.dot(a, b, preferred_element_type=jnp.float32)


def far_first(leaves):
    half = leaves // 2
    return [1] + list(range(half, leaves)) + list(range(2, half)) if leaves > 2 else [1]


def two_parts(m):
    hi = m.astype(jnp.bfloat16)
    return jnp.asarray(np.stack([hi, (m - hi.astype(np.float64)).astype(jnp.bfloat16)]))


def moment_matrix():
    wide = leaf_matrix()
    g = wide[:R, : 8 * R : 8].astype(np.float64)
    half = R // 2
    q = np.zeros((R, R))
    for n in range(half):
        q[n, n] = 1.0
        q[half + n, half + n] = 2.0 if n else 1.0
        if n:
            q[half + n, half - n] = -1.0
    return np.kron(np.eye(2), g @ q)


def first_matrix(count):
    m = radix_matrix(0, count)
    return np.einsum("xbc,cd->xbd", m.reshape(m.shape[0], -1, 2 * R), moment_matrix()).reshape(m.shape)


def merge_rows(parts):
    row = lax.broadcasted_iota(jnp.int32, (8, LANES), 0)
    step = 1
    while len(parts) > 1:
        low = row // step % 2 == 0
        half = len(parts) // 2
        pairs = [(parts[2 * k], parts[2 * k + 1]) for k in range(half)]
        parts = [jnp.where(low, a, b) + pltpu.roll(jnp.where(low, b, a), step, 0) for a, b in pairs]
        step *= 2
    return parts[0]


def swap_bits(slots, pairs):
    lane = lax.broadcasted_iota(jnp.int32, (8, LANES), 1)
    slots = list(slots)
    for slot_bit, lane_bit in pairs:
        low = lane // 2**lane_bit % 2 == 0
        for k in range(len(slots)):
            if k >> slot_bit & 1 == 0:
                a, b = slots[k], slots[k + 2**slot_bit]
                slots[k] = jnp.where(low, a, pltpu.roll(b, 2**lane_bit, 1))
                slots[k + 2**slot_bit] = jnp.where(low, pltpu.roll(a, LANES - 2**lane_bit, 1), b)
    return slots


def mm3(w, x):
    hi, lo = split_pair(x)
    return dot16(w[0], hi) + dot16(w[0], lo) + dot16(w[1], hi)


def whole_kernel(pos_hbm, str_hbm, w1_hbm, w2_hbm, w3_hbm, w4_hbm, a_hbm, tgt_hbm, out_hbm,
                 pos, amp, p_t, re_t, im_t, stack, w1, w2, w3, w4, y, got, x2, x3, x4, mine,
                 tgt, out, a_buf, tab, coefs,
                 isem, wsem, send1, recv1, send, recv, gsend, grecv, osem,
                 *, digits, leaves, blocks, depth, rows):
    me, blk_no = lax.axis_index("leaf"), lax.axis_index("blk")
    bits = leaves.bit_length() - 1
    own = digits // leaves
    mesh_id = pl.DeviceIdType.MESH
    across = lax.rem(blk_no + blocks // 2, blocks)
    beside = blk_no + 1 - 2 * (blk_no % 2)
    groups = digits // 8

    def take(g):
        return [
            pltpu.make_async_copy(pos_hbm.at[:, g], pos.at[g], isem.at[0, g]),
            pltpu.make_async_copy(str_hbm.at[0, :, g], amp.at[0, g], isem.at[1, g]),
            pltpu.make_async_copy(str_hbm.at[1, :, g], amp.at[1, g], isem.at[2, g]),
        ]

    later = [
        pltpu.make_async_copy(src, dst, wsem.at[k])
        for k, (src, dst) in enumerate([(w1_hbm, w1), (w2_hbm, w2), (w3_hbm, w3), (w4_hbm, w4), (a_hbm, a_buf), (tgt_hbm, tgt)])
    ]
    for g in range(groups):
        for copy in take(g):
            copy.start()
    barrier = pltpu.get_barrier_semaphore()
    signals = 0
    for d in range(leaves):
        for peer in ([blk_no] if d else [beside]) + ([across] if d < leaves // 2 else []):
            pl.semaphore_signal(barrier, inc=1, device_id=(xor(me, d, bits), peer), device_id_type=mesh_id)
            signals += 1

    cells_at = lax.broadcasted_iota(jnp.int32, (8, LANES), 1)
    cos_at, sin_at = cos_sin_turns((cells_at * (TOP_TICKS // 2)).astype(jnp.float32) * (2.0**-32))

    def turn_over(g, beta, slot):
        here = pl.ds(beta, LANES, stride=8)
        p_t[slot] = pos.reshape(groups, LANES * 8, LANES)[g, here, :].T
        re_t[slot] = amp.reshape(2, groups, LANES * 8, LANES)[0, g, here, :].T
        im_t[slot] = amp.reshape(2, groups, LANES * 8, LANES)[1, g, here, :].T

    def chunk(slot, i, acc):
        here = pl.ds(i * 8, 8)
        r = p_t[slot, here, :] & (BOX_CELLS - 1)
        c = jnp.take_along_axis(cos_at, r, axis=1)
        s = jnp.take_along_axis(sin_at, r, axis=1)
        a, b = re_t[slot, here, :], im_t[slot, here, :]
        v = r.astype(jnp.float32) * (2.0 / BOX_CELLS) - 1.0
        v2 = v + v
        cheb = [None, v]
        for k in range(2, R // 2 + 1):
            cheb.append(v2 * v - 1.0 if k == 2 else v2 * cheb[-1] - cheb[-2])
        x, z = c * a - s * b, s * a + c * b
        result = []
        for part, (x, z) in enumerate([(x, z), (cheb[-1] * x, cheb[-1] * z)]):
            for k in range(R // 2):
                u, w = acc[part * (R // 2) + k]
                result.append((u + x, w + z) if k == 0 else (u + cheb[k] * x, w + cheb[k] * z))
        return tuple(result)

    def shuffle(g, d):
        peer = xor(me, d, bits)
        return pltpu.make_async_remote_copy(
            src_ref=y.at[g, peer], dst_ref=got.at[g, me],
            send_sem=send1.at[g, d], recv_sem=recv1.at[g, d],
            device_id=(peer, blk_no), device_id_type=mesh_id,
        )

    for g in range(groups):
        for copy in take(g):
            copy.wait()
        if g == 0:
            for copy in later:
                copy.start()
        turn_over(g, 0, 0)

        def tile(beta, carry, g=g):
            slot = lax.rem(beta, 2)
            turn_over(g, jnp.minimum(beta + 1, 7), 1 - slot)
            zero = jnp.zeros((8, LANES), jnp.float32)
            acc = tuple((zero, zero) for _ in range(R))
            for i in range(PER_BOX // 8):
                acc = chunk(slot, i, acc)
            half = R // 2
            for part in range(2):
                for k in range(2):
                    stack[g * 8 + beta, (2 * part + k) * 8 : (2 * part + k + 1) * 8, :] = merge_rows(
                        [acc[k * half + n][part] for n in range(half)])
            return carry

        lax.fori_loop(0, 8, tile, 0)
        if g == 0:
            later[0].wait()
            pl.semaphore_wait(barrier, signals)
        y[g] = mm3(w1, stack[g * 8 : (g + 1) * 8].reshape(8 * 2 * R, LANES)).reshape(leaves, 2 * R, LANES)
        for d in far_first(leaves):
            shuffle(g, d).start()

    got[:, me] = y[:, me]
    for g in range(groups):
        for d in range(1, leaves):
            shuffle(g, d).wait_recv()

    n2 = digits.bit_length() - 1
    for cg in range(2 * R // 8):
        slots = [got[j, k, cg * 8 : cg * 8 + 8, :] for k in range(leaves) for j in range(own)]
        slots = swap_bits(slots, [(n2 - bits + k, k) for k in range(bits)])
        for k, v in enumerate(slots):
            x2[k * 2 * R + cg * 8 : k * 2 * R + cg * 8 + 8, :] = v
    later[1].wait()
    z2 = mm3(w2, x2[...])
    x2[...] = z2
    for cg in range(2 * R // 8):
        slots = [x2[k * 2 * R + cg * 8 : k * 2 * R + cg * 8 + 8, :] for k in range(digits)]
        slots = swap_bits(slots, [(k, bits + k) for k in range(n2)])
        for k, v in enumerate(slots):
            x3[k * 2 * R + cg * 8 : k * 2 * R + cg * 8 + 8, :] = v
    later[2].wait()
    z3 = mm3(w3, x3[...])
    x3[...] = z3
    for cg in range(2 * R // 8):
        slots = [x3[k * 2 * R + cg * 8 : k * 2 * R + cg * 8 + 8, :] for k in range(digits)]
        slots = swap_bits(slots, [(n2 - bits + k, k) for k in range(bits)])
        for k, v in enumerate(slots):
            x4[k // own * 2 * R + cg * 8 : k // own * 2 * R + cg * 8 + 8, k % own * LANES : (k % own + 1) * LANES] = v
    later[3].wait()
    z4 = mm3(w4, x4[...])
    for a in range(own):
        mine[:, a] = z4[:, a * LANES : (a + 1) * LANES].reshape(leaves, 2 * R, LANES)

    width = own * LANES
    cells = BOX_CELLS * 2**depth
    ticks = TOP_TICKS // 2**depth
    suffix = reverse_bits(me, bits)

    def ship(way, d):
        peer = xor(me, d, bits)
        return pltpu.make_async_remote_copy(
            src_ref=mine.at[reverse_bits(peer, bits)], dst_ref=coefs.at[blk_no, me],
            send_sem=send.at[way, d], recv_sem=recv.at[way, d],
            device_id=(peer, across if way else blk_no), device_id_type=mesh_id,
        )

    def relay(d):
        here = coefs.at[blk_no, xor(me, d, bits)]
        return pltpu.make_async_remote_copy(
            src_ref=here, dst_ref=here, send_sem=send.at[1, d], recv_sem=recv.at[1, d],
            device_id=(me, across), device_id_type=mesh_id,
        )

    def forward(way, d):
        here = coefs.at[across if way else blk_no, xor(me, d, bits)]
        return pltpu.make_async_remote_copy(
            src_ref=here, dst_ref=here,
            send_sem=gsend.at[way, d], recv_sem=grecv.at[way, d],
            device_id=(me, beside), device_id_type=mesh_id,
        )

    pitch = ticks // LANES
    tilt = (blocks * cells - 1) / 2.0 * (pitch // 2) / 2.0**32
    cos_poly = fit_even(lambda y: np.cos(2 * np.pi * y), tilt, 3)
    sin_poly = fit_even(lambda y: np.sin(2 * np.pi * y) / y, tilt, 3)
    cos_poly = [c * tilt ** (2 * k) for k, c in enumerate(cos_poly)]
    sin_poly = [c * tilt ** (2 * k + 1) for k, c in enumerate(sin_poly)]
    below = lax.broadcasted_iota(jnp.int32, (rows, LANES), 0) * (own * leaves * ticks)

    def tables(chunk, slot):
        parts = [split_pair(jnp.concatenate([coefs[q, chunk, t] for q in range(blocks)], axis=0).T) for t in range(own)]
        hi, lo = [jnp.concatenate(part, axis=0) for part in zip(*parts)]
        lhs = jnp.concatenate([hi, lo, hi], axis=1)
        for p in range(DEGREE + 1):
            both = dot16(lhs, a_buf[:, 2 * p * LANES : 2 * (p + 1) * LANES])
            tab[slot, 2 * p] = both[:, :LANES]
            tab[slot, 2 * p + 1] = both[:, LANES:]

    def points(chunk, slot):
        first = pl.multiple_of(chunk * width, width)
        for i in range(width // rows):
            box = first + own * (i * rows % LANES) + i * rows // LANES
            base = (box * leaves + suffix) * ticks
            u = (tgt[pl.ds(box, rows, stride=own), :] - (below + base)).astype(jnp.float32)
            cell = (u * (1.0 / pitch) + (0.5 / pitch)).astype(jnp.int32)
            s = (u - cell.astype(jnp.float32) * pitch) * (2.0 / pitch) - 1.0
            got_at = [jnp.take_along_axis(tab[slot, n, i * rows : (i + 1) * rows, :], cell, axis=1)
                      for n in range(2 * (DEGREE + 1))]
            z = s * s
            powers = [None, s, z, z * s, z * z]
            re, im = [[got_at[2 * p + part] * powers[p] if p else got_at[part] for p in range(DEGREE + 1)]
                      for part in range(2)]
            re = (re[0] + re[1]) + (re[2] + re[3]) + re[4]
            im = (im[0] + im[1]) + (im[2] + im[3]) + im[4]
            pc, ps = horner(cos_poly, z), s * horner(sin_poly, z)
            out[pl.ds(2 * box, rows, stride=2 * own), :] = pc * re - ps * im
            out[pl.ds(2 * box + 1, rows, stride=2 * own), :] = pc * im + ps * re

    def put(d):
        span = pl.ds(pl.multiple_of(xor(me, d, bits) * (2 * width), 2 * width), 2 * width)
        return pltpu.make_async_copy(out.at[span], out_hbm.at[span], osem.at[d])

    order = list(range(leaves))
    near = leaves // 2
    for d in order:
        for way in range(2 if d < near else 1):
            if way or d:
                ship(way, d).start()
    coefs[blk_no, me] = mine[suffix]
    for step in range(leaves + 5):
        if step < leaves:
            d = order[step]
            if d:
                ship(0, d).wait_recv()
            forward(0, d).start()
            if d < near:
                ship(1, d).wait_recv()
                forward(1, d).start()
            else:
                relay(d).start()
        if 0 <= step - 3 < leaves and order[step - 3] >= near:
            d = order[step - 3]
            relay(d).wait_recv()
            forward(1, d).start()
        if step == 4:
            later[4].wait()
            later[5].wait()
        if 0 <= step - 4 < leaves:
            d = order[step - 4]
            for way in range(2):
                forward(way, d).wait_recv()
            tables(xor(me, d, bits), step % 2)
        if 0 <= step - 5:
            d = order[step - 5]
            points(xor(me, d, bits), (step - 1) % 2)
            put(d).start()
    for d in order:
        if d:
            for g in range(groups):
                shuffle(g, d).wait_send()
            ship(0, d).wait_send()
        (ship(1, d) if d < near else relay(d)).wait_send()
        for way in range(2):
            forward(way, d).wait_send()
        put(d).wait()


def whole_call(pos, strengths, ticks, leaves, blocks, depth):
    boxes = ticks.shape[0]
    digits = boxes // LANES
    groups = digits // 8
    own = digits // leaves
    n1, n2 = leaves.bit_length() - 1, digits.bit_length() - 1
    n, m = digits * 2 * R, leaves * 2 * R
    grid = split_rows(grid_matrix(depth, blocks))
    anywhere = pl.BlockSpec(memory_space=pl.ANY)
    dma = pltpu.SemaphoreType.DMA
    f32, bf16 = jnp.float32, jnp.bfloat16
    return pl.pallas_call(
        functools.partial(whole_kernel, digits=digits, leaves=leaves, blocks=blocks, depth=depth, rows=8),
        out_shape=jax.ShapeDtypeStruct((2 * boxes, TGT_BOX), f32),
        in_specs=[anywhere] * 8,
        out_specs=anywhere,
        scratch_shapes=[
            pltpu.VMEM((groups, LANES, 8, LANES), jnp.int32),
            pltpu.VMEM((2, groups, LANES, 8, LANES), f32),
            pltpu.VMEM((2, LANES, LANES), jnp.int32),
            pltpu.VMEM((2, LANES, LANES), f32),
            pltpu.VMEM((2, LANES, LANES), f32),
            pltpu.VMEM((digits, 2 * R, LANES), f32),
            pltpu.VMEM((2, m, m), bf16),
            pltpu.VMEM((2, n, n), bf16),
            pltpu.VMEM((2, n, n), bf16),
            pltpu.VMEM((2, m, m), bf16),
            pltpu.VMEM((groups, leaves, 2 * R, LANES), f32),
            pltpu.VMEM((groups, leaves, 2 * R, LANES), f32),
            pltpu.VMEM((n, LANES), f32),
            pltpu.VMEM((n, LANES), f32),
            pltpu.VMEM((m, own * LANES), f32),
            pltpu.VMEM((leaves, own, 2 * R, LANES), f32),
            pltpu.VMEM((boxes, TGT_BOX), jnp.int32),
            pltpu.VMEM((2 * boxes, TGT_BOX), f32),
            pltpu.VMEM(grid.shape, bf16),
            pltpu.VMEM((2, 2 * (DEGREE + 1), own * LANES, LANES), f32),
            pltpu.VMEM((blocks, leaves, own, 2 * R, LANES), f32),
            dma((3, groups)), dma((6,)), dma((groups, leaves)), dma((groups, leaves)),
            dma((2, leaves)), dma((2, leaves)), dma((2, leaves)), dma((2, leaves)), dma((leaves,)),
        ],
        compiler_params=pltpu.CompilerParams(collective_id=0, has_side_effects=True),
        name="whole",
    )(
        pos.reshape(LANES, groups, 8, LANES), strengths.reshape(2, LANES, groups, 8, LANES),
        two_parts(first_matrix(n1)), two_parts(radix_matrix(n1, n2)),
        two_parts(radix_matrix(n1 + n2, n2)), two_parts(radix_matrix(n1 + 2 * n2, n1)),
        grid, ticks,
    )


def local_two_shuffles(src_pos, strengths, tgt_pos):
    leaves, blocks = lax.axis_size("leaf"), lax.axis_size("blk")
    boxes = src_pos.shape[1] // PER_BOX
    depth = boxes.bit_length() - 1 + leaves.bit_length() - 1
    out = whole_call(src_pos, strengths, tgt_pos.reshape(boxes, TGT_BOX), leaves, blocks, depth)
    return out.reshape(boxes, 2, TGT_BOX).transpose(1, 0, 2).reshape(2, boxes * TGT_BOX)


def solution(mesh):
    def local(src_pos, strengths, tgt_pos):
        boxes = src_pos.shape[1] // PER_BOX
        digits = boxes // LANES
        fits = digits % 8 == 0 and digits == 2 * mesh.shape["leaf"] and mesh.shape["leaf"] * digits == LANES
        near = fits and mesh.shape["blk"] == 4
        run = local_two_shuffles if near else local_butterfly
        return run(src_pos, strengths, tgt_pos)

    return jax.shard_map(
        local,
        mesh=mesh,
        in_specs=(P("blk", "leaf"), P(None, "blk", "leaf"), P(("leaf", "blk"))),
        out_specs=P(None, ("leaf", "blk")),
        check_vma=False,
    )
```

```python
import functools
import math

import jax
import jax.numpy as jnp
import numpy as np
from jax import lax
from jax.experimental import pallas as pl
from jax.experimental.pallas import tpu as pltpu
from jax.sharding import PartitionSpec as P

R = 16
PER_BOX = 128
TGT_BOX = 128
BOX_CELLS = 128
TOP_TICKS = 201326592
LANES = 128
HIGHEST = lax.Precision.HIGHEST


def fit_even(values, span, count):
    u = 0.5 * span * span * (1.0 + np.cos(np.pi * (np.arange(400) + 0.5) / 400))
    cheb = np.polynomial.chebyshev.Chebyshev.fit(u, values(np.sqrt(u)), count - 1, domain=[0, span * span])
    return [float(c) for c in cheb.convert(kind=np.polynomial.Polynomial).coef]


COS_POLY = fit_even(lambda y: np.cos(np.pi * y), 0.5, 5)
SIN_POLY = fit_even(lambda y: np.sin(np.pi * y) / y, 0.5, 4)


def horner(coefs, u):
    out = u * coefs[-1] + coefs[-2]
    for c in coefs[-3::-1]:
        out = out * u + c
    return out


def cos_sin_turns(y):
    u = y * y
    c, s = horner(COS_POLY, u), y * horner(SIN_POLY, u)
    twice = s + s
    return 1.0 - twice * s, twice * c


def node_offsets(box_cells):
    node_index = np.arange(R)
    unit_nodes = (1.0 - np.cos(np.pi * (node_index + 0.5) / R)) / 2.0
    return np.floor(box_cells * unit_nodes).astype(np.int64)


def lagrange_values(node_pos, points):
    rows = []
    for row_node in range(node_pos.shape[0]):
        column = np.ones(points.shape[0])
        for other in range(node_pos.shape[0]):
            if other != row_node:
                column = column * (points - node_pos[other]) / (node_pos[row_node] - node_pos[other])
        rows.append(column)
    return np.stack(rows)


def as_real(m):
    return np.block([[m.real, -m.imag], [m.imag, m.real]])


def turn64(a, b):
    product = (a * b + 2**31) % 2**32 - 2**31
    return product * (2.0 * np.pi / 2.0**32)


@functools.cache
def step_matrix(level):
    cells = BOX_CELLS * 2**level
    child, parent = node_offsets(cells), node_offsets(2 * cells)
    inner = np.concatenate([child, child + cells])
    blend = lagrange_values(parent / (2.0 * cells), inner / (2.0 * cells)).reshape(R, 2, R)
    half = TOP_TICKS // 2 ** (level + 2)
    assert half * cells % 2**32 == 2**31
    out = np.zeros((2, 2, 2 * R, 2 * R))
    for e in range(2):
        phase = np.exp(1j * turn64(half if e else -half, child))
        for j in range(2):
            out[e, j] = as_real((-1.0) ** j * blend[:, j, :] * phase[None, :])
    return out


def radix_matrix(first, count):
    total = np.eye(2 * R)[None, None]
    for k in range(count):
        m = step_matrix(first + k)
        n = total.shape[0]
        new = np.zeros((2 * n, 2 * n, 2 * R, 2 * R))
        for a in range(n):
            for b in range(n):
                for e in range(2):
                    for j in range(2):
                        new[2 * a + e, b + j * n] = m[e, j] @ total[a, b]
        total = new
    n = total.shape[0]
    return total.transpose(0, 2, 1, 3).reshape(n * 2 * R, n * 2 * R)


DEGREE = 4


def fit_turn(theta):
    s = np.cos(np.pi * (np.arange(64) + 0.5) / 64)
    fit = np.polynomial.chebyshev.chebfit(s, np.exp(1j * s[:, None] * theta[None, :]), DEGREE)
    power = np.zeros((DEGREE + 1, DEGREE + 1))
    for n in range(DEGREE + 1):
        c = np.polynomial.chebyshev.cheb2poly(np.eye(DEGREE + 1)[n])
        power[: len(c), n] = c
    return power @ fit


@functools.cache
def grid_matrix(depth, blocks):
    cells = BOX_CELLS * 2**depth
    ticks = TOP_TICKS // 2**depth
    step = ticks // LANES
    assert step * LANES == ticks and step % 2 == 0
    nodes = (np.arange(blocks)[:, None] * cells + node_offsets(cells)[None, :]).reshape(-1)
    centers = np.arange(LANES) * step + step // 2 - ticks // 2
    phase = np.exp(1j * turn64(centers[None, :], nodes[:, None]))
    off = (nodes - (blocks * cells - 1) / 2.0) * (step // 2) * (2.0 * np.pi / 2.0**32)
    poly = fit_turn(off)
    out = np.zeros((blocks, 2, R, DEGREE + 1, 2, LANES))
    for p in range(DEGREE + 1):
        b = (poly[p][:, None] * phase).reshape(blocks, R, LANES)
        out[:, 0, :, p, 0], out[:, 0, :, p, 1] = b.real, b.imag
        out[:, 1, :, p, 0], out[:, 1, :, p, 1] = -b.imag, b.real
    return out.reshape(blocks * 2 * R, (DEGREE + 1) * 2 * LANES)


def split_rows(m):
    hi = m.astype(jnp.bfloat16)
    lo = (m - hi.astype(np.float64)).astype(jnp.bfloat16)
    return jnp.asarray(np.concatenate([hi, hi, lo], axis=0))


def leaf_matrix():
    nodes = node_offsets(BOX_CELLS)
    angles = np.pi * (np.arange(R) + 0.5) / R
    at_exact = lagrange_values(2.0 * nodes / BOX_CELLS - 1.0, np.cos(angles))
    cheb_at = np.stack([np.cos(n * angles) for n in range(R)])
    norm = np.where(np.arange(R) == 0, 1.0, 2.0) / R
    g = (norm[:, None] * (cheb_at @ at_exact.T)).astype(np.float32)
    wide = np.repeat(g.T, 8, axis=1)
    zero = np.zeros_like(wide)
    return np.block([[wide, zero], [zero, wide]]).astype(np.float32)


def leaf_kernel(pos_ref, str_ref, mix_ref, out_ref, p_t, re_t, im_t, *, digits):
    def turn_over(beta, slot):
        rows = pl.ds(beta, LANES, stride=digits)
        p_t[slot] = pos_ref[rows, :].T
        re_t[slot] = str_ref[0, rows, :].T
        im_t[slot] = str_ref[1, rows, :].T

    def tile(beta, carry):
        slot = lax.rem(beta, 2)
        turn_over(jnp.minimum(beta + 1, digits - 1), 1 - slot)
        zero = jnp.zeros((8, LANES), jnp.float32)
        acc = tuple((zero, zero) for _ in range(R))
        for i in range(PER_BOX // 8):
            acc = chunk(slot, i, acc)
        low, high = list(acc[: R // 2]), list(acc[R // 2 :])
        top = [high[0]]
        for k in range(1, R // 2):
            top.append(tuple(2.0 * h - m for h, m in zip(high[k], low[R // 2 - k])))
        both = low + top
        stack = jnp.concatenate([x for x, _ in both] + [y for _, y in both], axis=0)
        out_ref[beta] = jnp.dot(mix_ref[...], stack, precision=HIGHEST, preferred_element_type=jnp.float32)
        return carry

    def chunk(slot, i, acc):
        here = pl.ds(i * 8, 8)
        r = p_t[slot, here, :] & (BOX_CELLS - 1)
        turn = (r * (TOP_TICKS // 2)).astype(jnp.float32) * (2.0**-32)
        c, s = cos_sin_turns(turn)
        a, b = re_t[slot, here, :], im_t[slot, here, :]
        v = r.astype(jnp.float32) * (2.0 / BOX_CELLS) - 1.0
        v2 = v + v
        cheb = [None, v]
        for k in range(2, R // 2 + 1):
            cheb.append(v2 * v - 1.0 if k == 2 else v2 * cheb[-1] - cheb[-2])
        x, y = c * a - s * b, s * a + c * b
        out = []
        for part, (x, y) in enumerate([(x, y), (cheb[-1] * x, cheb[-1] * y)]):
            for k in range(R // 2):
                u, w = acc[part * (R // 2) + k]
                out.append((u + x, w + y) if k == 0 else (u + cheb[k] * x, w + cheb[k] * y))
        return tuple(out)

    turn_over(0, 0)
    lax.fori_loop(0, digits, tile, 0)


def leaf_call(pos, strengths):
    boxes = pos.shape[0]
    digits = boxes // LANES
    whole = pl.BlockSpec(memory_space=pltpu.VMEM)
    return pl.pallas_call(
        functools.partial(leaf_kernel, digits=digits),
        out_shape=jax.ShapeDtypeStruct((digits, 2 * R, LANES), jnp.float32),
        in_specs=[whole, whole, whole],
        out_specs=whole,
        scratch_shapes=[
            pltpu.VMEM((2, LANES, LANES), jnp.int32),
            pltpu.VMEM((2, LANES, LANES), jnp.float32),
            pltpu.VMEM((2, LANES, LANES), jnp.float32),
        ],
        name="leaf",
    )(pos, strengths, jnp.asarray(leaf_matrix()))


def finish_kernel(w_ref, tgt_hbm, m_ref, a_hbm, out_hbm, tgt, out, a_buf, tab, bufs, got, coefs,
                  send, recv, gsend, grecv, tsem, asem, osem, *, leaves, blocks, chunks, depth, rows):
    leaf_no, blk_no = lax.axis_index("leaf"), lax.axis_index("blk")
    bits = leaves.bit_length() - 1
    boxes = w_ref.shape[1]
    width = boxes // chunks
    tiles = width // LANES
    cells = BOX_CELLS * 2**depth
    ticks = TOP_TICKS // 2**depth
    sides = [leaf_no // 2**k % 2 for k in range(bits)]
    partners = [leaf_no + (1 - 2 * sides[k]) * 2**k for k in range(bits)]
    suffix = jnp.int32(0)
    for k in range(bits):
        suffix = 2 * suffix + sides[k]
    peers = [lax.rem(blk_no + d, blocks) for d in range(1, blocks)]
    fetch = pltpu.make_async_copy(tgt_hbm, tgt, tsem)
    fetch.start()
    load = pltpu.make_async_copy(a_hbm, a_buf, asem)
    load.start()

    barrier = pltpu.get_barrier_semaphore()
    for k in range(bits):
        pl.semaphore_signal(barrier, inc=1, device_id=(partners[k], blk_no), device_id_type=pl.DeviceIdType.MESH)
    for peer in peers:
        pl.semaphore_signal(barrier, inc=1, device_id=(leaf_no, peer), device_id_type=pl.DeviceIdType.MESH)
    pl.semaphore_wait(barrier, bits + blocks - 1)

    def own(stage, c):
        return w_ref.at[:, pl.ds(c * width, width)] if stage == 0 else bufs.at[stage - 1, c]

    def exchange(stage, c):
        return pltpu.make_async_remote_copy(
            src_ref=own(stage, c), dst_ref=got.at[stage, c],
            send_sem=send.at[stage, c], recv_sem=recv.at[stage, c],
            device_id=(partners[stage], blk_no), device_id_type=pl.DeviceIdType.MESH,
        )

    def spread(d, c):
        here = coefs.at[blk_no, pl.ds(c * tiles, tiles)]
        return pltpu.make_async_remote_copy(
            src_ref=here, dst_ref=here,
            send_sem=gsend.at[d - 1, c], recv_sem=grecv.at[d - 1, c],
            device_id=(leaf_no, peers[d - 1]), device_id_type=pl.DeviceIdType.MESH,
        )

    def combine(todo):
        for stage, c in todo:
            exchange(stage, c).wait_recv()
        results = []
        for stage, c in todo:
            pair = jnp.concatenate([own(stage, c)[...], got[stage, c]], axis=0)
            results.append(mm(m_ref[stage, sides[stage]], pair))
        for (stage, c), w in zip(todo, results):
            if stage < bits - 1:
                bufs[stage, c] = w
            else:
                for i in range(tiles):
                    coefs[blk_no, c * tiles + i] = w[:, i * LANES : (i + 1) * LANES]
        for stage, c in todo:
            if stage < bits - 1:
                exchange(stage + 1, c).start()
            else:
                for d in range(1, blocks):
                    spread(d, c).start()

    pitch = ticks // LANES
    tilt = (blocks * cells - 1) / 2.0 * (pitch // 2) / 2.0**32
    cos_poly = fit_even(lambda y: np.cos(2 * np.pi * y), tilt, 3)
    sin_poly = fit_even(lambda y: np.sin(2 * np.pi * y) / y, tilt, 3)
    cos_poly = [c * tilt ** (2 * k) for k, c in enumerate(cos_poly)]
    sin_poly = [c * tilt ** (2 * k + 1) for k, c in enumerate(sin_poly)]
    below = lax.broadcasted_iota(jnp.int32, (rows, LANES), 0) * (leaves * ticks)

    def evaluate(tile, carry):
        whole = jnp.concatenate([coefs[q, tile] for q in range(blocks)], axis=0).T
        hi = whole.astype(jnp.bfloat16)
        lo = (whole - hi.astype(jnp.float32)).astype(jnp.bfloat16)
        lhs = jnp.concatenate([hi, lo, hi], axis=1)
        for n in range(2 * (DEGREE + 1)):
            tab[n] = jnp.dot(lhs, a_buf[:, n * LANES : (n + 1) * LANES], preferred_element_type=jnp.float32)
        first = pl.multiple_of(tile * LANES, LANES)
        for i in range(LANES // rows):
            base = ((first + i * rows) * leaves + suffix) * ticks
            u = (tgt[pl.ds(first + i * rows, rows), :] - (below + base)).astype(jnp.float32)
            cell = (u * (1.0 / pitch) + (0.5 / pitch)).astype(jnp.int32)
            s = (u - cell.astype(jnp.float32) * pitch) * (2.0 / pitch) - 1.0
            got_at = [jnp.take_along_axis(tab[n, i * rows : (i + 1) * rows, :], cell, axis=1)
                      for n in range(2 * (DEGREE + 1))]
            re, im = got_at[-2], got_at[-1]
            for p in range(DEGREE - 1, -1, -1):
                re, im = re * s + got_at[2 * p], im * s + got_at[2 * p + 1]
            z = s * s
            pc, ps = horner(cos_poly, z), s * horner(sin_poly, z)
            out[pl.ds(2 * (first + i * rows), rows, stride=2), :] = pc * re - ps * im
            out[pl.ds(2 * (first + i * rows) + 1, rows, stride=2), :] = pc * im + ps * re
        return carry

    def put(c):
        span = pl.ds(2 * c * width, 2 * width)
        return pltpu.make_async_copy(out.at[span], out_hbm.at[span], osem.at[c])

    def field(c):
        if c == 0:
            fetch.wait()
            load.wait()
        for d in range(1, blocks):
            spread(d, c).wait_recv()
        lax.fori_loop(c * tiles, (c + 1) * tiles, evaluate, 0)
        put(c).start()

    ahead = min(3, chunks)
    for c in range(ahead):
        exchange(0, c).start()
    for step in range(chunks + bits):
        combine([(k, step - k) for k in range(bits - 1, -1, -1) if 0 <= step - k < chunks])
        if step + ahead < chunks:
            exchange(0, step + ahead).start()
        if step >= bits:
            field(step - bits)
    for c in range(chunks):
        for stage in range(bits):
            exchange(stage, c).wait_send()
        for d in range(1, blocks):
            spread(d, c).wait_send()
        put(c).wait()


def finish_call(weights, ticks, matrices, grid, leaves, blocks, depth, chunks):
    boxes = ticks.shape[0]
    bits = leaves.bit_length() - 1
    width = boxes // chunks
    whole = pl.BlockSpec(memory_space=pltpu.VMEM)
    anywhere = pl.BlockSpec(memory_space=pl.ANY)
    dma = pltpu.SemaphoreType.DMA
    return pl.pallas_call(
        functools.partial(finish_kernel, leaves=leaves, blocks=blocks, chunks=chunks, depth=depth, rows=8),
        out_shape=jax.ShapeDtypeStruct((2 * boxes, TGT_BOX), jnp.float32),
        in_specs=[whole, anywhere, whole, anywhere],
        out_specs=anywhere,
        scratch_shapes=[
            pltpu.VMEM((boxes, TGT_BOX), jnp.int32),
            pltpu.VMEM((2 * boxes, TGT_BOX), jnp.float32),
            pltpu.VMEM(grid.shape, jnp.bfloat16),
            pltpu.VMEM((2 * (DEGREE + 1), LANES, LANES), jnp.float32),
            pltpu.VMEM((bits - 1, chunks, 2 * R, width), jnp.float32),
            pltpu.VMEM((bits, chunks, 2 * R, width), jnp.float32),
            pltpu.VMEM((blocks, boxes // LANES, 2 * R, LANES), jnp.float32),
        ] + [
            dma((bits, chunks)), dma((bits, chunks)),
            dma((blocks - 1, chunks)), dma((blocks - 1, chunks)),
            dma, dma, dma((chunks,)),
        ],
        compiler_params=pltpu.CompilerParams(collective_id=0, has_side_effects=True),
        name="finish",
    )(weights, ticks, matrices, grid)


def table(m):
    return jnp.asarray(m.astype(np.float32))


def mm(a, b):
    return jnp.dot(a, b, precision=HIGHEST, preferred_element_type=jnp.float32)


def local_tree(leaf, boxes):
    low = leaf.shape[0]
    n1 = low.bit_length() - 1
    rest = boxes.bit_length() - 1 - n1
    n2 = rest - rest // 2
    n3 = rest - n2
    c = 2 * R
    y = mm(table(radix_matrix(0, n1)), leaf.reshape(low * c, -1))
    y = y.reshape(low, c, 2**n3, 2**n2).transpose(3, 1, 0, 2).reshape(2**n2 * c, -1)
    y = mm(table(radix_matrix(n1, n2)), y)
    y = y.reshape(2**n2, c, low, 2**n3).transpose(3, 1, 2, 0).reshape(2**n3 * c, -1)
    y = mm(table(radix_matrix(n1 + n2, n3)), y)
    return y.reshape(2**n3, c, low * 2**n2).transpose(1, 2, 0).reshape(c, boxes)


def local_butterfly(src_pos, strengths, tgt_pos):
    leaf_count = lax.axis_size("leaf")
    leaf_bits = leaf_count.bit_length() - 1
    boxes = src_pos.shape[1] // PER_BOX
    local_depth = boxes.bit_length() - 1
    leaf = leaf_call(src_pos.reshape(boxes, PER_BOX), strengths.reshape(2, boxes, PER_BOX))
    weights = local_tree(leaf, boxes)
    steps = np.stack([step_matrix(local_depth + k) for k in range(leaf_bits)])
    steps[:, 1] = steps[:, 1, ::-1]
    steps = np.concatenate([steps[:, :, 0], steps[:, :, 1]], axis=-1)
    out = finish_call(
        weights, tgt_pos.reshape(boxes, TGT_BOX), table(steps),
        split_rows(grid_matrix(local_depth + leaf_bits, lax.axis_size("blk"))), leaf_count, lax.axis_size("blk"),
        local_depth + leaf_bits, 8,
    )
    return out.reshape(boxes, 2, TGT_BOX).transpose(1, 0, 2).reshape(2, boxes * TGT_BOX)


def xor(a, d, bits):
    return sum(((a // 2**k % 2 + (d >> k) % 2) % 2) * 2**k for k in range(bits))


def reverse_bits(a, bits):
    return sum((a // 2**k % 2) * 2 ** (bits - 1 - k) for k in range(bits))


def split_pair(x):
    hi = x.astype(jnp.bfloat16)
    return hi, (x - hi.astype(jnp.float32)).astype(jnp.bfloat16)


def dot16(a, b):
    return jnp.dot(a, b, preferred_element_type=jnp.float32)


def far_first(leaves):
    half = leaves // 2
    return [1] + list(range(half, leaves)) + list(range(2, half)) if leaves > 2 else [1]


def two_parts(m):
    hi = m.astype(jnp.bfloat16)
    return jnp.asarray(np.stack([hi, (m - hi.astype(np.float64)).astype(jnp.bfloat16)]))


def moment_matrix():
    wide = leaf_matrix()
    g = wide[:R, : 8 * R : 8].astype(np.float64)
    half = R // 2
    q = np.zeros((R, R))
    for n in range(half):
        q[n, n] = 1.0
        q[half + n, half + n] = 2.0 if n else 1.0
        if n:
            q[half + n, half - n] = -1.0
    return np.kron(np.eye(2), g @ q)


def first_matrix(count):
    m = radix_matrix(0, count)
    return np.einsum("xbc,cd->xbd", m.reshape(m.shape[0], -1, 2 * R), moment_matrix()).reshape(m.shape)


def merge_rows(parts):
    row = lax.broadcasted_iota(jnp.int32, (8, LANES), 0)
    step = 1
    while len(parts) > 1:
        low = row // step % 2 == 0
        half = len(parts) // 2
        pairs = [(parts[2 * k], parts[2 * k + 1]) for k in range(half)]
        parts = [jnp.where(low, a, b) + pltpu.roll(jnp.where(low, b, a), step, 0) for a, b in pairs]
        step *= 2
    return parts[0]


def swap_bits(slots, pairs):
    lane = lax.broadcasted_iota(jnp.int32, (8, LANES), 1)
    slots = list(slots)
    for slot_bit, lane_bit in pairs:
        low = lane // 2**lane_bit % 2 == 0
        for k in range(len(slots)):
            if k >> slot_bit & 1 == 0:
                a, b = slots[k], slots[k + 2**slot_bit]
                slots[k] = jnp.where(low, a, pltpu.roll(b, 2**lane_bit, 1))
                slots[k + 2**slot_bit] = jnp.where(low, pltpu.roll(a, LANES - 2**lane_bit, 1), b)
    return slots


def mm3(w, x):
    hi, lo = split_pair(x)
    return dot16(w[0], hi) + dot16(w[0], lo) + dot16(w[1], hi)


def whole_kernel(pos_hbm, str_hbm, w1_hbm, w2_hbm, w3_hbm, w4_hbm, a_hbm, tgt_hbm, out,
                 pos, amp, p_t, re_t, im_t, stack, w1, w2, w3, w4, y, got, x2, x3, x4, mine,
                 tgt, a_buf, tab, coefs,
                 isem, wsem, send1, recv1, send, recv, gsend, grecv,
                 *, digits, leaves, blocks, depth, rows):
    me, blk_no = lax.axis_index("leaf"), lax.axis_index("blk")
    bits = leaves.bit_length() - 1
    own = digits // leaves
    mesh_id = pl.DeviceIdType.MESH
    across = lax.rem(blk_no + blocks // 2, blocks)
    beside = blk_no + 1 - 2 * (blk_no % 2)
    groups = digits // 8

    def take(g):
        return [
            pltpu.make_async_copy(pos_hbm.at[:, g], pos.at[g], isem.at[0, g]),
            pltpu.make_async_copy(str_hbm.at[0, :, g], amp.at[0, g], isem.at[1, g]),
            pltpu.make_async_copy(str_hbm.at[1, :, g], amp.at[1, g], isem.at[2, g]),
        ]

    later = [
        pltpu.make_async_copy(src, dst, wsem.at[k])
        for k, (src, dst) in enumerate([(w1_hbm, w1), (w2_hbm, w2), (w3_hbm, w3), (w4_hbm, w4), (a_hbm, a_buf), (tgt_hbm, tgt)])
    ]
    for g in range(groups):
        for copy in take(g):
            copy.start()
    barrier = pltpu.get_barrier_semaphore()
    signals = 0
    for d in range(leaves):
        for peer in ([blk_no] if d else [beside]) + ([across] if d < leaves // 2 else []):
            pl.semaphore_signal(barrier, inc=1, device_id=(xor(me, d, bits), peer), device_id_type=mesh_id)
            signals += 1

    cells_at = lax.broadcasted_iota(jnp.int32, (8, LANES), 1)
    cos_at, sin_at = cos_sin_turns((cells_at * (TOP_TICKS // 2)).astype(jnp.float32) * (2.0**-32))

    def turn_over(g, beta, slot):
        here = pl.ds(beta, LANES, stride=8)
        p_t[slot] = pos.reshape(groups, LANES * 8, LANES)[g, here, :].T
        re_t[slot] = amp.reshape(2, groups, LANES * 8, LANES)[0, g, here, :].T
        im_t[slot] = amp.reshape(2, groups, LANES * 8, LANES)[1, g, here, :].T

    def chunk(slot, i, acc):
        here = pl.ds(i * 8, 8)
        r = p_t[slot, here, :] & (BOX_CELLS - 1)
        c = jnp.take_along_axis(cos_at, r, axis=1)
        s = jnp.take_along_axis(sin_at, r, axis=1)
        a, b = re_t[slot, here, :], im_t[slot, here, :]
        v = r.astype(jnp.float32) * (2.0 / BOX_CELLS) - 1.0
        v2 = v + v
        cheb = [None, v]
        for k in range(2, R // 2 + 1):
            cheb.append(v2 * v - 1.0 if k == 2 else v2 * cheb[-1] - cheb[-2])
        x, z = c * a - s * b, s * a + c * b
        result = []
        for part, (x, z) in enumerate([(x, z), (cheb[-1] * x, cheb[-1] * z)]):
            for k in range(R // 2):
                u, w = acc[part * (R // 2) + k]
                result.append((u + x, w + z) if k == 0 else (u + cheb[k] * x, w + cheb[k] * z))
        return tuple(result)

    def shuffle(g, d):
        peer = xor(me, d, bits)
        return pltpu.make_async_remote_copy(
            src_ref=y.at[g, peer], dst_ref=got.at[g, me],
            send_sem=send1.at[g, d], recv_sem=recv1.at[g, d],
            device_id=(peer, blk_no), device_id_type=mesh_id,
        )

    for g in range(groups):
        for copy in take(g):
            copy.wait()
        if g == 0:
            for copy in later:
                copy.start()
        turn_over(g, 0, 0)

        def tile(beta, carry, g=g):
            slot = lax.rem(beta, 2)
            turn_over(g, jnp.minimum(beta + 1, 7), 1 - slot)
            zero = jnp.zeros((8, LANES), jnp.float32)
            acc = tuple((zero, zero) for _ in range(R))
            for i in range(PER_BOX // 8):
                acc = chunk(slot, i, acc)
            half = R // 2
            for part in range(2):
                for k in range(2):
                    stack[g * 8 + beta, (2 * part + k) * 8 : (2 * part + k + 1) * 8, :] = merge_rows(
                        [acc[k * half + n][part] for n in range(half)])
            return carry

        lax.fori_loop(0, 8, tile, 0)
        if g == 0:
            later[0].wait()
            pl.semaphore_wait(barrier, signals)
        y[g] = mm3(w1, stack[g * 8 : (g + 1) * 8].reshape(8 * 2 * R, LANES)).reshape(leaves, 2 * R, LANES)
        for d in far_first(leaves):
            shuffle(g, d).start()

    got[:, me] = y[:, me]
    for g in range(groups):
        for d in range(1, leaves):
            shuffle(g, d).wait_recv()

    n2 = digits.bit_length() - 1
    for cg in range(2 * R // 8):
        slots = [got[j, k, cg * 8 : cg * 8 + 8, :] for k in range(leaves) for j in range(own)]
        slots = swap_bits(slots, [(n2 - bits + k, k) for k in range(bits)])
        for k, v in enumerate(slots):
            x2[k * 2 * R + cg * 8 : k * 2 * R + cg * 8 + 8, :] = v
    later[1].wait()
    z2 = mm3(w2, x2[...])
    x2[...] = z2
    for cg in range(2 * R // 8):
        slots = [x2[k * 2 * R + cg * 8 : k * 2 * R + cg * 8 + 8, :] for k in range(digits)]
        slots = swap_bits(slots, [(k, bits + k) for k in range(n2)])
        for k, v in enumerate(slots):
            x3[k * 2 * R + cg * 8 : k * 2 * R + cg * 8 + 8, :] = v
    later[2].wait()
    z3 = mm3(w3, x3[...])
    x3[...] = z3
    for cg in range(2 * R // 8):
        slots = [x3[k * 2 * R + cg * 8 : k * 2 * R + cg * 8 + 8, :] for k in range(digits)]
        slots = swap_bits(slots, [(n2 - bits + k, k) for k in range(bits)])
        for k, v in enumerate(slots):
            x4[k // own * 2 * R + cg * 8 : k // own * 2 * R + cg * 8 + 8, k % own * LANES : (k % own + 1) * LANES] = v
    later[3].wait()
    z4 = mm3(w4, x4[...])
    for a in range(own):
        mine[:, a] = z4[:, a * LANES : (a + 1) * LANES].reshape(leaves, 2 * R, LANES)

    width = own * LANES
    cells = BOX_CELLS * 2**depth
    ticks = TOP_TICKS // 2**depth
    suffix = reverse_bits(me, bits)

    def ship(way, d):
        peer = xor(me, d, bits)
        return pltpu.make_async_remote_copy(
            src_ref=mine.at[reverse_bits(peer, bits)], dst_ref=coefs.at[blk_no, me],
            send_sem=send.at[way, d], recv_sem=recv.at[way, d],
            device_id=(peer, across if way else blk_no), device_id_type=mesh_id,
        )

    def relay(d):
        here = coefs.at[blk_no, xor(me, d, bits)]
        return pltpu.make_async_remote_copy(
            src_ref=here, dst_ref=here, send_sem=send.at[1, d], recv_sem=recv.at[1, d],
            device_id=(me, across), device_id_type=mesh_id,
        )

    def forward(way, d):
        here = coefs.at[across if way else blk_no, xor(me, d, bits)]
        return pltpu.make_async_remote_copy(
            src_ref=here, dst_ref=here,
            send_sem=gsend.at[way, d], recv_sem=grecv.at[way, d],
            device_id=(me, beside), device_id_type=mesh_id,
        )

    pitch = ticks // LANES
    tilt = (blocks * cells - 1) / 2.0 * (pitch // 2) / 2.0**32
    cos_poly = fit_even(lambda y: np.cos(2 * np.pi * y), tilt, 3)
    sin_poly = fit_even(lambda y: np.sin(2 * np.pi * y) / y, tilt, 3)
    cos_poly = [c * tilt ** (2 * k) for k, c in enumerate(cos_poly)]
    sin_poly = [c * tilt ** (2 * k + 1) for k, c in enumerate(sin_poly)]
    below = lax.broadcasted_iota(jnp.int32, (rows, LANES), 0) * (own * leaves * ticks)

    def tables(chunk, slot):
        parts = [split_pair(jnp.concatenate([coefs[q, chunk, t] for q in range(blocks)], axis=0).T) for t in range(own)]
        hi, lo = [jnp.concatenate(part, axis=0) for part in zip(*parts)]
        lhs = jnp.concatenate([hi, lo, hi], axis=1)
        for p in range(DEGREE + 1):
            both = dot16(lhs, a_buf[:, 2 * p * LANES : 2 * (p + 1) * LANES])
            tab[slot, 2 * p] = both[:, :LANES]
            tab[slot, 2 * p + 1] = both[:, LANES:]

    def points(chunk, slot):
        first = pl.multiple_of(chunk * width, width)
        for i in range(width // rows):
            box = first + own * (i * rows % LANES) + i * rows // LANES
            base = (box * leaves + suffix) * ticks
            u = (tgt[pl.ds(box, rows, stride=own), :] - (below + base)).astype(jnp.float32)
            cell = (u * (1.0 / pitch) + (0.5 / pitch)).astype(jnp.int32)
            s = (u - cell.astype(jnp.float32) * pitch) * (2.0 / pitch) - 1.0
            got_at = [jnp.take_along_axis(tab[slot, n, i * rows : (i + 1) * rows, :], cell, axis=1)
                      for n in range(2 * (DEGREE + 1))]
            z = s * s
            powers = [None, s, z, z * s, z * z]
            re, im = [[got_at[2 * p + part] * powers[p] if p else got_at[part] for p in range(DEGREE + 1)]
                      for part in range(2)]
            re = (re[0] + re[1]) + (re[2] + re[3]) + re[4]
            im = (im[0] + im[1]) + (im[2] + im[3]) + im[4]
            pc, ps = horner(cos_poly, z), s * horner(sin_poly, z)
            out[pl.ds(2 * box, rows, stride=2 * own), :] = pc * re - ps * im
            out[pl.ds(2 * box + 1, rows, stride=2 * own), :] = pc * im + ps * re

    order = list(range(leaves))
    near = leaves // 2
    for d in order:
        for way in range(2 if d < near else 1):
            if way or d:
                ship(way, d).start()
    coefs[blk_no, me] = mine[suffix]
    for step in range(leaves + 5):
        if step < leaves:
            d = order[step]
            if d:
                ship(0, d).wait_recv()
            forward(0, d).start()
            if d < near:
                ship(1, d).wait_recv()
                forward(1, d).start()
            else:
                relay(d).start()
        if 0 <= step - 3 < leaves and order[step - 3] >= near:
            d = order[step - 3]
            relay(d).wait_recv()
            forward(1, d).start()
        if step == 4:
            later[4].wait()
            later[5].wait()
        if 0 <= step - 4 < leaves:
            d = order[step - 4]
            for way in range(2):
                forward(way, d).wait_recv()
            tables(xor(me, d, bits), step % 2)
        if 0 <= step - 5:
            d = order[step - 5]
            points(xor(me, d, bits), (step - 1) % 2)
    for d in order:
        if d:
            for g in range(groups):
                shuffle(g, d).wait_send()
            ship(0, d).wait_send()
        (ship(1, d) if d < near else relay(d)).wait_send()
        for way in range(2):
            forward(way, d).wait_send()


def whole_call(pos, strengths, ticks, leaves, blocks, depth):
    boxes = ticks.shape[0]
    digits = boxes // LANES
    groups = digits // 8
    own = digits // leaves
    n1, n2 = leaves.bit_length() - 1, digits.bit_length() - 1
    n, m = digits * 2 * R, leaves * 2 * R
    grid = split_rows(grid_matrix(depth, blocks))
    anywhere = pl.BlockSpec(memory_space=pltpu.HBM)
    dma = pltpu.SemaphoreType.DMA
    f32, bf16 = jnp.float32, jnp.bfloat16
    return pl.pallas_call(
        functools.partial(whole_kernel, digits=digits, leaves=leaves, blocks=blocks, depth=depth, rows=8),
        out_shape=pltpu.VMEM((2 * boxes, TGT_BOX), f32),
        in_specs=[anywhere] * 8,
        out_specs=pl.BlockSpec(memory_space=pltpu.VMEM),
        scratch_shapes=[
            pltpu.VMEM((groups, LANES, 8, LANES), jnp.int32),
            pltpu.VMEM((2, groups, LANES, 8, LANES), f32),
            pltpu.VMEM((2, LANES, LANES), jnp.int32),
            pltpu.VMEM((2, LANES, LANES), f32),
            pltpu.VMEM((2, LANES, LANES), f32),
            pltpu.VMEM((digits, 2 * R, LANES), f32),
            pltpu.VMEM((2, m, m), bf16),
            pltpu.VMEM((2, n, n), bf16),
            pltpu.VMEM((2, n, n), bf16),
            pltpu.VMEM((2, m, m), bf16),
            pltpu.VMEM((groups, leaves, 2 * R, LANES), f32),
            pltpu.VMEM((groups, leaves, 2 * R, LANES), f32),
            pltpu.VMEM((n, LANES), f32),
            pltpu.VMEM((n, LANES), f32),
            pltpu.VMEM((m, own * LANES), f32),
            pltpu.VMEM((leaves, own, 2 * R, LANES), f32),
            pltpu.VMEM((boxes, TGT_BOX), jnp.int32),
            pltpu.VMEM(grid.shape, bf16),
            pltpu.VMEM((2, 2 * (DEGREE + 1), own * LANES, LANES), f32),
            pltpu.VMEM((blocks, leaves, own, 2 * R, LANES), f32),
            dma((3, groups)), dma((6,)), dma((groups, leaves)), dma((groups, leaves)),
            dma((2, leaves)), dma((2, leaves)), dma((2, leaves)), dma((2, leaves)),
        ],
        compiler_params=pltpu.CompilerParams(collective_id=0, has_side_effects=True, vmem_limit_bytes=60 * 10**6),
        name="whole",
    )(
        pos.reshape(LANES, groups, 8, LANES), strengths.reshape(2, LANES, groups, 8, LANES),
        two_parts(first_matrix(n1)), two_parts(radix_matrix(n1, n2)),
        two_parts(radix_matrix(n1 + n2, n2)), two_parts(radix_matrix(n1 + 2 * n2, n1)),
        grid, ticks,
    )


def hand_over(x_ref, out_hbm, sem):
    parts = sem.shape[0]
    size = x_ref.shape[0] // parts
    copies = [pltpu.make_async_copy(x_ref.at[pl.ds(k * size, size)], out_hbm.at[pl.ds(k * size, size)], sem.at[k])
              for k in range(parts)]
    for copy in copies:
        copy.start()
    for copy in copies:
        copy.wait()


def hand_over_call(x):
    return pl.pallas_call(
        hand_over,
        out_shape=jax.ShapeDtypeStruct(x.shape, x.dtype),
        in_specs=[pl.BlockSpec(memory_space=pltpu.VMEM)],
        out_specs=pl.BlockSpec(memory_space=pl.ANY),
        scratch_shapes=[pltpu.SemaphoreType.DMA((8,))],
        compiler_params=pltpu.CompilerParams(vmem_limit_bytes=16 * 2**20),
        name="hand_over",
    )(x)


def local_two_shuffles(src_pos, strengths, tgt_pos):
    leaves, blocks = lax.axis_size("leaf"), lax.axis_size("blk")
    boxes = src_pos.shape[1] // PER_BOX
    depth = boxes.bit_length() - 1 + leaves.bit_length() - 1
    out = whole_call(src_pos, strengths, tgt_pos.reshape(boxes, TGT_BOX), leaves, blocks, depth)
    out = hand_over_call(out)
    return out.reshape(boxes, 2, TGT_BOX).transpose(1, 0, 2).reshape(2, boxes * TGT_BOX)


def solution(mesh):
    def local(src_pos, strengths, tgt_pos):
        boxes = src_pos.shape[1] // PER_BOX
        digits = boxes // LANES
        fits = digits % 8 == 0 and digits == 2 * mesh.shape["leaf"] and mesh.shape["leaf"] * digits == LANES
        near = fits and mesh.shape["blk"] == 4
        run = local_two_shuffles if near else local_butterfly
        return run(src_pos, strengths, tgt_pos)

    return jax.shard_map(
        local,
        mesh=mesh,
        in_specs=(P("blk", "leaf"), P(None, "blk", "leaf"), P(("leaf", "blk"))),
        out_specs=P(None, ("leaf", "blk")),
        check_vma=False,
    )
```

```python
import functools
import math

import jax
import jax.numpy as jnp
import numpy as np
from jax import lax
from jax.experimental import pallas as pl
from jax.experimental.pallas import tpu as pltpu
from jax.sharding import PartitionSpec as P

R = 16
PER_BOX = 128
TGT_BOX = 128
BOX_CELLS = 128
TOP_TICKS = 201326592
LANES = 128
HIGHEST = lax.Precision.HIGHEST


def fit_even(values, span, count):
    u = 0.5 * span * span * (1.0 + np.cos(np.pi * (np.arange(400) + 0.5) / 400))
    cheb = np.polynomial.chebyshev.Chebyshev.fit(u, values(np.sqrt(u)), count - 1, domain=[0, span * span])
    return [float(c) for c in cheb.convert(kind=np.polynomial.Polynomial).coef]


COS_POLY = fit_even(lambda y: np.cos(np.pi * y), 0.5, 5)
SIN_POLY = fit_even(lambda y: np.sin(np.pi * y) / y, 0.5, 4)


def horner(coefs, u):
    out = u * coefs[-1] + coefs[-2]
    for c in coefs[-3::-1]:
        out = out * u + c
    return out


def cos_sin_turns(y):
    u = y * y
    c, s = horner(COS_POLY, u), y * horner(SIN_POLY, u)
    twice = s + s
    return 1.0 - twice * s, twice * c


def node_offsets(box_cells):
    node_index = np.arange(R)
    unit_nodes = (1.0 - np.cos(np.pi * (node_index + 0.5) / R)) / 2.0
    return np.floor(box_cells * unit_nodes).astype(np.int64)


def lagrange_values(node_pos, points):
    rows = []
    for row_node in range(node_pos.shape[0]):
        column = np.ones(points.shape[0])
        for other in range(node_pos.shape[0]):
            if other != row_node:
                column = column * (points - node_pos[other]) / (node_pos[row_node] - node_pos[other])
        rows.append(column)
    return np.stack(rows)


def as_real(m):
    return np.block([[m.real, -m.imag], [m.imag, m.real]])


def turn64(a, b):
    product = (a * b + 2**31) % 2**32 - 2**31
    return product * (2.0 * np.pi / 2.0**32)


@functools.cache
def step_matrix(level):
    cells = BOX_CELLS * 2**level
    child, parent = node_offsets(cells), node_offsets(2 * cells)
    inner = np.concatenate([child, child + cells])
    blend = lagrange_values(parent / (2.0 * cells), inner / (2.0 * cells)).reshape(R, 2, R)
    half = TOP_TICKS // 2 ** (level + 2)
    assert half * cells % 2**32 == 2**31
    out = np.zeros((2, 2, 2 * R, 2 * R))
    for e in range(2):
        phase = np.exp(1j * turn64(half if e else -half, child))
        for j in range(2):
            out[e, j] = as_real((-1.0) ** j * blend[:, j, :] * phase[None, :])
    return out


def radix_matrix(first, count):
    total = np.eye(2 * R)[None, None]
    for k in range(count):
        m = step_matrix(first + k)
        n = total.shape[0]
        new = np.zeros((2 * n, 2 * n, 2 * R, 2 * R))
        for a in range(n):
            for b in range(n):
                for e in range(2):
                    for j in range(2):
                        new[2 * a + e, b + j * n] = m[e, j] @ total[a, b]
        total = new
    n = total.shape[0]
    return total.transpose(0, 2, 1, 3).reshape(n * 2 * R, n * 2 * R)


DEGREE = 4


def fit_turn(theta):
    s = np.cos(np.pi * (np.arange(64) + 0.5) / 64)
    fit = np.polynomial.chebyshev.chebfit(s, np.exp(1j * s[:, None] * theta[None, :]), DEGREE)
    power = np.zeros((DEGREE + 1, DEGREE + 1))
    for n in range(DEGREE + 1):
        c = np.polynomial.chebyshev.cheb2poly(np.eye(DEGREE + 1)[n])
        power[: len(c), n] = c
    return power @ fit


@functools.cache
def grid_matrix(depth, blocks):
    cells = BOX_CELLS * 2**depth
    ticks = TOP_TICKS // 2**depth
    step = ticks // LANES
    assert step * LANES == ticks and step % 2 == 0
    nodes = (np.arange(blocks)[:, None] * cells + node_offsets(cells)[None, :]).reshape(-1)
    centers = np.arange(LANES) * step + step // 2 - ticks // 2
    phase = np.exp(1j * turn64(centers[None, :], nodes[:, None]))
    off = (nodes - (blocks * cells - 1) / 2.0) * (step // 2) * (2.0 * np.pi / 2.0**32)
    poly = fit_turn(off)
    out = np.zeros((blocks, 2, R, DEGREE + 1, 2, LANES))
    for p in range(DEGREE + 1):
        b = (poly[p][:, None] * phase).reshape(blocks, R, LANES)
        out[:, 0, :, p, 0], out[:, 0, :, p, 1] = b.real, b.imag
        out[:, 1, :, p, 0], out[:, 1, :, p, 1] = -b.imag, b.real
    return out.reshape(blocks * 2 * R, (DEGREE + 1) * 2 * LANES)


def split_rows(m):
    hi = m.astype(jnp.bfloat16)
    lo = (m - hi.astype(np.float64)).astype(jnp.bfloat16)
    return jnp.asarray(np.concatenate([hi, hi, lo], axis=0))


def leaf_matrix():
    nodes = node_offsets(BOX_CELLS)
    angles = np.pi * (np.arange(R) + 0.5) / R
    at_exact = lagrange_values(2.0 * nodes / BOX_CELLS - 1.0, np.cos(angles))
    cheb_at = np.stack([np.cos(n * angles) for n in range(R)])
    norm = np.where(np.arange(R) == 0, 1.0, 2.0) / R
    g = (norm[:, None] * (cheb_at @ at_exact.T)).astype(np.float32)
    wide = np.repeat(g.T, 8, axis=1)
    zero = np.zeros_like(wide)
    return np.block([[wide, zero], [zero, wide]]).astype(np.float32)


def leaf_kernel(pos_ref, str_ref, mix_ref, out_ref, p_t, re_t, im_t, *, digits):
    def turn_over(beta, slot):
        rows = pl.ds(beta, LANES, stride=digits)
        p_t[slot] = pos_ref[rows, :].T
        re_t[slot] = str_ref[0, rows, :].T
        im_t[slot] = str_ref[1, rows, :].T

    def tile(beta, carry):
        slot = lax.rem(beta, 2)
        turn_over(jnp.minimum(beta + 1, digits - 1), 1 - slot)
        zero = jnp.zeros((8, LANES), jnp.float32)
        acc = tuple((zero, zero) for _ in range(R))
        for i in range(PER_BOX // 8):
            acc = chunk(slot, i, acc)
        low, high = list(acc[: R // 2]), list(acc[R // 2 :])
        top = [high[0]]
        for k in range(1, R // 2):
            top.append(tuple(2.0 * h - m for h, m in zip(high[k], low[R // 2 - k])))
        both = low + top
        stack = jnp.concatenate([x for x, _ in both] + [y for _, y in both], axis=0)
        out_ref[beta] = jnp.dot(mix_ref[...], stack, precision=HIGHEST, preferred_element_type=jnp.float32)
        return carry

    def chunk(slot, i, acc):
        here = pl.ds(i * 8, 8)
        r = p_t[slot, here, :] & (BOX_CELLS - 1)
        turn = (r * (TOP_TICKS // 2)).astype(jnp.float32) * (2.0**-32)
        c, s = cos_sin_turns(turn)
        a, b = re_t[slot, here, :], im_t[slot, here, :]
        v = r.astype(jnp.float32) * (2.0 / BOX_CELLS) - 1.0
        v2 = v + v
        cheb = [None, v]
        for k in range(2, R // 2 + 1):
            cheb.append(v2 * v - 1.0 if k == 2 else v2 * cheb[-1] - cheb[-2])
        x, y = c * a - s * b, s * a + c * b
        out = []
        for part, (x, y) in enumerate([(x, y), (cheb[-1] * x, cheb[-1] * y)]):
            for k in range(R // 2):
                u, w = acc[part * (R // 2) + k]
                out.append((u + x, w + y) if k == 0 else (u + cheb[k] * x, w + cheb[k] * y))
        return tuple(out)

    turn_over(0, 0)
    lax.fori_loop(0, digits, tile, 0)


def leaf_call(pos, strengths):
    boxes = pos.shape[0]
    digits = boxes // LANES
    whole = pl.BlockSpec(memory_space=pltpu.VMEM)
    return pl.pallas_call(
        functools.partial(leaf_kernel, digits=digits),
        out_shape=jax.ShapeDtypeStruct((digits, 2 * R, LANES), jnp.float32),
        in_specs=[whole, whole, whole],
        out_specs=whole,
        scratch_shapes=[
            pltpu.VMEM((2, LANES, LANES), jnp.int32),
            pltpu.VMEM((2, LANES, LANES), jnp.float32),
            pltpu.VMEM((2, LANES, LANES), jnp.float32),
        ],
        name="leaf",
    )(pos, strengths, jnp.asarray(leaf_matrix()))


def finish_kernel(w_ref, tgt_hbm, m_ref, a_hbm, out_hbm, tgt, out, a_buf, tab, bufs, got, coefs,
                  send, recv, gsend, grecv, tsem, asem, osem, *, leaves, blocks, chunks, depth, rows):
    leaf_no, blk_no = lax.axis_index("leaf"), lax.axis_index("blk")
    bits = leaves.bit_length() - 1
    boxes = w_ref.shape[1]
    width = boxes // chunks
    tiles = width // LANES
    cells = BOX_CELLS * 2**depth
    ticks = TOP_TICKS // 2**depth
    sides = [leaf_no // 2**k % 2 for k in range(bits)]
    partners = [leaf_no + (1 - 2 * sides[k]) * 2**k for k in range(bits)]
    suffix = jnp.int32(0)
    for k in range(bits):
        suffix = 2 * suffix + sides[k]
    peers = [lax.rem(blk_no + d, blocks) for d in range(1, blocks)]
    fetch = pltpu.make_async_copy(tgt_hbm, tgt, tsem)
    fetch.start()
    load = pltpu.make_async_copy(a_hbm, a_buf, asem)
    load.start()

    barrier = pltpu.get_barrier_semaphore()
    for k in range(bits):
        pl.semaphore_signal(barrier, inc=1, device_id=(partners[k], blk_no), device_id_type=pl.DeviceIdType.MESH)
    for peer in peers:
        pl.semaphore_signal(barrier, inc=1, device_id=(leaf_no, peer), device_id_type=pl.DeviceIdType.MESH)
    pl.semaphore_wait(barrier, bits + blocks - 1)

    def own(stage, c):
        return w_ref.at[:, pl.ds(c * width, width)] if stage == 0 else bufs.at[stage - 1, c]

    def exchange(stage, c):
        return pltpu.make_async_remote_copy(
            src_ref=own(stage, c), dst_ref=got.at[stage, c],
            send_sem=send.at[stage, c], recv_sem=recv.at[stage, c],
            device_id=(partners[stage], blk_no), device_id_type=pl.DeviceIdType.MESH,
        )

    def spread(d, c):
        here = coefs.at[blk_no, pl.ds(c * tiles, tiles)]
        return pltpu.make_async_remote_copy(
            src_ref=here, dst_ref=here,
            send_sem=gsend.at[d - 1, c], recv_sem=grecv.at[d - 1, c],
            device_id=(leaf_no, peers[d - 1]), device_id_type=pl.DeviceIdType.MESH,
        )

    def combine(todo):
        for stage, c in todo:
            exchange(stage, c).wait_recv()
        results = []
        for stage, c in todo:
            pair = jnp.concatenate([own(stage, c)[...], got[stage, c]], axis=0)
            results.append(mm(m_ref[stage, sides[stage]], pair))
        for (stage, c), w in zip(todo, results):
            if stage < bits - 1:
                bufs[stage, c] = w
            else:
                for i in range(tiles):
                    coefs[blk_no, c * tiles + i] = w[:, i * LANES : (i + 1) * LANES]
        for stage, c in todo:
            if stage < bits - 1:
                exchange(stage + 1, c).start()
            else:
                for d in range(1, blocks):
                    spread(d, c).start()

    pitch = ticks // LANES
    tilt = (blocks * cells - 1) / 2.0 * (pitch // 2) / 2.0**32
    cos_poly = fit_even(lambda y: np.cos(2 * np.pi * y), tilt, 3)
    sin_poly = fit_even(lambda y: np.sin(2 * np.pi * y) / y, tilt, 3)
    cos_poly = [c * tilt ** (2 * k) for k, c in enumerate(cos_poly)]
    sin_poly = [c * tilt ** (2 * k + 1) for k, c in enumerate(sin_poly)]
    below = lax.broadcasted_iota(jnp.int32, (rows, LANES), 0) * (leaves * ticks)

    def evaluate(tile, carry):
        whole = jnp.concatenate([coefs[q, tile] for q in range(blocks)], axis=0).T
        hi = whole.astype(jnp.bfloat16)
        lo = (whole - hi.astype(jnp.float32)).astype(jnp.bfloat16)
        lhs = jnp.concatenate([hi, lo, hi], axis=1)
        for n in range(2 * (DEGREE + 1)):
            tab[n] = jnp.dot(lhs, a_buf[:, n * LANES : (n + 1) * LANES], preferred_element_type=jnp.float32)
        first = pl.multiple_of(tile * LANES, LANES)
        for i in range(LANES // rows):
            base = ((first + i * rows) * leaves + suffix) * ticks
            u = (tgt[pl.ds(first + i * rows, rows), :] - (below + base)).astype(jnp.float32)
            cell = (u * (1.0 / pitch) + (0.5 / pitch)).astype(jnp.int32)
            s = (u - cell.astype(jnp.float32) * pitch) * (2.0 / pitch) - 1.0
            got_at = [jnp.take_along_axis(tab[n, i * rows : (i + 1) * rows, :], cell, axis=1)
                      for n in range(2 * (DEGREE + 1))]
            re, im = got_at[-2], got_at[-1]
            for p in range(DEGREE - 1, -1, -1):
                re, im = re * s + got_at[2 * p], im * s + got_at[2 * p + 1]
            z = s * s
            pc, ps = horner(cos_poly, z), s * horner(sin_poly, z)
            out[pl.ds(2 * (first + i * rows), rows, stride=2), :] = pc * re - ps * im
            out[pl.ds(2 * (first + i * rows) + 1, rows, stride=2), :] = pc * im + ps * re
        return carry

    def put(c):
        span = pl.ds(2 * c * width, 2 * width)
        return pltpu.make_async_copy(out.at[span], out_hbm.at[span], osem.at[c])

    def field(c):
        if c == 0:
            fetch.wait()
            load.wait()
        for d in range(1, blocks):
            spread(d, c).wait_recv()
        lax.fori_loop(c * tiles, (c + 1) * tiles, evaluate, 0)
        put(c).start()

    ahead = min(3, chunks)
    for c in range(ahead):
        exchange(0, c).start()
    for step in range(chunks + bits):
        combine([(k, step - k) for k in range(bits - 1, -1, -1) if 0 <= step - k < chunks])
        if step + ahead < chunks:
            exchange(0, step + ahead).start()
        if step >= bits:
            field(step - bits)
    for c in range(chunks):
        for stage in range(bits):
            exchange(stage, c).wait_send()
        for d in range(1, blocks):
            spread(d, c).wait_send()
        put(c).wait()


def finish_call(weights, ticks, matrices, grid, leaves, blocks, depth, chunks):
    boxes = ticks.shape[0]
    bits = leaves.bit_length() - 1
    width = boxes // chunks
    whole = pl.BlockSpec(memory_space=pltpu.VMEM)
    anywhere = pl.BlockSpec(memory_space=pl.ANY)
    dma = pltpu.SemaphoreType.DMA
    return pl.pallas_call(
        functools.partial(finish_kernel, leaves=leaves, blocks=blocks, chunks=chunks, depth=depth, rows=8),
        out_shape=jax.ShapeDtypeStruct((2 * boxes, TGT_BOX), jnp.float32),
        in_specs=[whole, anywhere, whole, anywhere],
        out_specs=anywhere,
        scratch_shapes=[
            pltpu.VMEM((boxes, TGT_BOX), jnp.int32),
            pltpu.VMEM((2 * boxes, TGT_BOX), jnp.float32),
            pltpu.VMEM(grid.shape, jnp.bfloat16),
            pltpu.VMEM((2 * (DEGREE + 1), LANES, LANES), jnp.float32),
            pltpu.VMEM((bits - 1, chunks, 2 * R, width), jnp.float32),
            pltpu.VMEM((bits, chunks, 2 * R, width), jnp.float32),
            pltpu.VMEM((blocks, boxes // LANES, 2 * R, LANES), jnp.float32),
        ] + [
            dma((bits, chunks)), dma((bits, chunks)),
            dma((blocks - 1, chunks)), dma((blocks - 1, chunks)),
            dma, dma, dma((chunks,)),
        ],
        compiler_params=pltpu.CompilerParams(collective_id=0, has_side_effects=True),
        name="finish",
    )(weights, ticks, matrices, grid)


def table(m):
    return jnp.asarray(m.astype(np.float32))


def mm(a, b):
    return jnp.dot(a, b, precision=HIGHEST, preferred_element_type=jnp.float32)


def local_tree(leaf, boxes):
    low = leaf.shape[0]
    n1 = low.bit_length() - 1
    rest = boxes.bit_length() - 1 - n1
    n2 = rest - rest // 2
    n3 = rest - n2
    c = 2 * R
    y = mm(table(radix_matrix(0, n1)), leaf.reshape(low * c, -1))
    y = y.reshape(low, c, 2**n3, 2**n2).transpose(3, 1, 0, 2).reshape(2**n2 * c, -1)
    y = mm(table(radix_matrix(n1, n2)), y)
    y = y.reshape(2**n2, c, low, 2**n3).transpose(3, 1, 2, 0).reshape(2**n3 * c, -1)
    y = mm(table(radix_matrix(n1 + n2, n3)), y)
    return y.reshape(2**n3, c, low * 2**n2).transpose(1, 2, 0).reshape(c, boxes)


def local_butterfly(src_pos, strengths, tgt_pos):
    leaf_count = lax.axis_size("leaf")
    leaf_bits = leaf_count.bit_length() - 1
    boxes = src_pos.shape[1] // PER_BOX
    local_depth = boxes.bit_length() - 1
    leaf = leaf_call(src_pos.reshape(boxes, PER_BOX), strengths.reshape(2, boxes, PER_BOX))
    weights = local_tree(leaf, boxes)
    steps = np.stack([step_matrix(local_depth + k) for k in range(leaf_bits)])
    steps[:, 1] = steps[:, 1, ::-1]
    steps = np.concatenate([steps[:, :, 0], steps[:, :, 1]], axis=-1)
    out = finish_call(
        weights, tgt_pos.reshape(boxes, TGT_BOX), table(steps),
        split_rows(grid_matrix(local_depth + leaf_bits, lax.axis_size("blk"))), leaf_count, lax.axis_size("blk"),
        local_depth + leaf_bits, 8,
    )
    return out.reshape(boxes, 2, TGT_BOX).transpose(1, 0, 2).reshape(2, boxes * TGT_BOX)


def xor(a, d, bits):
    return sum(((a // 2**k % 2 + (d >> k) % 2) % 2) * 2**k for k in range(bits))


def reverse_bits(a, bits):
    return sum((a // 2**k % 2) * 2 ** (bits - 1 - k) for k in range(bits))


def split_pair(x):
    hi = x.astype(jnp.bfloat16)
    return hi, (x - hi.astype(jnp.float32)).astype(jnp.bfloat16)


def dot16(a, b):
    return jnp.dot(a, b, preferred_element_type=jnp.float32)


def far_first(leaves):
    half = leaves // 2
    return [1] + list(range(half, leaves)) + list(range(2, half)) if leaves > 2 else [1]


def two_parts(m):
    hi = m.astype(jnp.bfloat16)
    return jnp.asarray(np.stack([hi, (m - hi.astype(np.float64)).astype(jnp.bfloat16)]))


def moment_matrix():
    wide = leaf_matrix()
    g = wide[:R, : 8 * R : 8].astype(np.float64)
    half = R // 2
    q = np.zeros((R, R))
    for n in range(half):
        q[n, n] = 1.0
        q[half + n, half + n] = 2.0 if n else 1.0
        if n:
            q[half + n, half - n] = -1.0
    return np.kron(np.eye(2), g @ q)


def first_matrix(count):
    m = radix_matrix(0, count)
    return np.einsum("xbc,cd->xbd", m.reshape(m.shape[0], -1, 2 * R), moment_matrix()).reshape(m.shape)


def merge_rows(parts):
    row = lax.broadcasted_iota(jnp.int32, (8, LANES), 0)
    step = 1
    while len(parts) > 1:
        low = row // step % 2 == 0
        half = len(parts) // 2
        pairs = [(parts[2 * k], parts[2 * k + 1]) for k in range(half)]
        parts = [jnp.where(low, a, b) + pltpu.roll(jnp.where(low, b, a), step, 0) for a, b in pairs]
        step *= 2
    return parts[0]


def swap_bits(slots, pairs):
    lane = lax.broadcasted_iota(jnp.int32, (8, LANES), 1)
    slots = list(slots)
    for slot_bit, lane_bit in pairs:
        low = lane // 2**lane_bit % 2 == 0
        for k in range(len(slots)):
            if k >> slot_bit & 1 == 0:
                a, b = slots[k], slots[k + 2**slot_bit]
                slots[k] = jnp.where(low, a, pltpu.roll(b, 2**lane_bit, 1))
                slots[k + 2**slot_bit] = jnp.where(low, pltpu.roll(a, LANES - 2**lane_bit, 1), b)
    return slots


def mm3(w, x):
    hi, lo = split_pair(x)
    return dot16(w[0], hi) + dot16(w[0], lo) + dot16(w[1], hi)


def whole_kernel(pos_hbm, str_hbm, w1_hbm, w2_hbm, w3_hbm, w4_hbm, a_hbm, tgt_hbm, out,
                 pos, amp, p_t, re_t, im_t, stack, w1, w2, w3, w4, y, got, x2, x3, x4, mine,
                 tgt, a_buf, tab, coefs,
                 isem, wsem, send1, recv1, send, recv, gsend, grecv,
                 *, digits, leaves, blocks, depth, rows):
    me, blk_no = lax.axis_index("leaf"), lax.axis_index("blk")
    bits = leaves.bit_length() - 1
    own = digits // leaves
    mesh_id = pl.DeviceIdType.MESH
    across = lax.rem(blk_no + blocks // 2, blocks)
    beside = blk_no + 1 - 2 * (blk_no % 2)
    groups = digits // 8

    def take(g):
        return [
            pltpu.make_async_copy(pos_hbm.at[:, g], pos.at[g], isem.at[0, g]),
            pltpu.make_async_copy(str_hbm.at[0, :, g], amp.at[0, g], isem.at[1, g]),
            pltpu.make_async_copy(str_hbm.at[1, :, g], amp.at[1, g], isem.at[2, g]),
        ]

    later = [
        pltpu.make_async_copy(src, dst, wsem.at[k])
        for k, (src, dst) in enumerate([(w1_hbm, w1), (w2_hbm, w2), (w3_hbm, w3), (w4_hbm, w4), (a_hbm, a_buf), (tgt_hbm, tgt)])
    ]
    for copy in take(0):
        copy.start()
    barrier = pltpu.get_barrier_semaphore()
    signals = 0
    for d in range(leaves):
        for peer in ([blk_no] if d else [beside]) + ([across] if d < leaves // 2 else []):
            pl.semaphore_signal(barrier, inc=1, device_id=(xor(me, d, bits), peer), device_id_type=mesh_id)
            signals += 1

    cells_at = lax.broadcasted_iota(jnp.int32, (8, LANES), 1)
    cos_at, sin_at = cos_sin_turns((cells_at * (TOP_TICKS // 2)).astype(jnp.float32) * (2.0**-32))

    def turn_over(g, beta, slot):
        here = pl.ds(beta, LANES, stride=8)
        p_t[slot] = pos.reshape(groups, LANES * 8, LANES)[g, here, :].T
        re_t[slot] = amp.reshape(2, groups, LANES * 8, LANES)[0, g, here, :].T
        im_t[slot] = amp.reshape(2, groups, LANES * 8, LANES)[1, g, here, :].T

    def chunk(slot, i, acc):
        here = pl.ds(i * 8, 8)
        r = p_t[slot, here, :] & (BOX_CELLS - 1)
        c = jnp.take_along_axis(cos_at, r, axis=1)
        s = jnp.take_along_axis(sin_at, r, axis=1)
        a, b = re_t[slot, here, :], im_t[slot, here, :]
        v = r.astype(jnp.float32) * (2.0 / BOX_CELLS) - 1.0
        v2 = v + v
        cheb = [None, v]
        for k in range(2, R // 2 + 1):
            cheb.append(v2 * v - 1.0 if k == 2 else v2 * cheb[-1] - cheb[-2])
        x, z = c * a - s * b, s * a + c * b
        result = []
        for part, (x, z) in enumerate([(x, z), (cheb[-1] * x, cheb[-1] * z)]):
            for k in range(R // 2):
                u, w = acc[part * (R // 2) + k]
                result.append((u + x, w + z) if k == 0 else (u + cheb[k] * x, w + cheb[k] * z))
        return tuple(result)

    def shuffle(g, d):
        peer = xor(me, d, bits)
        return pltpu.make_async_remote_copy(
            src_ref=y.at[g, peer], dst_ref=got.at[g, me],
            send_sem=send1.at[g, d], recv_sem=recv1.at[g, d],
            device_id=(peer, blk_no), device_id_type=mesh_id,
        )

    for g in range(groups):
        for copy in take(g):
            copy.wait()
        if g == 0:
            for copy in [copy for h in range(1, groups) for copy in take(h)] + later:
                copy.start()
        turn_over(g, 0, 0)

        def tile(beta, carry, g=g):
            slot = lax.rem(beta, 2)
            turn_over(g, jnp.minimum(beta + 1, 7), 1 - slot)
            zero = jnp.zeros((8, LANES), jnp.float32)
            acc = tuple((zero, zero) for _ in range(R))
            for i in range(PER_BOX // 8):
                acc = chunk(slot, i, acc)
            half = R // 2
            for part in range(2):
                for k in range(2):
                    stack[g * 8 + beta, (2 * part + k) * 8 : (2 * part + k + 1) * 8, :] = merge_rows(
                        [acc[k * half + n][part] for n in range(half)])
            return carry

        lax.fori_loop(0, 8, tile, 0)
        if g == 0:
            later[0].wait()
            pl.semaphore_wait(barrier, signals)
        y[g] = mm3(w1, stack[g * 8 : (g + 1) * 8].reshape(8 * 2 * R, LANES)).reshape(leaves, 2 * R, LANES)
        for d in far_first(leaves):
            shuffle(g, d).start()

    n2 = digits.bit_length() - 1
    for j in range(own):
        got[j, me] = y[j, me]
        for d in range(1, leaves):
            shuffle(j, d).wait_recv()
        for cg in range(2 * R // 8):
            slots = [got[j, k, cg * 8 : cg * 8 + 8, :] for k in range(leaves)]
            slots = swap_bits(slots, [(k, k) for k in range(bits)])
            for k, v in enumerate(slots):
                first = (j * leaves + k) * 2 * R + cg * 8
                x2[first : first + 8, :] = v
        if j == 0:
            later[1].wait()
        span = slice(j * leaves * 2 * R, (j + 1) * leaves * 2 * R)
        term = mm3((w2[0, :, span], w2[1, :, span]), x2[span, :])
        if j < own - 1:
            x3[...] = term if j == 0 else x3[...] + term
    z2 = x3[...] + term
    x2[...] = z2
    for cg in range(2 * R // 8):
        slots = [x2[k * 2 * R + cg * 8 : k * 2 * R + cg * 8 + 8, :] for k in range(digits)]
        slots = swap_bits(slots, [(k, bits + k) for k in range(n2)])
        for k, v in enumerate(slots):
            x3[k * 2 * R + cg * 8 : k * 2 * R + cg * 8 + 8, :] = v
    later[2].wait()
    z3 = mm3(w3, x3[...])
    x3[...] = z3
    for cg in range(2 * R // 8):
        slots = [x3[k * 2 * R + cg * 8 : k * 2 * R + cg * 8 + 8, :] for k in range(digits)]
        slots = swap_bits(slots, [(n2 - bits + k, k) for k in range(bits)])
        for k, v in enumerate(slots):
            x4[k // own * 2 * R + cg * 8 : k // own * 2 * R + cg * 8 + 8, k % own * LANES : (k % own + 1) * LANES] = v
    later[3].wait()
    z4 = mm3(w4, x4[...])
    for a in range(own):
        mine[:, a] = z4[:, a * LANES : (a + 1) * LANES].reshape(leaves, 2 * R, LANES)

    width = own * LANES
    cells = BOX_CELLS * 2**depth
    ticks = TOP_TICKS // 2**depth
    suffix = reverse_bits(me, bits)

    def ship(way, d):
        peer = xor(me, d, bits)
        return pltpu.make_async_remote_copy(
            src_ref=mine.at[reverse_bits(peer, bits)], dst_ref=coefs.at[blk_no, me],
            send_sem=send.at[way, d], recv_sem=recv.at[way, d],
            device_id=(peer, across if way else blk_no), device_id_type=mesh_id,
        )

    def relay(d):
        here = coefs.at[blk_no, xor(me, d, bits)]
        return pltpu.make_async_remote_copy(
            src_ref=here, dst_ref=here, send_sem=send.at[1, d], recv_sem=recv.at[1, d],
            device_id=(me, across), device_id_type=mesh_id,
        )

    def forward(way, d):
        here = coefs.at[across if way else blk_no, xor(me, d, bits)]
        return pltpu.make_async_remote_copy(
            src_ref=here, dst_ref=here,
            send_sem=gsend.at[way, d], recv_sem=grecv.at[way, d],
            device_id=(me, beside), device_id_type=mesh_id,
        )

    pitch = ticks // LANES
    tilt = (blocks * cells - 1) / 2.0 * (pitch // 2) / 2.0**32
    cos_poly = fit_even(lambda y: np.cos(2 * np.pi * y), tilt, 3)
    sin_poly = fit_even(lambda y: np.sin(2 * np.pi * y) / y, tilt, 3)
    cos_poly = [c * tilt ** (2 * k) for k, c in enumerate(cos_poly)]
    sin_poly = [c * tilt ** (2 * k + 1) for k, c in enumerate(sin_poly)]
    below = lax.broadcasted_iota(jnp.int32, (rows, LANES), 0) * (own * leaves * ticks)

    def tables(chunk, slot):
        parts = [split_pair(jnp.concatenate([coefs[q, chunk, t] for q in range(blocks)], axis=0).T) for t in range(own)]
        hi, lo = [jnp.concatenate(part, axis=0) for part in zip(*parts)]
        lhs = jnp.concatenate([hi, lo, hi], axis=1)
        for p in range(DEGREE + 1):
            both = dot16(lhs, a_buf[:, 2 * p * LANES : 2 * (p + 1) * LANES])
            tab[slot, 2 * p] = both[:, :LANES]
            tab[slot, 2 * p + 1] = both[:, LANES:]

    def points(chunk, slot):
        first = pl.multiple_of(chunk * width, width)
        for i in range(width // rows):
            box = first + own * (i * rows % LANES) + i * rows // LANES
            base = (box * leaves + suffix) * ticks
            u = (tgt[pl.ds(box, rows, stride=own), :] - (below + base)).astype(jnp.float32)
            cell = (u * (1.0 / pitch) + (0.5 / pitch)).astype(jnp.int32)
            s = (u - cell.astype(jnp.float32) * pitch) * (2.0 / pitch) - 1.0
            got_at = [jnp.take_along_axis(tab[slot, n, i * rows : (i + 1) * rows, :], cell, axis=1)
                      for n in range(2 * (DEGREE + 1))]
            z = s * s
            powers = [None, s, z, z * s, z * z]
            re, im = [[got_at[2 * p + part] * powers[p] if p else got_at[part] for p in range(DEGREE + 1)]
                      for part in range(2)]
            re = (re[0] + re[1]) + (re[2] + re[3]) + re[4]
            im = (im[0] + im[1]) + (im[2] + im[3]) + im[4]
            pc, ps = horner(cos_poly, z), s * horner(sin_poly, z)
            out[pl.ds(2 * box, rows, stride=2 * own), :] = pc * re - ps * im
            out[pl.ds(2 * box + 1, rows, stride=2 * own), :] = pc * im + ps * re

    order = list(range(leaves))
    near = leaves // 2
    for d in order:
        for way in range(2 if d < near else 1):
            if way or d:
                ship(way, d).start()
    coefs[blk_no, me] = mine[suffix]
    for step in range(leaves + 6):
        if step < leaves:
            d = order[step]
            if d:
                ship(0, d).wait_recv()
            forward(0, d).start()
            if d < near:
                ship(1, d).wait_recv()
                forward(1, d).start()
            else:
                relay(d).start()
        if 0 <= step - 4 < leaves and order[step - 4] >= near:
            d = order[step - 4]
            relay(d).wait_recv()
            forward(1, d).start()
        if step == 5:
            later[4].wait()
            later[5].wait()
        if 0 <= step - 5 < leaves:
            d = order[step - 5]
            for way in range(2):
                forward(way, d).wait_recv()
            tables(xor(me, d, bits), step % 2)
        if 0 <= step - 6:
            d = order[step - 6]
            points(xor(me, d, bits), (step - 1) % 2)
    for d in order:
        if d:
            for g in range(groups):
                shuffle(g, d).wait_send()
            ship(0, d).wait_send()
        (ship(1, d) if d < near else relay(d)).wait_send()
        for way in range(2):
            forward(way, d).wait_send()


def halves_first(m, own):
    rows = m.shape[0]
    return m.reshape(rows, -1, own, 2 * R).transpose(0, 2, 1, 3).reshape(rows, -1)


def whole_call(pos, strengths, ticks, leaves, blocks, depth):
    boxes = ticks.shape[0]
    digits = boxes // LANES
    groups = digits // 8
    own = digits // leaves
    n1, n2 = leaves.bit_length() - 1, digits.bit_length() - 1
    n, m = digits * 2 * R, leaves * 2 * R
    grid = split_rows(grid_matrix(depth, blocks))
    anywhere = pl.BlockSpec(memory_space=pltpu.HBM)
    dma = pltpu.SemaphoreType.DMA
    f32, bf16 = jnp.float32, jnp.bfloat16
    return pl.pallas_call(
        functools.partial(whole_kernel, digits=digits, leaves=leaves, blocks=blocks, depth=depth, rows=8),
        out_shape=pltpu.VMEM((2 * boxes, TGT_BOX), f32),
        in_specs=[anywhere] * 8,
        out_specs=pl.BlockSpec(memory_space=pltpu.VMEM),
        scratch_shapes=[
            pltpu.VMEM((groups, LANES, 8, LANES), jnp.int32),
            pltpu.VMEM((2, groups, LANES, 8, LANES), f32),
            pltpu.VMEM((2, LANES, LANES), jnp.int32),
            pltpu.VMEM((2, LANES, LANES), f32),
            pltpu.VMEM((2, LANES, LANES), f32),
            pltpu.VMEM((digits, 2 * R, LANES), f32),
            pltpu.VMEM((2, m, m), bf16),
            pltpu.VMEM((2, n, n), bf16),
            pltpu.VMEM((2, n, n), bf16),
            pltpu.VMEM((2, m, m), bf16),
            pltpu.VMEM((groups, leaves, 2 * R, LANES), f32),
            pltpu.VMEM((groups, leaves, 2 * R, LANES), f32),
            pltpu.VMEM((n, LANES), f32),
            pltpu.VMEM((n, LANES), f32),
            pltpu.VMEM((m, own * LANES), f32),
            pltpu.VMEM((leaves, own, 2 * R, LANES), f32),
            pltpu.VMEM((boxes, TGT_BOX), jnp.int32),
            pltpu.VMEM(grid.shape, bf16),
            pltpu.VMEM((2, 2 * (DEGREE + 1), own * LANES, LANES), f32),
            pltpu.VMEM((blocks, leaves, own, 2 * R, LANES), f32),
            dma((3, groups)), dma((6,)), dma((groups, leaves)), dma((groups, leaves)),
            dma((2, leaves)), dma((2, leaves)), dma((2, leaves)), dma((2, leaves)),
        ],
        compiler_params=pltpu.CompilerParams(collective_id=0, has_side_effects=True, vmem_limit_bytes=60 * 10**6),
        name="whole",
    )(
        pos.reshape(LANES, groups, 8, LANES), strengths.reshape(2, LANES, groups, 8, LANES),
        two_parts(first_matrix(n1)), two_parts(halves_first(radix_matrix(n1, n2), own)),
        two_parts(radix_matrix(n1 + n2, n2)), two_parts(radix_matrix(n1 + 2 * n2, n1)),
        grid, ticks,
    )


def hand_over(x_ref, out_hbm, sem):
    parts = sem.shape[0]
    size = x_ref.shape[0] // parts
    copies = [pltpu.make_async_copy(x_ref.at[pl.ds(k * size, size)], out_hbm.at[pl.ds(k * size, size)], sem.at[k])
              for k in range(parts)]
    for copy in copies:
        copy.start()
    for copy in copies:
        copy.wait()


def hand_over_call(x):
    return pl.pallas_call(
        hand_over,
        out_shape=jax.ShapeDtypeStruct(x.shape, x.dtype),
        in_specs=[pl.BlockSpec(memory_space=pltpu.VMEM)],
        out_specs=pl.BlockSpec(memory_space=pl.ANY),
        scratch_shapes=[pltpu.SemaphoreType.DMA((8,))],
        compiler_params=pltpu.CompilerParams(vmem_limit_bytes=16 * 2**20),
        name="hand_over",
    )(x)


def local_two_shuffles(src_pos, strengths, tgt_pos):
    leaves, blocks = lax.axis_size("leaf"), lax.axis_size("blk")
    boxes = src_pos.shape[1] // PER_BOX
    depth = boxes.bit_length() - 1 + leaves.bit_length() - 1
    out = whole_call(src_pos, strengths, tgt_pos.reshape(boxes, TGT_BOX), leaves, blocks, depth)
    out = hand_over_call(out)
    return out.reshape(boxes, 2, TGT_BOX).transpose(1, 0, 2).reshape(2, boxes * TGT_BOX)


def solution(mesh):
    def local(src_pos, strengths, tgt_pos):
        boxes = src_pos.shape[1] // PER_BOX
        digits = boxes // LANES
        fits = digits % 8 == 0 and digits == 2 * mesh.shape["leaf"] and mesh.shape["leaf"] * digits == LANES
        near = fits and mesh.shape["blk"] == 4
        run = local_two_shuffles if near else local_butterfly
        return run(src_pos, strengths, tgt_pos)

    return jax.shard_map(
        local,
        mesh=mesh,
        in_specs=(P("blk", "leaf"), P(None, "blk", "leaf"), P(("leaf", "blk"))),
        out_specs=P(None, ("leaf", "blk")),
        check_vma=False,
    )
```
